32 devices in a mesh: dp: 4 (over y, x), tensor: 8 (over z, core).
Axes of the slice: x: 2, y: 2, z: 4, core: 2. Of those that a mesh axis runs over, the one named last changes fastest.
Arguments:
- layer_input: bfloat16 [8192, 2048], P(('dp', 'tensor')), may hold values from -6 to 6
- segment_ids: int32 [8192], P('dp'), may hold values from 0 to 31, never falling along the last dimension, each value on 1 to 512 neighbouring positions
- first_gain: float32 [2048], replicated, may hold values from 0.5 to 1.5
- first_shift: float32 [2048], replicated, may hold values from -3 to 3
- qkv_weight: bfloat16 [3, 2048, 2048], P(None, 'dp', 'tensor'), may hold values from -0.125 to 0.125
- query_value_bias: float32 [2, 2048], P(None, 'tensor'), may hold values from -3 to 3
- dense_weight: bfloat16 [2048, 2048], P('tensor', 'dp'), may hold values from -0.5 to 0.5
- dense_bias: float32 [2048], replicated, may hold values from -2 to 2
- second_gain: float32 [2048], replicated, may hold values from 0.5 to 1.5
- second_shift: float32 [2048], replicated, may hold values from -3 to 3
- up_weight: bfloat16 [2048, 8192], P('dp', 'tensor'), may hold values from -0.125 to 0.125
- up_bias: float32 [8192], P('tensor'), may hold values from -3 to 3
- down_weight: bfloat16 [8192, 2048], P('tensor', 'dp'), may hold values from -0.0625 to 0.0625
- down_bias: float32 [2048], replicated, may hold values from -2 to 2
- out_grad: bfloat16 [8192, 2048], P(('dp', 'tensor')), may hold values from -6 to 6
Outputs:
- layer_out: bfloat16 [8192, 2048], P(('dp', 'tensor'))
- input_grad: float32 [8192, 2048], P(('dp', 'tensor'))
- first_gain_grad: float32 [2048], replicated
- first_shift_grad: float32 [2048], replicated
- qkv_weight_grad: float32 [3, 2048, 2048], P(None, 'dp', 'tensor')
- query_value_bias_grad: float32 [2, 2048], P(None, 'tensor')
- dense_weight_grad: float32 [2048, 2048], P('tensor', 'dp')
- dense_bias_grad: float32 [2048], replicated
- second_gain_grad: float32 [2048], replicated
- second_shift_grad: float32 [2048], replicated
- up_weight_grad: float32 [2048, 8192], P('dp', 'tensor')
- up_bias_grad: float32 [8192], P('tensor')
- down_weight_grad: float32 [8192, 2048], P('tensor', 'dp')
- down_bias_grad: float32 [2048], replicated
The draws below stay inside these ranges and needn't reach their ends.
Inputs may be any that keep to these rules, and one draw needn't show every extreme that they name: `segment_ids`: segment numbers never fall along the whole array; a run of equal numbers is one document of at most 512 tokens, and some document has exactly that many.
All inputs are finite; a program needn't handle non-finite values.
Results may differ from the reference program's by a relative error of at most 0.014.
Values may be sent and summed in bfloat16 or wider, within the bound.
A program may use at most 256 MiB of HBM per device.

```python
import math
import jax
import jax.numpy as jnp
import numpy as np
from jax import lax

D = 2048
HEADS = 32
HEAD_DIM = 64
FF = 8192
SEQ_LEN = 2048
TOKENS = 8192
DOCS = 32
N_DP = 4


def level_of(rng, extent, pieces, least, top_value):
    def one(position, parts):
        heights = jax.random.uniform(jax.random.fold_in(jax.random.fold_in(rng, 6), position), (parts,), jnp.float32, least / len(pieces), top_value / len(pieces))
        return jnp.repeat(jnp.exp(heights), extent[position] // parts).reshape((-1,) + (1,) * (len(extent) - position - 1))

    factor_of = one(*pieces[0])
    for cut in pieces[1:]:
        factor_of = factor_of * one(*cut)
    return factor_of


def split_up(count, total, reach, skew):
    weights = [(1 << 20) // math.isqrt(grade ** skew) + 1 for grade in range(2, count + 1)]
    spare, holding = total - reach - (count - 1), [1] * (count - 1)
    while spare > 0:
        candidates = [i for i in range(count - 1) if holding[i] < reach]
        pool, budget = sum([weights[i] for i in candidates]), spare
        for i in candidates:
            addition = min(reach - holding[i], max(1, budget * weights[i] // pool), spare)
            holding[i] = holding[i] + addition
            spare = spare - addition
    return np.array([reach] + holding)


def uneven_parts(own_key, amount, total, bound, lean):
    if amount == 2:
        one = jax.random.randint(own_key, (), max(1, total - bound), min(bound, total - 1) + 1)
        return jnp.stack([one, total - one])
    tallies = jnp.asarray(split_up(amount, total, bound, lean), jnp.int32)
    pairs = (amount - 1) // 2
    giver, taker = tallies[1:1 + 2 * pairs:2], tallies[2:2 + 2 * pairs:2]
    slack = jnp.minimum(giver - 1, bound - taker)
    passed = jax.random.randint(jax.random.fold_in(own_key, 1), (pairs,), 0, 1 << 20) % (slack + 1)
    tallies = tallies.at[1:1 + 2 * pairs:2].set(giver - passed).at[2:2 + 2 * pairs:2].set(taker + passed)
    return tallies[jax.random.permutation(jax.random.fold_in(own_key, 2), amount)]


def normal_values(rng, dims, deviation, bound, cuts=(), held_as=jnp.bfloat16):
    factor_of = level_of(rng, dims, cuts, -0.22, 0.18) if cuts else 1.0
    drawn = jax.random.normal(rng, dims, jnp.float32) * deviation * factor_of
    return jnp.minimum(jnp.maximum(drawn, -bound), bound).astype(held_as)


def setup_inputs(seed: int = 0) -> dict:
    key_list = jax.random.split(jax.random.key(seed), 16)
    return {
        "layer_input": normal_values(key_list[0], (TOKENS, D), 1.0, 6.0, ((0, 32),)),
        "segment_ids": jnp.searchsorted(jnp.cumsum(uneven_parts(key_list[1], DOCS, TOKENS, SEQ_LEN // 4, 0)), jnp.arange(TOKENS), side="right").astype(jnp.int32),
        "first_gain": jnp.clip(1.0 + 0.1 * jax.random.normal(key_list[2], (D,), jnp.float32), 0.5, 1.5),
        "first_shift": normal_values(key_list[3], (D,), 0.5, 3.0, (), jnp.float32),
        "qkv_weight": normal_values(key_list[4], (3, D, D), D ** -0.5, 0.125, ((1, 4), (2, 8))),
        "query_value_bias": normal_values(key_list[5], (2, D), 0.5, 3.0, ((1, 8),), jnp.float32),
        "dense_weight": normal_values(key_list[6], (D, D), (D // 16) ** -0.5, 0.5, ((0, 8), (1, 4))),
        "dense_bias": normal_values(key_list[7], (D,), 0.3, 2.0, (), jnp.float32),
        "second_gain": jnp.clip(1.0 + 0.1 * jax.random.normal(key_list[8], (D,), jnp.float32), 0.5, 1.5),
        "second_shift": normal_values(key_list[9], (D,), 0.5, 3.0, (), jnp.float32),
        "up_weight": normal_values(key_list[10], (D, FF), D ** -0.5, 0.125, ((0, 4), (1, 8))),
        "up_bias": normal_values(key_list[11], (FF,), 0.5, 3.0, ((0, 8),), jnp.float32),
        "down_weight": normal_values(key_list[12], (FF, D), FF ** -0.5, 0.0625, ((0, 8), (1, 4))),
        "down_bias": normal_values(key_list[13], (D,), 0.3, 2.0, (), jnp.float32),
        "out_grad": normal_values(key_list[14], (TOKENS, D), 1.0, 6.0, ((0, 32),)),
    }


PRECISE = lax.Precision.HIGHEST
EPSILON = 1e-05
NEG_FILL = -1e+30

@jax.custom_vjp
def low(v):
    return lax.optimization_barrier(v.astype(jnp.bfloat16)).astype(jnp.float32)

@jax.custom_vjp
def low_back(v):
    return v

def low_keep(v):
    return (low(v), None)

def low_pass(kept, grad):
    return (grad,)

def back_keep(v):
    return (v, None)

def back_low(kept, grad):
    return (low(grad),)
low.defvjp(low_keep, low_pass)
low_back.defvjp(back_keep, back_low)

def layer_norm(source_rows, norm_gain, norm_shift):
    centre = lax.optimization_barrier(jnp.mean(source_rows, axis=-1, keepdims=True))
    centred = source_rows - centre
    spread = lax.optimization_barrier(jnp.mean(centred * centred, axis=-1, keepdims=True))
    return centred * lax.rsqrt(spread + EPSILON) * norm_gain + norm_shift

def attend(query_all, key_all, value_all, segments):
    block_len = min(512, SEQ_LEN)
    blocks = SEQ_LEN // block_len
    factor = 1.0 / math.sqrt(HEAD_DIM)
    key_heads = key_all.reshape(SEQ_LEN, HEADS, HEAD_DIM)
    value_heads = value_all.reshape(SEQ_LEN, HEADS, HEAD_DIM)
    query_blocks = query_all.reshape(blocks, block_len, HEADS, HEAD_DIM)
    positions = jnp.arange(SEQ_LEN, dtype=jnp.int32)
    slopes = jnp.power(2.0, -8.0 * (jnp.arange(HEADS, dtype=jnp.int32) + 1).astype(jnp.float32) / HEADS)

    def one_block(operands):
        query_rows, block_id = operands
        first_row = block_id * block_len
        query_pos = first_row + jnp.arange(block_len, dtype=jnp.int32)
        query_seg = lax.dynamic_slice_in_dim(segments, first_row, block_len)
        scores = jnp.einsum('bhe,khe->hbk', query_rows, key_heads, precision=PRECISE) * factor
        distance = (query_pos[:, None] - positions[None, :]).astype(scores.dtype)
        scores = scores - slopes.astype(scores.dtype)[:, None, None] * distance[None]
        allowed = (query_seg[:, None] == segments[None, :]) & (positions[None, :] <= query_pos[:, None])
        scores = low_back(jnp.where(allowed[None], scores, NEG_FILL))
        weights = low(jax.nn.softmax(scores, axis=-1))
        return jnp.einsum('hbk,khe->bhe', weights, value_heads, precision=PRECISE)
    attended = lax.map(jax.checkpoint(one_block), (query_blocks, jnp.arange(blocks, dtype=jnp.int32)))
    return attended.reshape(SEQ_LEN, D)

def transformer_layer(token_rows, segments, first_gain, first_shift, qkv_weight, query_value_bias, dense_weight, dense_bias, second_gain, second_shift, up_weight, up_bias, down_weight, down_bias):
    normed1 = low(layer_norm(token_rows, first_gain, first_shift))
    projected = jnp.einsum('sd,cde->cse', normed1, qkv_weight, precision=PRECISE)
    zero_row = jnp.zeros_like(query_value_bias[0])
    bias_rows = jnp.stack([query_value_bias[0], zero_row, query_value_bias[1]])
    projected = low(low_back(projected + bias_rows[:, None, :]))
    attended = low(low_back(attend(projected[0], projected[1], projected[2], segments)))
    attn_branch = low_back(jnp.dot(attended, dense_weight, precision=PRECISE) + dense_bias)
    residual = token_rows + attn_branch
    normed2 = low(layer_norm(residual, second_gain, second_shift))
    pre_act = low_back(jnp.dot(normed2, up_weight, precision=PRECISE) + up_bias)
    activated = low(jax.nn.gelu(pre_act, approximate=False))
    mlp_branch = low_back(jnp.dot(activated, down_weight, precision=PRECISE) + down_bias)
    return residual + mlp_branch

def reference(layer_input, segment_ids, first_gain, first_shift, qkv_weight, query_value_bias, dense_weight, dense_bias, second_gain, second_shift, up_weight, up_bias, down_weight, down_bias, out_grad):
    params = tuple((item.astype(jnp.float32) for item in (first_gain, first_shift, qkv_weight, query_value_bias, dense_weight, dense_bias, second_gain, second_shift, up_weight, up_bias, down_weight, down_bias)))
    inputs = layer_input.astype(jnp.float32).reshape(N_DP, SEQ_LEN, D)
    cotangents = out_grad.astype(jnp.float32).reshape(N_DP, SEQ_LEN, D)
    segments_all = segment_ids.reshape(N_DP, SEQ_LEN)

    def per_sequence(accum, sequence_item):
        token_rows, segments, cotangent = sequence_item

        def forward(rows_in, param_tuple):
            return transformer_layer(rows_in, segments, *param_tuple)
        result, backward = jax.vjp(forward, token_rows, params)
        rows_grad, param_grads = backward(cotangent)
        accum = tuple((total + piece for total, piece in zip(accum, param_grads)))
        return (accum, (result.astype(jnp.bfloat16), rows_grad))
    initial = tuple((jnp.zeros_like(item) for item in params))
    totals, (outputs, input_grads) = lax.scan(per_sequence, initial, (inputs, segments_all, cotangents))
    return (outputs.reshape(TOKENS, D), input_grads.reshape(TOKENS, D), totals[0], totals[1], totals[2], totals[3], totals[4], totals[5], totals[6], totals[7], totals[8], totals[9], totals[10], totals[11])
```

```python
import functools
import math

import jax
import jax.numpy as jnp
from jax import lax
from jax.experimental import pallas as pl
from jax.experimental.pallas import tpu as pltpu
from jax.sharding import PartitionSpec as P

HEADS = 32
EPSILON = 1e-05
MESH = pl.DeviceIdType.MESH
HEAD_DIM = 64
PAIR = 2 * HEAD_DIM
Q_BLOCK = 256
MASKED = -1e32
NT = (((1,), (1,)), ((), ()))
NN = (((1,), (0,)), ((), ()))


def key_window(seq_len, block):
    width = min(seq_len, Q_BLOCK + seq_len // 4)
    start = jnp.maximum(block * Q_BLOCK + Q_BLOCK - width, 0)
    return width, pl.multiple_of(start, 128)


def masked_distance(seg_row, seg_col, first_query, first_key, width):
    shape = (width, Q_BLOCK)
    key_pos = lax.broadcasted_iota(jnp.int32, shape, 0) + first_key
    query_pos = lax.broadcasted_iota(jnp.int32, shape, 1) + first_query
    delta = key_pos - query_pos
    allowed = (seg_col == seg_row) & (delta <= 0)
    return jnp.where(allowed, delta.astype(jnp.float32), MASKED)


def half_lanes(rows, half):
    lane = lax.broadcasted_iota(jnp.int32, rows.shape, 1)
    return jnp.where((lane < HEAD_DIM) == (half == 0), rows, jnp.zeros_like(rows))


def forward_kernel(slope_ref, proj_ref, seg_row_ref, seg_col_ref, out_ref, lse_ref, value_t, bias_ref):
    seq_len = proj_ref.shape[0]
    width_all = out_ref.shape[1]
    block = pl.program_id(0)

    @pl.when(block == 0)
    def _():
        value_t[...] = proj_ref[:, 2 * width_all :].T

    first = pl.multiple_of(block * Q_BLOCK, Q_BLOCK)
    width, start = key_window(seq_len, block)
    queries = pl.ds(first, Q_BLOCK)
    keys = pl.ds(start, width)
    bias_ref[...] = masked_distance(
        seg_row_ref[:, queries], seg_col_ref[keys, :], first, start, width
    )
    for pair in range(width_all // PAIR):
        cols = pair * PAIR
        query_pair = proj_ref[queries, cols : cols + PAIR] * 0.125
        key_pair = proj_ref[keys, width_all + cols : width_all + cols + PAIR]
        value_pair = value_t[cols : cols + PAIR, keys]
        mixed = []
        for half in range(2):
            head = 2 * pair + half
            scores = lax.dot_general(
                key_pair, half_lanes(query_pair, half), NT, preferred_element_type=jnp.float32
            )
            scores = scores + slope_ref[head] * bias_ref[...]
            highest = jnp.max(scores, axis=0, keepdims=True)
            exponent = jnp.exp(scores - highest)
            total = jnp.sum(exponent, axis=0, keepdims=True)
            part = lax.dot_general(
                value_pair[half * HEAD_DIM : (half + 1) * HEAD_DIM],
                exponent.astype(jnp.bfloat16),
                NN,
                preferred_element_type=jnp.float32,
            )
            mixed.append(part / total)
            lse_ref[head : head + 1, :] = highest + jnp.log(total)
        out_ref[:, cols : cols + PAIR] = jnp.concatenate(mixed, axis=0).T.astype(jnp.bfloat16)


def attention_forward(projected, segments, slopes):
    seq_len, all_cols = projected.shape
    cols = all_cols // 3
    heads = cols // HEAD_DIM
    width = min(seq_len, Q_BLOCK + seq_len // 4)
    return pl.pallas_call(
        forward_kernel,
        grid=(seq_len // Q_BLOCK,),
        in_specs=[
            pl.BlockSpec(memory_space=pltpu.SMEM),
            pl.BlockSpec((seq_len, all_cols), lambda i: (0, 0)),
            pl.BlockSpec((1, seq_len), lambda i: (0, 0)),
            pl.BlockSpec((seq_len, 1), lambda i: (0, 0)),
        ],
        out_specs=[
            pl.BlockSpec((Q_BLOCK, cols), lambda i: (i, 0)),
            pl.BlockSpec((heads, Q_BLOCK), lambda i: (0, i)),
        ],
        out_shape=[
            jax.ShapeDtypeStruct((seq_len, cols), jnp.bfloat16),
            jax.ShapeDtypeStruct((heads, seq_len), jnp.float32),
        ],
        scratch_shapes=[
            pltpu.VMEM((cols, seq_len), jnp.bfloat16),
            pltpu.VMEM((width, Q_BLOCK), jnp.float32),
        ],
        compiler_params=pltpu.CompilerParams(vmem_limit_bytes=40 * 2**20),
        cost_estimate=pl.CostEstimate(flops=4 * seq_len * width * cols, bytes_accessed=6 * seq_len * cols, transcendentals=0),
        name="attention_forward",
    )(slopes, projected, segments[None, :], segments[:, None])


def backward_kernel(slope_ref, proj_ref, grad_ref, lse_ref, seg_row_ref, seg_col_ref, out_ref,
                    key_t, bias_ref, key_sum, value_sum):
    seq_len = proj_ref.shape[0]
    width_all = grad_ref.shape[1]
    block = pl.program_id(0)

    @pl.when(block == 0)
    def _():
        key_t[...] = proj_ref[:, width_all : 2 * width_all].T
        key_sum[...] = jnp.zeros_like(key_sum)
        value_sum[...] = jnp.zeros_like(value_sum)

    first = pl.multiple_of(block * Q_BLOCK, Q_BLOCK)
    width, start = key_window(seq_len, block)
    queries = pl.ds(first, Q_BLOCK)
    keys = pl.ds(start, width)
    bias_ref[...] = masked_distance(
        seg_row_ref[:, queries], seg_col_ref[keys, :], first, start, width
    )
    for pair in range(width_all // PAIR):
        cols = pair * PAIR
        query_pair = proj_ref[queries, cols : cols + PAIR] * 0.125
        key_pair = proj_ref[keys, width_all + cols : width_all + cols + PAIR]
        value_pair = proj_ref[keys, 2 * width_all + cols : 2 * width_all + cols + PAIR]
        grad_pair = grad_ref[queries, cols : cols + PAIR]
        query_grads = []
        key_part = value_part = None
        for half in range(2):
            head = 2 * pair + half
            query_half = half_lanes(query_pair, half)
            grad_half = half_lanes(grad_pair, half)
            scores = lax.dot_general(key_pair, query_half, NT, preferred_element_type=jnp.float32)
            probs = jnp.exp(scores + slope_ref[head] * bias_ref[...] - lse_ref[head : head + 1, queries])
            prob_grad = lax.dot_general(value_pair, grad_half, NT, preferred_element_type=jnp.float32)
            inner = jnp.sum(probs * prob_grad, axis=0, keepdims=True)
            score_grad = (probs * (prob_grad - inner)).astype(jnp.bfloat16)
            value_half = jnp.dot(probs.astype(jnp.bfloat16), grad_half, preferred_element_type=jnp.float32)
            key_half = jnp.dot(score_grad, query_half, preferred_element_type=jnp.float32)
            query_grads.append(
                jnp.dot(
                    key_t[cols + half * HEAD_DIM : cols + (half + 1) * HEAD_DIM, keys],
                    score_grad,
                    preferred_element_type=jnp.float32,
                )
                * 0.125
            )
            value_part = value_half if half == 0 else value_part + value_half
            key_part = key_half if half == 0 else key_part + key_half
        key_sum[keys, cols : cols + PAIR] += key_part
        value_sum[keys, cols : cols + PAIR] += value_part
        out_ref[queries, cols : cols + PAIR] = (
            jnp.concatenate(query_grads, axis=0).T.astype(jnp.bfloat16)
        )

    @pl.when(block == pl.num_programs(0) - 1)
    def _():
        out_ref[:, width_all : 2 * width_all] = key_sum[...].astype(jnp.bfloat16)
        out_ref[:, 2 * width_all :] = value_sum[...].astype(jnp.bfloat16)


def attention_backward(projected, head_grad, segments, slopes, log_sums):
    seq_len, all_cols = projected.shape
    cols = all_cols // 3
    heads = cols // HEAD_DIM
    width = min(seq_len, Q_BLOCK + seq_len // 4)
    return pl.pallas_call(
        backward_kernel,
        grid=(seq_len // Q_BLOCK,),
        in_specs=[
            pl.BlockSpec(memory_space=pltpu.SMEM),
            pl.BlockSpec((seq_len, all_cols), lambda i: (0, 0)),
            pl.BlockSpec((seq_len, cols), lambda i: (0, 0)),
            pl.BlockSpec((heads, seq_len), lambda i: (0, 0)),
            pl.BlockSpec((1, seq_len), lambda i: (0, 0)),
            pl.BlockSpec((seq_len, 1), lambda i: (0, 0)),
        ],
        out_specs=pl.BlockSpec((seq_len, all_cols), lambda i: (0, 0)),
        out_shape=jax.ShapeDtypeStruct((seq_len, all_cols), jnp.bfloat16),
        scratch_shapes=[
            pltpu.VMEM((cols, seq_len), jnp.bfloat16),
            pltpu.VMEM((width, Q_BLOCK), jnp.float32),
            pltpu.VMEM((seq_len, cols), jnp.float32),
            pltpu.VMEM((seq_len, cols), jnp.float32),
        ],
        compiler_params=pltpu.CompilerParams(vmem_limit_bytes=48 * 2**20),
        cost_estimate=pl.CostEstimate(flops=10 * seq_len * width * cols, bytes_accessed=14 * seq_len * cols, transcendentals=0),
        name="attention_backward",
    )(slopes, projected, head_grad, log_sums, segments[None, :], segments[:, None])


ROW_TILE = 16
SUBS = 2


def remote(src, dst, send_sem, recv_sem, peer):
    return pltpu.make_async_remote_copy(
        src_ref=src,
        dst_ref=dst,
        send_sem=send_sem,
        recv_sem=recv_sem,
        device_id={"tensor": peer},
        device_id_type=MESH,
    )


class Line:
    def __init__(self, chips, rows):
        self.chips = chips
        self.sub_rows = rows // SUBS
        self.me = lax.axis_index("tensor")
        self.place = self.me // 2
        self.core = self.me % 2
        self.above = self.me + 2
        self.below = self.me - 2
        self.partner = self.me + 1 - 2 * self.core
        self.has_above = self.place < chips - 1
        self.has_below = self.place > 0

    def rows(self, sub):
        return pl.ds(sub * self.sub_rows, self.sub_rows)

    def enter(self):
        barrier = pltpu.get_barrier_semaphore()

        def greet(peer):
            pl.semaphore_signal(barrier, inc=1, device_id={"tensor": peer}, device_id_type=MESH)

        pl.when(self.has_above)(lambda: greet(self.above))
        pl.when(self.has_below)(lambda: greet(self.below))
        greet(self.partner)
        pl.semaphore_wait(
            barrier, 1 + self.has_above.astype(jnp.int32) + self.has_below.astype(jnp.int32)
        )


class Gather:
    def __init__(self, line, source, target, sems):
        self.line, self.source, self.target = line, source, target
        self.own_sem, self.line_send, self.line_recv, self.pair_send, self.pair_recv = sems

    @staticmethod
    def scratch(chips):
        dma = pltpu.SemaphoreType.DMA
        return [
            dma((SUBS,)),
            dma((2, chips, SUBS)),
            dma((2, chips, SUBS)),
            dma((chips, SUBS)),
            dma((chips, SUBS)),
        ]

    def hop(self, way, step, sub, src, block):
        peer = self.line.above if way == 0 else self.line.below
        return remote(
            src,
            self.target.at[block, self.line.rows(sub)],
            self.line_send.at[way, step, sub],
            self.line_recv.at[way, step, sub],
            peer,
        )

    def across(self, chip, sub, src, block):
        return remote(
            src,
            self.target.at[block, self.line.rows(sub)],
            self.pair_send.at[chip, sub],
            self.pair_recv.at[chip, sub],
            self.line.partner,
        )

    def own(self, sub):
        return pltpu.make_async_copy(
            self.source.at[self.line.rows(sub)],
            self.target.at[self.line.me, self.line.rows(sub)],
            self.own_sem.at[sub],
        )

    def start(self, sub):
        line = self.line
        src = self.source.at[line.rows(sub)]
        pl.when(line.has_above)(lambda: self.hop(0, 0, sub, src, line.me).start())
        pl.when(line.has_below)(lambda: self.hop(1, 0, sub, src, line.me).start())
        self.across(line.place, sub, src, line.me).start()
        self.own(sub).start()

    def step(self, sub, step):
        line = self.line
        for way, sign in ((0, -1), (1, 1)):
            block = line.me + 2 * sign * (step + 1)
            onward = line.has_above if way == 0 else line.has_below

            @pl.when(block >= 0 if way == 0 else block < 2 * line.chips)
            def _():
                src = self.target.at[block, line.rows(sub)]
                self.hop(way, step, sub, src, block).wait_recv()
                if step + 1 < line.chips - 1:
                    pl.when(onward)(lambda: self.hop(way, step + 1, sub, src, block).start())
                self.across(block // 2, sub, src, block).start()

    def finish(self):
        line = self.line
        for sub in range(SUBS):
            src = self.source.at[line.rows(sub)]
            for chip in range(line.chips):
                copy = self.across(chip, sub, src, 2 * chip + 1 - line.core)
                copy.wait_recv()
                copy.wait_send()
            for step in range(line.chips - 1):
                sent_up = line.has_above & (line.place >= step)
                sent_down = line.has_below & (line.place + step < line.chips)
                pl.when(sent_up)(lambda: self.hop(0, step, sub, src, line.me).wait_send())
                pl.when(sent_down)(lambda: self.hop(1, step, sub, src, line.me).wait_send())
            self.own(sub).wait()


class Reduce:
    def __init__(self, line, partial, bufs, sems):
        self.line, self.partial = line, partial
        self.held, self.paired, self.from_below, self.from_above = bufs
        self.held_sem, self.pair_send, self.pair_recv, self.line_send, self.line_recv = sems

    @staticmethod
    def scratch(chips, rows, width):
        dma = pltpu.SemaphoreType.DMA
        return [pltpu.VMEM((chips, rows, width), jnp.bfloat16)] * 4 + [
            dma((chips, SUBS)),
            dma((chips, SUBS)),
            dma((chips, SUBS)),
            dma((2, chips, SUBS)),
            dma((2, chips, SUBS)),
        ]

    def load(self, chip, sub):
        rows = self.line.rows(sub)
        return pltpu.make_async_copy(
            self.partial.at[2 * chip + self.line.core, rows],
            self.held.at[chip, rows],
            self.held_sem.at[chip, sub],
        )

    def across(self, chip, sub):
        rows = self.line.rows(sub)
        return remote(
            self.partial.at[2 * chip + 1 - self.line.core, rows],
            self.paired.at[chip, rows],
            self.pair_send.at[chip, sub],
            self.pair_recv.at[chip, sub],
            self.line.partner,
        )

    def hop(self, way, chip, sub):
        rows = self.line.rows(sub)
        return remote(
            self.held.at[chip, rows],
            (self.from_below if way == 0 else self.from_above).at[chip, rows],
            self.line_send.at[way, chip, sub],
            self.line_recv.at[way, chip, sub],
            self.line.above if way == 0 else self.line.below,
        )

    def start(self):
        line = self.line
        order = []
        for step in range(line.chips):
            chip = line.chips - 1 - step // 2 if step % 2 == 0 else step // 2
            order.append(chip)
        for sub in range(SUBS):
            for chip in order:
                self.across(chip, sub).start()
                self.load(chip, sub).start()
        zeros = jnp.zeros((ROW_TILE, self.held.shape[2]), jnp.bfloat16)

        def clear(buf, chip):
            @pl.loop(0, self.held.shape[1] // ROW_TILE)
            def _(tile):
                buf[chip, pl.ds(pl.multiple_of(tile * ROW_TILE, ROW_TILE), ROW_TILE), :] = zeros

        pl.when(jnp.logical_not(line.has_below))(lambda: clear(self.from_below, 0))
        pl.when(jnp.logical_not(line.has_above))(lambda: clear(self.from_above, line.chips - 1))

    def step(self, sub, step):
        line = self.line
        for way in range(2):
            chip = line.chips - 1 - step if way == 0 else step
            arrived = self.from_below if way == 0 else self.from_above
            inner = line.has_below if way == 0 else line.has_above

            @pl.when(chip > line.place if way == 0 else chip < line.place)
            def _():
                self.load(chip, sub).wait()
                self.across(chip, sub).wait_recv()

                def add(with_arrived):
                    @pl.loop(0, line.sub_rows // ROW_TILE)
                    def _(tile):
                        at = pl.ds(
                            pl.multiple_of(sub * line.sub_rows + tile * ROW_TILE, ROW_TILE), ROW_TILE
                        )
                        total = self.held[chip, at, :].astype(jnp.float32)
                        total = total + self.paired[chip, at, :].astype(jnp.float32)
                        if with_arrived:
                            total = total + arrived[chip, at, :].astype(jnp.float32)
                        self.held[chip, at, :] = total.astype(jnp.bfloat16)

                @pl.when(inner)
                def _():
                    self.hop(way, chip, sub).wait_recv()
                    add(True)

                pl.when(jnp.logical_not(inner))(lambda: add(False))
                self.hop(way, chip, sub).start()

    def arrive(self, sub):
        line = self.line
        place = line.place
        self.load(place, sub).wait()
        self.across(place, sub).wait_recv()
        pl.when(line.has_below)(lambda: self.hop(0, place, sub).wait_recv())
        pl.when(line.has_above)(lambda: self.hop(1, place, sub).wait_recv())

    def total(self, at):
        place = self.line.place
        total = self.held[place, at, :].astype(jnp.float32)
        total = total + self.paired[place, at, :].astype(jnp.float32)
        total = total + self.from_below[place, at, :].astype(jnp.float32)
        return total + self.from_above[place, at, :].astype(jnp.float32)

    def finish(self):
        line = self.line
        for sub in range(SUBS):
            for chip in range(line.chips):
                self.across(chip, sub).wait_send()
                pl.when(chip > line.place)(lambda: self.hop(0, chip, sub).wait_send())
                pl.when(chip < line.place)(lambda: self.hop(1, chip, sub).wait_send())


def for_tiles(line, sub, body):
    @pl.loop(0, line.sub_rows // ROW_TILE)
    def _(tile):
        body(pl.ds(pl.multiple_of(sub * line.sub_rows + tile * ROW_TILE, ROW_TILE), ROW_TILE))


def run_line(line, reduce, gather, rows_done):
    steps = line.chips - 1
    line.enter()
    if reduce is not None:
        reduce.start()
    for sub in range(SUBS + 1):
        for step in range(steps):
            if reduce is not None and sub < SUBS:
                reduce.step(sub, step)
            if gather is not None and sub >= 1:
                gather.step(sub - 1, step)
        if sub < SUBS:
            if reduce is not None:
                reduce.arrive(sub)
            for_tiles(line, sub, rows_done)
            if gather is not None:
                gather.start(sub)
    if reduce is not None:
        reduce.finish()
    if gather is not None:
        gather.finish()


def unit_of(rows):
    centre = jnp.mean(rows, axis=1, keepdims=True)
    centred = rows - centre
    inv_std = lax.rsqrt(jnp.mean(centred * centred, axis=1, keepdims=True) + EPSILON)
    return centred * inv_std, inv_std


def norm_back(grad, unit, inv_std, gain):
    scaled = grad * gain
    return inv_std * (
        scaled
        - jnp.mean(scaled, axis=1, keepdims=True)
        - unit * jnp.mean(scaled * unit, axis=1, keepdims=True)
    )


def fold(rows):
    return jnp.sum(rows.reshape(-1, 8, rows.shape[1]), axis=0)


def norm_gather_kernel(chips, input_ref, gain_ref, shift_ref, whole_ref, normed_ref, *sems):
    line = Line(chips, input_ref.shape[0])
    gather = Gather(line, normed_ref, whole_ref, sems)

    def rows_done(at):
        unit, _ = unit_of(input_ref[at, :].astype(jnp.float32))
        normed_ref[at, :] = (unit * gain_ref[...] + shift_ref[...]).astype(jnp.bfloat16)

    run_line(line, None, gather, rows_done)


def branch_norm_gather_kernel(
    chips, partial_ref, input_ref, bias_ref, gain_ref, shift_ref, whole_ref, residual_ref, normed_ref, *rest
):
    line = Line(chips, input_ref.shape[0])
    reduce = Reduce(line, partial_ref, rest[:4], rest[4:9])
    gather = Gather(line, normed_ref, whole_ref, rest[9:])

    def rows_done(at):
        residual = input_ref[at, :].astype(jnp.float32) + (reduce.total(at) + bias_ref[...])
        residual_ref[at, :] = residual
        unit, _ = unit_of(residual)
        normed_ref[at, :] = (unit * gain_ref[...] + shift_ref[...]).astype(jnp.bfloat16)

    run_line(line, reduce, gather, rows_done)


def grad_gather_kernel(
    chips, partial_ref, residual_ref, grad_ref, gain_ref, whole_ref, residual_grad_ref, sums_ref, branch_ref, *rest
):
    line = Line(chips, grad_ref.shape[0])
    reduce = Reduce(line, partial_ref, rest[:4], rest[4:9])
    gather = Gather(line, branch_ref, whole_ref, rest[9:])
    sums_ref[...] = jnp.zeros_like(sums_ref)

    def rows_done(at):
        unit, inv_std = unit_of(residual_ref[at, :])
        grad = reduce.total(at)
        out_grad = grad_ref[at, :].astype(jnp.float32)
        residual_grad = out_grad + norm_back(grad, unit, inv_std, gain_ref[...])
        residual_grad_ref[at, :] = residual_grad
        branch = residual_grad.astype(jnp.bfloat16)
        branch_ref[at, :] = branch
        sums_ref[0] += fold(grad * unit)
        sums_ref[1] += fold(grad)
        sums_ref[2] += fold(branch.astype(jnp.float32))
        sums_ref[3] += fold(out_grad)

    run_line(line, reduce, gather, rows_done)


def grad_kernel(chips, partial_ref, input_ref, residual_grad_ref, gain_ref, out_ref, sums_ref, *rest):
    line = Line(chips, input_ref.shape[0])
    reduce = Reduce(line, partial_ref, rest[:4], rest[4:9])
    sums_ref[...] = jnp.zeros_like(sums_ref)

    def rows_done(at):
        unit, inv_std = unit_of(input_ref[at, :].astype(jnp.float32))
        grad = reduce.total(at)
        out_ref[at, :] = residual_grad_ref[at, :] + norm_back(grad, unit, inv_std, gain_ref[...])
        sums_ref[0] += fold(grad * unit)
        sums_ref[1] += fold(grad)

    run_line(line, reduce, None, rows_done)


def line_call(kernel, name, collective_id, operands, outs, gathers, reduces, rows, width):
    chips = lax.axis_size("tensor") // 2
    whole = jax.ShapeDtypeStruct((2 * chips, rows, width), jnp.bfloat16)
    in_vmem = pl.BlockSpec(memory_space=pltpu.VMEM)
    in_place = pl.BlockSpec(memory_space=pl.ANY)
    scratch = []
    if gathers:
        scratch.append(pltpu.VMEM((rows, width), jnp.bfloat16))
    if reduces:
        scratch += Reduce.scratch(chips, rows, width)
    if gathers:
        scratch += Gather.scratch(chips)
    return pl.pallas_call(
        functools.partial(kernel, chips),
        in_specs=([in_place] if reduces else []) + [in_vmem] * (len(operands) - int(reduces)),
        out_specs=([in_place] if gathers else []) + [in_vmem] * len(outs),
        out_shape=([whole] if gathers else []) + list(outs),
        scratch_shapes=scratch,
        compiler_params=pltpu.CompilerParams(
            collective_id=collective_id, has_side_effects=True, vmem_limit_bytes=48 * 2**20
        ),
        cost_estimate=pl.CostEstimate(
            flops=8 * rows * width * 100, bytes_accessed=100 * rows * width, transcendentals=0
        ),
        name=name,
    )(*operands)


def over_dp(grad, dimension):
    return lax.psum_scatter(
        grad.astype(jnp.bfloat16), "dp", scatter_dimension=dimension, tiled=True
    ).astype(jnp.float32)


def shards(
    layer_input,
    segment_ids,
    first_gain,
    first_shift,
    qkv_weight,
    query_value_bias,
    dense_weight,
    dense_bias,
    second_gain,
    second_shift,
    up_weight,
    up_bias,
    down_weight,
    down_bias,
    out_grad,
):
    rows, width = layer_input.shape
    ranks = lax.axis_size("tensor")
    tokens = ranks * rows
    f32_rows = jax.ShapeDtypeStruct((rows, width), jnp.float32)

    qkv_full = lax.all_gather(qkv_weight, "dp", axis=1, tiled=True)
    dense_full = lax.all_gather(dense_weight, "dp", axis=1, tiled=True)
    up_full = lax.all_gather(up_weight, "dp", axis=0, tiled=True)
    down_full = lax.all_gather(down_weight, "dp", axis=1, tiled=True)
    out_whole = lax.all_gather(out_grad, "tensor", axis=0, tiled=True)

    head_width = qkv_full.shape[2]
    up_width = up_bias.shape[0]
    qkv_cat = jnp.transpose(qkv_full, (1, 0, 2)).reshape(width, 3 * head_width)

    (whole1,) = line_call(
        norm_gather_kernel, "norm_gather", 1,
        (layer_input, first_gain[None], first_shift[None]), (), True, False, rows, width,
    )
    whole1 = whole1.reshape(tokens, width)
    zero_bias = jnp.zeros_like(query_value_bias[0])
    bias_cat = jnp.concatenate([query_value_bias[0], zero_bias, query_value_bias[1]])
    projected = (jnp.dot(whole1, qkv_cat, preferred_element_type=jnp.float32) + bias_cat).astype(
        jnp.bfloat16
    )
    head_count = head_width // HEAD_DIM
    tensor_pos = lax.axis_index("tensor")
    global_heads = tensor_pos * head_count + jnp.arange(head_count, dtype=jnp.int32)
    slopes = jnp.power(2.0, -8.0 * (global_heads + 1).astype(jnp.float32) / HEADS)
    attended, log_sums = attention_forward(projected, segment_ids, slopes)
    attn_part = jnp.dot(attended, dense_full, preferred_element_type=jnp.float32).astype(jnp.bfloat16)
    whole2, residual = line_call(
        branch_norm_gather_kernel, "branch_norm_gather", 2,
        (attn_part.reshape(ranks, rows, width), layer_input, dense_bias[None], second_gain[None], second_shift[None]),
        (f32_rows,), True, True, rows, width,
    )
    whole2 = whole2.reshape(tokens, width)
    pre_act = jnp.dot(whole2, up_full, preferred_element_type=jnp.float32) + up_bias
    activated = jax.nn.gelu(pre_act, approximate=False).astype(jnp.bfloat16)
    mlp_part = jnp.dot(activated, down_full, preferred_element_type=jnp.float32).astype(jnp.bfloat16)
    mlp_rows = lax.psum_scatter(mlp_part, "tensor", scatter_dimension=0, tiled=True)
    mlp_branch = mlp_rows.astype(jnp.float32) + down_bias
    layer_out = (residual + mlp_branch).astype(jnp.bfloat16)

    act_grad = lax.dot_general(
        out_whole, down_full, (((1,), (1,)), ((), ())), preferred_element_type=jnp.float32
    )
    unused_out, gelu_back = jax.vjp(functools.partial(jax.nn.gelu, approximate=False), pre_act)
    pre_grad = gelu_back(act_grad)[0].astype(jnp.bfloat16)
    up_bias_part = jnp.sum(pre_grad.astype(jnp.float32), axis=0)
    normed2_part = lax.dot_general(
        pre_grad, up_full, (((1,), (1,)), ((), ())), preferred_element_type=jnp.float32
    ).astype(jnp.bfloat16)
    down_grad = lax.dot_general(
        activated, out_whole, (((0,), (0,)), ((), ())), preferred_element_type=jnp.float32
    )
    down_wgrad = over_dp(down_grad, 1)
    up_grad = lax.dot_general(
        whole2, pre_grad, (((0,), (0,)), ((), ())), preferred_element_type=jnp.float32
    )
    up_wgrad = over_dp(up_grad, 0)

    branch_whole, residual_grad, second_sums = line_call(
        grad_gather_kernel, "grad_gather", 3,
        (normed2_part.reshape(ranks, rows, width), residual, out_grad, second_gain[None]),
        (f32_rows, jax.ShapeDtypeStruct((4, 8, width), jnp.float32)), True, True, rows, width,
    )
    branch_whole = branch_whole.reshape(tokens, width)
    attended_grad = lax.dot_general(
        branch_whole, dense_full, (((1,), (1,)), ((), ())), preferred_element_type=jnp.float32
    ).astype(jnp.bfloat16)
    qkv_grad_cat = attention_backward(projected, attended_grad, segment_ids, slopes, log_sums)
    dense_grad = lax.dot_general(
        attended, branch_whole, (((0,), (0,)), ((), ())), preferred_element_type=jnp.float32
    )
    dense_wgrad = over_dp(dense_grad, 1)
    qkv_sums = jnp.sum(qkv_grad_cat.astype(jnp.float32), axis=0)
    bias_part = jnp.stack([qkv_sums[:head_width], qkv_sums[2 * head_width :]])
    qkv_grad_flat = lax.dot_general(
        whole1, qkv_grad_cat, (((0,), (0,)), ((), ())), preferred_element_type=jnp.float32
    )
    qkv_grad = jnp.transpose(qkv_grad_flat.reshape(width, 3, head_width), (1, 0, 2))
    qkv_wgrad = over_dp(qkv_grad, 1)
    normed1_part = lax.dot_general(
        qkv_grad_cat, qkv_cat, (((1,), (1,)), ((), ())), preferred_element_type=jnp.float32
    ).astype(jnp.bfloat16)
    input_grad, first_sums = line_call(
        grad_kernel, "grad_rows", 4,
        (normed1_part.reshape(ranks, rows, width), layer_input, residual_grad, first_gain[None]),
        (f32_rows, jax.ShapeDtypeStruct((2, 8, width), jnp.float32)), False, True, rows, width,
    )
    early = lax.psum(jnp.sum(second_sums, axis=1), ("dp", "tensor"))
    own = lax.psum((bias_part, up_bias_part), "dp")
    late = lax.psum(jnp.sum(first_sums, axis=1), ("dp", "tensor"))
    return (
        layer_out,
        input_grad,
        late[0],
        late[1],
        qkv_wgrad,
        own[0],
        dense_wgrad,
        early[2],
        early[0],
        early[1],
        up_wgrad,
        own[1],
        down_wgrad,
        early[3],
    )


def solution(mesh):
    token_rows = P(("dp", "tensor"), None)
    placed = (
        token_rows,
        P("dp"),
        P(),
        P(),
        P(None, "dp", "tensor"),
        P(None, "tensor"),
        P("tensor", "dp"),
        P(),
        P(),
        P(),
        P("dp", "tensor"),
        P("tensor"),
        P("tensor", "dp"),
        P(),
        token_rows,
    )
    return jax.shard_map(
        shards,
        mesh=mesh,
        in_specs=placed,
        out_specs=(
            token_rows,
            token_rows,
            P(),
            P(),
            P(None, "dp", "tensor"),
            P(None, "tensor"),
            P("tensor", "dp"),
            P(),
            P(),
            P(),
            P("dp", "tensor"),
            P("tensor"),
            P("tensor", "dp"),
            P(),
        ),
        check_vma=False,
    )
```

```python
import functools

import jax
import jax.numpy as jnp
from jax import lax
from jax.experimental import pallas as pl
from jax.experimental.pallas import tpu as pltpu
from jax.sharding import PartitionSpec as P


HEADS = 32
EPSILON = 1e-05
MESH = pl.DeviceIdType.MESH
HEAD_DIM = 64
PAIR = 2 * HEAD_DIM
Q_BLOCK = 256
MASKED = -1e32
NT = (((1,), (1,)), ((), ()))
NN = (((1,), (0,)), ((), ()))


def key_window(seq_len, block):
    width = min(seq_len, Q_BLOCK + seq_len // 4)
    start = jnp.maximum(block * Q_BLOCK + Q_BLOCK - width, 0)
    return width, pl.multiple_of(start, 128)


def masked_distance(seg_row, seg_col, first_query, first_key, width):
    shape = (width, Q_BLOCK)
    key_pos = lax.broadcasted_iota(jnp.int32, shape, 0) + first_key
    query_pos = lax.broadcasted_iota(jnp.int32, shape, 1) + first_query
    delta = key_pos - query_pos
    allowed = (seg_col == seg_row) & (delta <= 0)
    return jnp.where(allowed, delta.astype(jnp.float32), MASKED)


def half_lanes(rows, half):
    lane = lax.broadcasted_iota(jnp.int32, rows.shape, 1)
    return jnp.where((lane < HEAD_DIM) == (half == 0), rows, jnp.zeros_like(rows))


def forward_kernel(slope_ref, proj_ref, seg_row_ref, seg_col_ref, out_ref, lse_ref, value_t, bias_ref):
    seq_len = proj_ref.shape[0]
    width_all = out_ref.shape[1]
    block = pl.program_id(0)

    @pl.when(block == 0)
    def _():
        value_t[...] = proj_ref[:, 2 * width_all :].T

    first = pl.multiple_of(block * Q_BLOCK, Q_BLOCK)
    width, start = key_window(seq_len, block)
    queries = pl.ds(first, Q_BLOCK)
    keys = pl.ds(start, width)
    bias_ref[...] = masked_distance(
        seg_row_ref[:, queries], seg_col_ref[keys, :], first, start, width
    )
    for pair in range(width_all // PAIR):
        cols = pair * PAIR
        query_pair = proj_ref[queries, cols : cols + PAIR] * 0.125
        key_pair = proj_ref[keys, width_all + cols : width_all + cols + PAIR]
        value_pair = value_t[cols : cols + PAIR, keys]
        mixed = []
        for half in range(2):
            head = 2 * pair + half
            scores = lax.dot_general(
                key_pair, half_lanes(query_pair, half), NT, preferred_element_type=jnp.float32
            )
            scores = scores + slope_ref[head] * bias_ref[...]
            highest = jnp.max(scores, axis=0, keepdims=True)
            exponent = jnp.exp(scores - highest)
            total = jnp.sum(exponent, axis=0, keepdims=True)
            part = lax.dot_general(
                value_pair[half * HEAD_DIM : (half + 1) * HEAD_DIM],
                exponent.astype(jnp.bfloat16),
                NN,
                preferred_element_type=jnp.float32,
            )
            mixed.append(part / total)
            lse_ref[head : head + 1, :] = highest + jnp.log(total)
        out_ref[:, cols : cols + PAIR] = jnp.concatenate(mixed, axis=0).T.astype(jnp.bfloat16)


def attention_forward(projected, segments, slopes):
    seq_len, all_cols = projected.shape
    cols = all_cols // 3
    heads = cols // HEAD_DIM
    width = min(seq_len, Q_BLOCK + seq_len // 4)
    return pl.pallas_call(
        forward_kernel,
        grid=(seq_len // Q_BLOCK,),
        in_specs=[
            pl.BlockSpec(memory_space=pltpu.SMEM),
            pl.BlockSpec((seq_len, all_cols), lambda i: (0, 0)),
            pl.BlockSpec((1, seq_len), lambda i: (0, 0)),
            pl.BlockSpec((seq_len, 1), lambda i: (0, 0)),
        ],
        out_specs=[
            pl.BlockSpec((Q_BLOCK, cols), lambda i: (i, 0)),
            pl.BlockSpec((heads, Q_BLOCK), lambda i: (0, i)),
        ],
        out_shape=[
            jax.ShapeDtypeStruct((seq_len, cols), jnp.bfloat16),
            jax.ShapeDtypeStruct((heads, seq_len), jnp.float32),
        ],
        scratch_shapes=[
            pltpu.VMEM((cols, seq_len), jnp.bfloat16),
            pltpu.VMEM((width, Q_BLOCK), jnp.float32),
        ],
        compiler_params=pltpu.CompilerParams(vmem_limit_bytes=40 * 2**20),
        cost_estimate=pl.CostEstimate(flops=4 * seq_len * width * cols, bytes_accessed=6 * seq_len * cols, transcendentals=0),
        name="attention_forward",
    )(slopes, projected, segments[None, :], segments[:, None])


def backward_kernel(slope_ref, proj_ref, grad_ref, lse_ref, seg_row_ref, seg_col_ref, out_ref,
                    key_t, bias_ref, key_sum, value_sum):
    seq_len = proj_ref.shape[0]
    width_all = grad_ref.shape[1]
    block = pl.program_id(0)

    @pl.when(block == 0)
    def _():
        key_t[...] = proj_ref[:, width_all : 2 * width_all].T
        key_sum[...] = jnp.zeros_like(key_sum)
        value_sum[...] = jnp.zeros_like(value_sum)

    first = pl.multiple_of(block * Q_BLOCK, Q_BLOCK)
    width, start = key_window(seq_len, block)
    queries = pl.ds(first, Q_BLOCK)
    keys = pl.ds(start, width)
    bias_ref[...] = masked_distance(
        seg_row_ref[:, queries], seg_col_ref[keys, :], first, start, width
    )
    for pair in range(width_all // PAIR):
        cols = pair * PAIR
        query_pair = proj_ref[queries, cols : cols + PAIR] * 0.125
        key_pair = proj_ref[keys, width_all + cols : width_all + cols + PAIR]
        value_pair = proj_ref[keys, 2 * width_all + cols : 2 * width_all + cols + PAIR]
        grad_pair = grad_ref[queries, cols : cols + PAIR]
        query_grads = []
        key_part = value_part = None
        for half in range(2):
            head = 2 * pair + half
            query_half = half_lanes(query_pair, half)
            grad_half = half_lanes(grad_pair, half)
            scores = lax.dot_general(key_pair, query_half, NT, preferred_element_type=jnp.float32)
            probs = jnp.exp(scores + slope_ref[head] * bias_ref[...] - lse_ref[head : head + 1, queries])
            prob_grad = lax.dot_general(value_pair, grad_half, NT, preferred_element_type=jnp.float32)
            inner = jnp.sum(probs * prob_grad, axis=0, keepdims=True)
            score_grad = (probs * (prob_grad - inner)).astype(jnp.bfloat16)
            value_half = jnp.dot(probs.astype(jnp.bfloat16), grad_half, preferred_element_type=jnp.float32)
            key_half = jnp.dot(score_grad, query_half, preferred_element_type=jnp.float32)
            query_grads.append(
                jnp.dot(
                    key_t[cols + half * HEAD_DIM : cols + (half + 1) * HEAD_DIM, keys],
                    score_grad,
                    preferred_element_type=jnp.float32,
                )
                * 0.125
            )
            value_part = value_half if half == 0 else value_part + value_half
            key_part = key_half if half == 0 else key_part + key_half
        key_sum[keys, cols : cols + PAIR] += key_part
        value_sum[keys, cols : cols + PAIR] += value_part
        out_ref[queries, cols : cols + PAIR] = (
            jnp.concatenate(query_grads, axis=0).T.astype(jnp.bfloat16)
        )

    @pl.when(block == pl.num_programs(0) - 1)
    def _():
        out_ref[:, width_all : 2 * width_all] = key_sum[...].astype(jnp.bfloat16)
        out_ref[:, 2 * width_all :] = value_sum[...].astype(jnp.bfloat16)


def attention_backward(projected, head_grad, segments, slopes, log_sums):
    seq_len, all_cols = projected.shape
    cols = all_cols // 3
    heads = cols // HEAD_DIM
    width = min(seq_len, Q_BLOCK + seq_len // 4)
    return pl.pallas_call(
        backward_kernel,
        grid=(seq_len // Q_BLOCK,),
        in_specs=[
            pl.BlockSpec(memory_space=pltpu.SMEM),
            pl.BlockSpec((seq_len, all_cols), lambda i: (0, 0)),
            pl.BlockSpec((seq_len, cols), lambda i: (0, 0)),
            pl.BlockSpec((heads, seq_len), lambda i: (0, 0)),
            pl.BlockSpec((1, seq_len), lambda i: (0, 0)),
            pl.BlockSpec((seq_len, 1), lambda i: (0, 0)),
        ],
        out_specs=pl.BlockSpec((seq_len, all_cols), lambda i: (0, 0)),
        out_shape=jax.ShapeDtypeStruct((seq_len, all_cols), jnp.bfloat16),
        scratch_shapes=[
            pltpu.VMEM((cols, seq_len), jnp.bfloat16),
            pltpu.VMEM((width, Q_BLOCK), jnp.float32),
            pltpu.VMEM((seq_len, cols), jnp.float32),
            pltpu.VMEM((seq_len, cols), jnp.float32),
        ],
        compiler_params=pltpu.CompilerParams(vmem_limit_bytes=48 * 2**20),
        cost_estimate=pl.CostEstimate(flops=10 * seq_len * width * cols, bytes_accessed=14 * seq_len * cols, transcendentals=0),
        name="attention_backward",
    )(slopes, projected, head_grad, log_sums, segments[None, :], segments[:, None])


ROW_TILE = 16
SUBS = 4
LAG = 0


def remote(src, dst, send_sem, recv_sem, peer):
    return pltpu.make_async_remote_copy(
        src_ref=src,
        dst_ref=dst,
        send_sem=send_sem,
        recv_sem=recv_sem,
        device_id={"tensor": peer},
        device_id_type=MESH,
    )


class Line:
    def __init__(self, chips, rows):
        self.chips = chips
        self.sub_rows = rows // SUBS
        self.me = lax.axis_index("tensor")
        self.place = self.me // 2
        self.core = self.me % 2
        self.above = self.me + 2
        self.below = self.me - 2
        self.partner = self.me + 1 - 2 * self.core
        self.has_above = self.place < chips - 1
        self.has_below = self.place > 0

    def rows(self, sub):
        return pl.ds(pl.multiple_of(sub * self.sub_rows, self.sub_rows), self.sub_rows)

    def tile(self, sub, tile):
        return pl.ds(pl.multiple_of(sub * self.sub_rows + tile * ROW_TILE, ROW_TILE), ROW_TILE)

    def enter(self):
        barrier = pltpu.get_barrier_semaphore()

        def greet(peer):
            pl.semaphore_signal(barrier, inc=1, device_id={"tensor": peer}, device_id_type=MESH)

        pl.when(self.has_above)(lambda: greet(self.above))
        pl.when(self.has_below)(lambda: greet(self.below))
        greet(self.partner)
        pl.semaphore_wait(
            barrier, 1 + self.has_above.astype(jnp.int32) + self.has_below.astype(jnp.int32)
        )


class Gather:
    def __init__(self, line, source, target, sems):
        self.line, self.source, self.target = line, source, target
        self.own_sem, self.line_send, self.line_recv, self.pair_send, self.pair_recv = sems

    @staticmethod
    def scratch(chips):
        dma = pltpu.SemaphoreType.DMA
        return [
            dma((SUBS,)),
            dma((2, chips, SUBS)),
            dma((2, chips, SUBS)),
            dma((chips, SUBS)),
            dma((chips, SUBS)),
        ]

    def hop(self, way, step, sub, src, block):
        peer = self.line.above if way == 0 else self.line.below
        return remote(
            src,
            self.target.at[block, self.line.rows(sub)],
            self.line_send.at[way, step, sub],
            self.line_recv.at[way, step, sub],
            peer,
        )

    def across(self, chip, sub, src, block):
        return remote(
            src,
            self.target.at[block, self.line.rows(sub)],
            self.pair_send.at[chip, sub],
            self.pair_recv.at[chip, sub],
            self.line.partner,
        )

    def own(self, sub):
        return pltpu.make_async_copy(
            self.source.at[self.line.rows(sub)],
            self.target.at[self.line.me, self.line.rows(sub)],
            self.own_sem.at[sub],
        )

    def start(self, sub):
        line = self.line
        src = self.source.at[line.rows(sub)]
        pl.when(line.has_above)(lambda: self.hop(0, 0, sub, src, line.me).start())
        pl.when(line.has_below)(lambda: self.hop(1, 0, sub, src, line.me).start())
        self.across(line.place, sub, src, line.me).start()
        self.own(sub).start()

    def step(self, sub, step, live):
        line = self.line
        for way, sign in ((0, -1), (1, 1)):
            block = line.me + 2 * sign * (step + 1)
            onward = line.has_above if way == 0 else line.has_below
            inside = block >= 0 if way == 0 else block < 2 * line.chips

            @pl.when(live & inside)
            def _():
                src = self.target.at[block, line.rows(sub)]
                self.hop(way, step, sub, src, block).wait_recv()

                @pl.when(onward)
                def _():
                    self.hop(way, step + 1, sub, src, block).start()

                self.across(block // 2, sub, src, block).start()

    def finish(self):
        line = self.line

        @pl.loop(0, SUBS)
        def _(sub):
            src = self.source.at[line.rows(sub)]
            for chip in range(line.chips):
                copy = self.across(chip, sub, src, 2 * chip + 1 - line.core)
                copy.wait_recv()
                copy.wait_send()
            for step in range(line.chips - 1):
                sent_up = line.has_above & (line.place >= step)
                sent_down = line.has_below & (line.place + step < line.chips)
                pl.when(sent_up)(lambda: self.hop(0, step, sub, src, line.me).wait_send())
                pl.when(sent_down)(lambda: self.hop(1, step, sub, src, line.me).wait_send())
            self.own(sub).wait()


class Reduce:
    def __init__(self, line, partial, bufs, sems):
        self.line, self.partial = line, partial
        self.held, self.paired, self.from_below, self.from_above = bufs
        self.held_sem, self.pair_send, self.pair_recv, self.line_send, self.line_recv = sems

    @staticmethod
    def scratch(chips, rows, width):
        dma = pltpu.SemaphoreType.DMA
        return [pltpu.VMEM((chips, rows, width), jnp.bfloat16)] * 4 + [
            dma((chips, SUBS)),
            dma((chips, SUBS)),
            dma((chips, SUBS)),
            dma((2, chips, SUBS)),
            dma((2, chips, SUBS)),
        ]

    def load(self, chip, sub):
        rows = self.line.rows(sub)
        return pltpu.make_async_copy(
            self.partial.at[2 * chip + self.line.core, rows],
            self.held.at[chip, rows],
            self.held_sem.at[chip, sub],
        )

    def across(self, chip, sub):
        rows = self.line.rows(sub)
        return remote(
            self.partial.at[2 * chip + 1 - self.line.core, rows],
            self.paired.at[chip, rows],
            self.pair_send.at[chip, sub],
            self.pair_recv.at[chip, sub],
            self.line.partner,
        )

    def hop(self, way, chip, sub):
        rows = self.line.rows(sub)
        return remote(
            self.held.at[chip, rows],
            (self.from_below if way == 0 else self.from_above).at[chip, rows],
            self.line_send.at[way, chip, sub],
            self.line_recv.at[way, chip, sub],
            self.line.above if way == 0 else self.line.below,
        )

    def start(self):
        line = self.line
        order = []
        for step in range(line.chips):
            chip = line.chips - 1 - step // 2 if step % 2 == 0 else step // 2
            order.append(chip)

        @pl.loop(0, SUBS)
        def _(sub):
            for chip in order:
                self.across(chip, sub).start()
                self.load(chip, sub).start()

        zeros = jnp.zeros((ROW_TILE, self.held.shape[2]), jnp.bfloat16)

        def clear(buf, chip):
            @pl.loop(0, self.held.shape[1] // ROW_TILE)
            def _(tile):
                buf[chip, pl.ds(pl.multiple_of(tile * ROW_TILE, ROW_TILE), ROW_TILE), :] = zeros

        pl.when(jnp.logical_not(line.has_below))(lambda: clear(self.from_below, 0))
        pl.when(jnp.logical_not(line.has_above))(lambda: clear(self.from_above, line.chips - 1))

    def step(self, way, sub, step, live):
        line = self.line
        chip = line.chips - 1 - step if way == 0 else step
        arrived = self.from_below if way == 0 else self.from_above
        inner = line.has_below if way == 0 else line.has_above

        @pl.when(live & (chip > line.place if way == 0 else chip < line.place))
        def _():
            self.load(chip, sub).wait()
            self.across(chip, sub).wait_recv()

            def add(with_arrived):
                @pl.loop(0, line.sub_rows // ROW_TILE)
                def _(tile):
                    at = line.tile(sub, tile)
                    total = self.held[chip, at, :].astype(jnp.float32)
                    total = total + self.paired[chip, at, :].astype(jnp.float32)
                    if with_arrived:
                        total = total + arrived[chip, at, :].astype(jnp.float32)
                    self.held[chip, at, :] = total.astype(jnp.bfloat16)

            @pl.when(inner)
            def _():
                self.hop(way, chip, sub).wait_recv()
                add(True)

            pl.when(jnp.logical_not(inner))(lambda: add(False))
            self.hop(way, chip, sub).start()

    def arrive(self, sub):
        line = self.line
        place = line.place
        self.load(place, sub).wait()
        self.across(place, sub).wait_recv()
        pl.when(line.has_below)(lambda: self.hop(0, place, sub).wait_recv())
        pl.when(line.has_above)(lambda: self.hop(1, place, sub).wait_recv())

    def total(self, at):
        place = self.line.place
        total = self.held[place, at, :].astype(jnp.float32)
        total = total + self.paired[place, at, :].astype(jnp.float32)
        total = total + self.from_below[place, at, :].astype(jnp.float32)
        return total + self.from_above[place, at, :].astype(jnp.float32)

    def finish(self):
        line = self.line

        @pl.loop(0, SUBS)
        def _(sub):
            for chip in range(line.chips):
                self.across(chip, sub).wait_send()
                pl.when(chip > line.place)(lambda: self.hop(0, chip, sub).wait_send())
                pl.when(chip < line.place)(lambda: self.hop(1, chip, sub).wait_send())


def for_tiles(line, sub, body):
    @pl.loop(0, line.sub_rows // ROW_TILE)
    def _(tile):
        body(line.tile(sub, tile))


def run_gather(line, gather, rows_done):
    line.enter()
    steps = line.chips - 1

    @pl.loop(0, SUBS)
    def _(sub):
        for_tiles(line, sub, rows_done)
        gather.start(sub)

    @pl.loop(0, steps * SUBS)
    def _(at):
        gather.step(at % SUBS, at // SUBS, True)

    gather.finish()


def run_line(line, reduce, gather, rows_done):
    steps = line.chips - 1
    line.enter()
    reduce.start()
    slots = steps * SUBS + LAG + (steps if gather is not None else 0) + 1

    @pl.loop(0, slots)
    def _(slot):
        for way in range(2):
            at = slot - (line.place if way == 0 else steps - line.place)
            sub = jnp.maximum(at, 0) // steps
            reduce.step(way, jnp.minimum(sub, SUBS - 1), jnp.maximum(at, 0) % steps, (at >= 0) & (sub < SUBS))
        at = slot - steps - LAG
        sub = jnp.maximum(at, 0) // steps

        @pl.when((at >= 0) & (at % steps == 0) & (sub < SUBS))
        def _():
            reduce.arrive(sub)
            for_tiles(line, sub, rows_done)
            if gather is not None:
                gather.start(sub)

        if gather is not None:
            at = slot - steps - LAG - 1
            sub = jnp.maximum(at, 0) // steps
            gather.step(
                jnp.minimum(sub, SUBS - 1), jnp.maximum(at, 0) % steps, (at >= 0) & (sub < SUBS)
            )

    reduce.finish()
    if gather is not None:
        gather.finish()


def unit_of(rows):
    centre = jnp.mean(rows, axis=1, keepdims=True)
    centred = rows - centre
    inv_std = lax.rsqrt(jnp.mean(centred * centred, axis=1, keepdims=True) + EPSILON)
    return centred * inv_std, inv_std


def norm_back(grad, unit, inv_std, gain):
    scaled = grad * gain
    return inv_std * (
        scaled
        - jnp.mean(scaled, axis=1, keepdims=True)
        - unit * jnp.mean(scaled * unit, axis=1, keepdims=True)
    )


def fold(rows):
    return jnp.sum(rows.reshape(-1, 8, rows.shape[1]), axis=0)


def norm_gather_kernel(chips, input_ref, gain_ref, shift_ref, whole_ref, normed_ref, *sems):
    line = Line(chips, input_ref.shape[0])
    gather = Gather(line, normed_ref, whole_ref, sems)

    def rows_done(at):
        unit, _ = unit_of(input_ref[at, :].astype(jnp.float32))
        normed_ref[at, :] = (unit * gain_ref[...] + shift_ref[...]).astype(jnp.bfloat16)

    run_gather(line, gather, rows_done)


def branch_norm_gather_kernel(
    chips, partial_ref, input_ref, bias_ref, gain_ref, shift_ref, whole_ref, residual_ref, normed_ref, *rest
):
    line = Line(chips, input_ref.shape[0])
    reduce = Reduce(line, partial_ref, rest[:4], rest[4:9])
    gather = Gather(line, normed_ref, whole_ref, rest[9:])

    def rows_done(at):
        residual = input_ref[at, :].astype(jnp.float32) + (reduce.total(at) + bias_ref[...])
        residual_ref[at, :] = residual
        unit, _ = unit_of(residual)
        normed_ref[at, :] = (unit * gain_ref[...] + shift_ref[...]).astype(jnp.bfloat16)

    run_line(line, reduce, gather, rows_done)


def grad_gather_kernel(
    chips, partial_ref, residual_ref, grad_ref, gain_ref, whole_ref, residual_grad_ref, sums_ref, branch_ref, *rest
):
    line = Line(chips, grad_ref.shape[0])
    reduce = Reduce(line, partial_ref, rest[:4], rest[4:9])
    gather = Gather(line, branch_ref, whole_ref, rest[9:])
    sums_ref[...] = jnp.zeros_like(sums_ref)

    def rows_done(at):
        unit, inv_std = unit_of(residual_ref[at, :])
        grad = reduce.total(at)
        out_grad = grad_ref[at, :].astype(jnp.float32)
        residual_grad = out_grad + norm_back(grad, unit, inv_std, gain_ref[...])
        residual_grad_ref[at, :] = residual_grad
        branch = residual_grad.astype(jnp.bfloat16)
        branch_ref[at, :] = branch
        sums_ref[0] += fold(grad * unit)
        sums_ref[1] += fold(grad)
        sums_ref[2] += fold(branch.astype(jnp.float32))
        sums_ref[3] += fold(out_grad)

    run_line(line, reduce, gather, rows_done)


def grad_kernel(chips, partial_ref, input_ref, residual_grad_ref, gain_ref, out_ref, sums_ref, *rest):
    line = Line(chips, input_ref.shape[0])
    reduce = Reduce(line, partial_ref, rest[:4], rest[4:9])
    sums_ref[...] = jnp.zeros_like(sums_ref)

    def rows_done(at):
        unit, inv_std = unit_of(input_ref[at, :].astype(jnp.float32))
        grad = reduce.total(at)
        out_ref[at, :] = residual_grad_ref[at, :] + norm_back(grad, unit, inv_std, gain_ref[...])
        sums_ref[0] += fold(grad * unit)
        sums_ref[1] += fold(grad)

    run_line(line, reduce, None, rows_done)


def line_call(kernel, collective_id, operands, outs, gathers, reduces, rows, width):
    chips = lax.axis_size("tensor") // 2
    whole = jax.ShapeDtypeStruct((2 * chips, rows, width), jnp.bfloat16)
    in_vmem = pl.BlockSpec(memory_space=pltpu.VMEM)
    in_place = pl.BlockSpec(memory_space=pl.ANY)
    scratch = []
    if gathers:
        scratch.append(pltpu.VMEM((rows, width), jnp.bfloat16))
    if reduces:
        scratch += Reduce.scratch(chips, rows, width)
    if gathers:
        scratch += Gather.scratch(chips)
    return pl.pallas_call(
        functools.partial(kernel, chips),
        in_specs=([in_place] if reduces else []) + [in_vmem] * (len(operands) - int(reduces)),
        out_specs=([in_place] if gathers else []) + [in_vmem] * len(outs),
        out_shape=([whole] if gathers else []) + list(outs),
        scratch_shapes=scratch,
        compiler_params=pltpu.CompilerParams(
            collective_id=collective_id, has_side_effects=True, vmem_limit_bytes=48 * 2**20
        ),
        cost_estimate=pl.CostEstimate(
            flops=8 * rows * width * 100, bytes_accessed=100 * rows * width, transcendentals=0
        ),
    )(*operands)


def total_kernel(ranks, groups, late_ref, early_ref, own_ref, all_ref, dp_ref, mine, first, stage, second, sems):
    send1, recv1, send2, recv2, send3, recv3 = sems
    me = lax.axis_index("tensor")
    group = lax.axis_index("dp")
    part = mine.shape[1] // ranks
    barrier = pltpu.get_barrier_semaphore()
    for step in range(1, ranks):
        pl.semaphore_signal(
            barrier, inc=1, device_id={"tensor": lax.rem(me + step, ranks)}, device_id_type=MESH
        )
    for step in range(1, groups):
        pl.semaphore_signal(
            barrier, inc=1, device_id={"dp": lax.rem(group + step, groups)}, device_id_type=MESH
        )
    mine[...] = jnp.zeros_like(mine)
    for row in range(late_ref.shape[0]):
        mine[row : row + 1, :] = jnp.sum(late_ref[row], axis=0, keepdims=True)
    for row in range(early_ref.shape[0]):
        at = late_ref.shape[0] + row
        mine[at : at + 1, :] = jnp.sum(early_ref[row], axis=0, keepdims=True)
    pl.semaphore_wait(barrier, ranks + groups - 2)

    def columns(rank):
        return pl.ds(pl.multiple_of(rank * part, part), part)

    def scatter(peer, slot, sem):
        return pltpu.make_async_remote_copy(
            src_ref=mine.at[:, columns(peer)],
            dst_ref=first.at[slot],
            send_sem=send1.at[sem],
            recv_sem=recv1.at[slot],
            device_id={"tensor": peer},
            device_id_type=MESH,
        )

    def exchange(peer, slot, sem):
        return pltpu.make_async_remote_copy(
            src_ref=stage,
            dst_ref=second.at[slot],
            send_sem=send2.at[sem],
            recv_sem=recv2.at[slot],
            device_id={"dp": peer},
            device_id_type=MESH,
        )

    def spread(peer, rank, sem):
        return pltpu.make_async_remote_copy(
            src_ref=all_ref.at[:, columns(me)],
            dst_ref=all_ref.at[:, columns(rank)],
            send_sem=send3.at[sem],
            recv_sem=recv3.at[rank],
            device_id={"tensor": peer},
            device_id_type=MESH,
        )

    for step in range(1, ranks):
        scatter(lax.rem(me + step, ranks), me, step).start()
    first[me] = mine[:, columns(me)]
    for step in range(1, ranks):
        other = lax.rem(me + step, ranks)
        scatter(other, other, step).wait_recv()
    rows = mine.shape[0]
    total = first[0]
    for rank in range(1, ranks):
        total = total + first[rank]
    stage[:rows, :] = total
    stage[rows:, :] = own_ref[...]
    for step in range(1, groups):
        exchange(lax.rem(group + step, groups), group, step).start()
    second[group] = stage[...]
    for step in range(1, groups):
        other = lax.rem(group + step, groups)
        exchange(other, other, step).wait_recv()
    total = second[0]
    for index in range(1, groups):
        total = total + second[index]
    all_ref[:, columns(me)] = total[:rows]
    dp_ref[...] = total[rows:]
    for step in range(1, ranks):
        spread(lax.rem(me + step, ranks), me, step).start()
    for step in range(1, ranks):
        other = lax.rem(me + step, ranks)
        spread(other, other, step).wait_recv()
    for step in range(1, ranks):
        other = lax.rem(me + step, ranks)
        scatter(other, me, step).wait_send()
        spread(other, me, step).wait_send()
    for step in range(1, groups):
        exchange(lax.rem(group + step, groups), group, step).wait_send()


def total_call(late, early, own):
    ranks = lax.axis_size("tensor")
    groups = lax.axis_size("dp")
    width = late.shape[2]
    part = width // ranks
    dma = pltpu.SemaphoreType.DMA

    def kernel(late_ref, early_ref, own_ref, all_ref, dp_ref, mine, first, stage, second, *sems):
        total_kernel(
            ranks, groups, late_ref, early_ref, own_ref, all_ref, dp_ref, mine, first, stage, second, sems
        )

    in_vmem = pl.BlockSpec(memory_space=pltpu.VMEM)
    return pl.pallas_call(
        kernel,
        in_specs=[in_vmem] * 3,
        out_specs=[in_vmem] * 2,
        out_shape=[
            jax.ShapeDtypeStruct((8, width), jnp.float32),
            jax.ShapeDtypeStruct((8, part), jnp.float32),
        ],
        scratch_shapes=[
            pltpu.VMEM((8, width), jnp.float32),
            pltpu.VMEM((ranks, 8, part), jnp.float32),
            pltpu.VMEM((16, part), jnp.float32),
            pltpu.VMEM((groups, 16, part), jnp.float32),
            dma((ranks,)),
            dma((ranks,)),
            dma((groups,)),
            dma((groups,)),
            dma((ranks,)),
            dma((ranks,)),
        ],
        compiler_params=pltpu.CompilerParams(collective_id=5, has_side_effects=True),
        name="total_sums",
    )(late, early, own)


def over_dp(grad, dimension):
    return lax.psum_scatter(grad, "dp", scatter_dimension=dimension, tiled=True).astype(jnp.float32)


def layer(
    layer_input,
    segment_ids,
    first_gain,
    first_shift,
    qkv_weight,
    query_value_bias,
    dense_weight,
    dense_bias,
    second_gain,
    second_shift,
    up_weight,
    up_bias,
    down_weight,
    down_bias,
    out_grad,
):
    rows, width = layer_input.shape
    ranks = lax.axis_size("tensor")
    tokens = ranks * rows
    f32_rows = jax.ShapeDtypeStruct((rows, width), jnp.float32)

    qkv_full = lax.all_gather(qkv_weight, "dp", axis=1, tiled=True)
    dense_full = lax.all_gather(dense_weight, "dp", axis=1, tiled=True)
    up_full = lax.all_gather(up_weight, "dp", axis=0, tiled=True)
    down_full = lax.all_gather(down_weight, "dp", axis=1, tiled=True)
    out_whole = lax.all_gather(out_grad, "tensor", axis=0, tiled=True)

    head_width = qkv_full.shape[2]
    up_width = up_bias.shape[0]
    qkv_cat = jnp.transpose(qkv_full, (1, 0, 2)).reshape(width, 3 * head_width)

    (whole1,) = line_call(
        norm_gather_kernel, 1,
        (layer_input, first_gain[None], first_shift[None]), (), True, False, rows, width,
    )
    whole1 = whole1.reshape(tokens, width)
    zero_bias = jnp.zeros_like(query_value_bias[0])
    bias_cat = jnp.concatenate([query_value_bias[0], zero_bias, query_value_bias[1]])
    projected = (jnp.dot(whole1, qkv_cat, preferred_element_type=jnp.float32) + bias_cat).astype(
        jnp.bfloat16
    )
    head_count = head_width // HEAD_DIM
    tensor_pos = lax.axis_index("tensor")
    global_heads = tensor_pos * head_count + jnp.arange(head_count, dtype=jnp.int32)
    slopes = jnp.power(2.0, -8.0 * (global_heads + 1).astype(jnp.float32) / HEADS)
    attended, log_sums = attention_forward(projected, segment_ids, slopes)
    attn_part = jnp.dot(attended, dense_full, preferred_element_type=jnp.float32).astype(jnp.bfloat16)
    whole2, residual = line_call(
        branch_norm_gather_kernel, 2,
        (attn_part.reshape(ranks, rows, width), layer_input, dense_bias[None], second_gain[None], second_shift[None]),
        (f32_rows,), True, True, rows, width,
    )
    whole2 = whole2.reshape(tokens, width)
    pre_act = jnp.dot(whole2, up_full, preferred_element_type=jnp.float32) + up_bias
    activated = jax.nn.gelu(pre_act, approximate=False).astype(jnp.bfloat16)
    mlp_part = jnp.dot(activated, down_full, preferred_element_type=jnp.float32).astype(jnp.bfloat16)
    act_grad = lax.dot_general(
        out_whole, down_full, (((1,), (1,)), ((), ())), preferred_element_type=jnp.float32
    )
    _, gelu_back = jax.vjp(functools.partial(jax.nn.gelu, approximate=False), pre_act)
    pre_grad = gelu_back(act_grad)[0].astype(jnp.bfloat16)
    up_bias_part = jnp.sum(pre_grad.astype(jnp.float32), axis=0)
    down_grad = lax.dot_general(
        activated, out_whole, (((0,), (0,)), ((), ())), preferred_element_type=jnp.float32
    ).astype(jnp.bfloat16)
    up_grad = lax.dot_general(
        whole2, pre_grad, (((0,), (0,)), ((), ())), preferred_element_type=jnp.float32
    ).astype(jnp.bfloat16)
    pre_grad, down_grad, up_grad, mlp_part = lax.optimization_barrier(
        (pre_grad, down_grad, up_grad, mlp_part)
    )
    down_wgrad = over_dp(down_grad, 1)
    up_wgrad = over_dp(up_grad, 0)
    normed2_part = lax.dot_general(
        pre_grad, up_full, (((1,), (1,)), ((), ())), preferred_element_type=jnp.float32
    ).astype(jnp.bfloat16)
    mlp_rows = lax.psum_scatter(mlp_part, "tensor", scatter_dimension=0, tiled=True)
    mlp_branch = mlp_rows.astype(jnp.float32) + down_bias
    layer_out = (residual + mlp_branch).astype(jnp.bfloat16)

    branch_whole, residual_grad, second_sums = line_call(
        grad_gather_kernel, 3,
        (normed2_part.reshape(ranks, rows, width), residual, out_grad, second_gain[None]),
        (f32_rows, jax.ShapeDtypeStruct((4, 8, width), jnp.float32)), True, True, rows, width,
    )
    branch_whole = branch_whole.reshape(tokens, width)
    attended_grad = lax.dot_general(
        branch_whole, dense_full, (((1,), (1,)), ((), ())), preferred_element_type=jnp.float32
    ).astype(jnp.bfloat16)
    dense_grad = lax.dot_general(
        attended, branch_whole, (((0,), (0,)), ((), ())), preferred_element_type=jnp.float32
    ).astype(jnp.bfloat16)
    attended_grad, dense_grad = lax.optimization_barrier((attended_grad, dense_grad))
    qkv_grad_cat = attention_backward(projected, attended_grad, segment_ids, slopes, log_sums)
    dense_wgrad = over_dp(dense_grad, 1)
    qkv_sums = jnp.sum(qkv_grad_cat.astype(jnp.float32), axis=0)
    bias_part = jnp.stack([qkv_sums[:head_width], qkv_sums[2 * head_width :]])
    qkv_grad_flat = lax.dot_general(
        whole1, qkv_grad_cat, (((0,), (0,)), ((), ())), preferred_element_type=jnp.float32
    )
    qkv_grad = jnp.transpose(
        qkv_grad_flat.astype(jnp.bfloat16).reshape(width, 3, head_width), (1, 0, 2)
    )
    qkv_grad, qkv_grad_cat = lax.optimization_barrier((qkv_grad, qkv_grad_cat))
    qkv_wgrad = over_dp(qkv_grad, 1)
    normed1_part = lax.dot_general(
        qkv_grad_cat, qkv_cat, (((1,), (1,)), ((), ())), preferred_element_type=jnp.float32
    ).astype(jnp.bfloat16)
    input_grad, first_sums = line_call(
        grad_kernel, 4,
        (normed1_part.reshape(ranks, rows, width), layer_input, residual_grad, first_gain[None]),
        (f32_rows, jax.ShapeDtypeStruct((2, 8, width), jnp.float32)), False, True, rows, width,
    )
    part = width // ranks
    own = jnp.concatenate([bias_part.reshape(-1), up_bias_part]).reshape(-1, part)
    bias_rows = 2 * head_width // part
    own = jnp.pad(own, ((0, 8 - own.shape[0]), (0, 0)))
    sums, own = total_call(first_sums, second_sums, own)
    up_rows = up_width // part
    return (
        layer_out,
        input_grad,
        sums[0],
        sums[1],
        qkv_wgrad,
        own[:bias_rows].reshape(2, head_width),
        dense_wgrad,
        sums[4],
        sums[2],
        sums[3],
        up_wgrad,
        own[bias_rows : bias_rows + up_rows].reshape(up_width),
        down_wgrad,
        sums[5],
    )


def solution(mesh):
    token_rows = P(("dp", "tensor"), None)
    placed = (
        token_rows,
        P("dp"),
        P(),
        P(),
        P(None, "dp", "tensor"),
        P(None, "tensor"),
        P("tensor", "dp"),
        P(),
        P(),
        P(),
        P("dp", "tensor"),
        P("tensor"),
        P("tensor", "dp"),
        P(),
        token_rows,
    )
    return jax.shard_map(
        layer,
        mesh=mesh,
        in_specs=placed,
        out_specs=(
            token_rows,
            token_rows,
            P(),
            P(),
            P(None, "dp", "tensor"),
            P(None, "tensor"),
            P("tensor", "dp"),
            P(),
            P(),
            P(),
            P("dp", "tensor"),
            P("tensor"),
            P("tensor", "dp"),
            P(),
        ),
        check_vma=False,
    )
```

```python
import functools
import math

import jax
import jax.numpy as jnp
from jax import lax
from jax.experimental import pallas as pl
from jax.experimental.pallas import tpu as pltpu
from jax.sharding import PartitionSpec as P


HEADS = 32
EPSILON = 1e-05
MESH = pl.DeviceIdType.MESH
HEAD_DIM = 64
PAIR = 2 * HEAD_DIM
Q_BLOCK = 256
MASKED = -1e32
NT = (((1,), (1,)), ((), ()))
NN = (((1,), (0,)), ((), ()))


def key_window(seq_len, block):
    width = min(seq_len, Q_BLOCK + seq_len // 4)
    start = jnp.maximum(block * Q_BLOCK + Q_BLOCK - width, 0)
    return width, pl.multiple_of(start, 128)


def masked_distance(seg_row, seg_col, first_query, first_key, width):
    shape = (width, Q_BLOCK)
    key_pos = lax.broadcasted_iota(jnp.int32, shape, 0) + first_key
    query_pos = lax.broadcasted_iota(jnp.int32, shape, 1) + first_query
    delta = key_pos - query_pos
    allowed = (seg_col == seg_row) & (delta <= 0)
    return jnp.where(allowed, delta.astype(jnp.float32), MASKED)


def half_lanes(rows, half):
    lane = lax.broadcasted_iota(jnp.int32, rows.shape, 1)
    return jnp.where((lane < HEAD_DIM) == (half == 0), rows, jnp.zeros_like(rows))


def forward_kernel(slope_ref, proj_ref, seg_row_ref, seg_col_ref, out_ref, lse_ref, value_t, bias_ref):
    seq_len = proj_ref.shape[0]
    width_all = out_ref.shape[1]
    block = pl.program_id(0)

    @pl.when(block == 0)
    def _():
        value_t[...] = proj_ref[:, 2 * width_all :].T

    first = pl.multiple_of(block * Q_BLOCK, Q_BLOCK)
    width, start = key_window(seq_len, block)
    queries = pl.ds(first, Q_BLOCK)
    keys = pl.ds(start, width)
    bias_ref[...] = masked_distance(
        seg_row_ref[:, queries], seg_col_ref[keys, :], first, start, width
    )
    for pair in range(width_all // PAIR):
        cols = pair * PAIR
        query_pair = proj_ref[queries, cols : cols + PAIR] * 0.125
        key_pair = proj_ref[keys, width_all + cols : width_all + cols + PAIR]
        value_pair = value_t[cols : cols + PAIR, keys]
        mixed = []
        for half in range(2):
            head = 2 * pair + half
            scores = lax.dot_general(
                key_pair, half_lanes(query_pair, half), NT, preferred_element_type=jnp.float32
            )
            scores = scores + slope_ref[head] * bias_ref[...]
            highest = jnp.max(scores, axis=0, keepdims=True)
            exponent = jnp.exp(scores - highest)
            total = jnp.sum(exponent, axis=0, keepdims=True)
            part = lax.dot_general(
                value_pair[half * HEAD_DIM : (half + 1) * HEAD_DIM],
                exponent.astype(jnp.bfloat16),
                NN,
                preferred_element_type=jnp.float32,
            )
            mixed.append(part / total)
            lse_ref[head : head + 1, :] = highest + jnp.log(total)
        out_ref[:, cols : cols + PAIR] = jnp.concatenate(mixed, axis=0).T.astype(jnp.bfloat16)


def attention_forward(projected, segments, slopes):
    seq_len, all_cols = projected.shape
    cols = all_cols // 3
    heads = cols // HEAD_DIM
    width = min(seq_len, Q_BLOCK + seq_len // 4)
    return pl.pallas_call(
        forward_kernel,
        grid=(seq_len // Q_BLOCK,),
        in_specs=[
            pl.BlockSpec(memory_space=pltpu.SMEM),
            pl.BlockSpec((seq_len, all_cols), lambda i: (0, 0)),
            pl.BlockSpec((1, seq_len), lambda i: (0, 0)),
            pl.BlockSpec((seq_len, 1), lambda i: (0, 0)),
        ],
        out_specs=[
            pl.BlockSpec((Q_BLOCK, cols), lambda i: (i, 0)),
            pl.BlockSpec((heads, Q_BLOCK), lambda i: (0, i)),
        ],
        out_shape=[
            jax.ShapeDtypeStruct((seq_len, cols), jnp.bfloat16),
            jax.ShapeDtypeStruct((heads, seq_len), jnp.float32),
        ],
        scratch_shapes=[
            pltpu.VMEM((cols, seq_len), jnp.bfloat16),
            pltpu.VMEM((width, Q_BLOCK), jnp.float32),
        ],
        compiler_params=pltpu.CompilerParams(vmem_limit_bytes=40 * 2**20),
        cost_estimate=pl.CostEstimate(flops=4 * seq_len * width * cols, bytes_accessed=6 * seq_len * cols, transcendentals=0),
        name="attention_forward",
    )(slopes, projected, segments[None, :], segments[:, None])


def backward_kernel(slope_ref, proj_ref, grad_ref, lse_ref, seg_row_ref, seg_col_ref, out_ref,
                    key_t, bias_ref, key_sum, value_sum):
    seq_len = proj_ref.shape[0]
    width_all = grad_ref.shape[1]
    block = pl.program_id(0)

    @pl.when(block == 0)
    def _():
        key_t[...] = proj_ref[:, width_all : 2 * width_all].T
        key_sum[...] = jnp.zeros_like(key_sum)
        value_sum[...] = jnp.zeros_like(value_sum)

    first = pl.multiple_of(block * Q_BLOCK, Q_BLOCK)
    width, start = key_window(seq_len, block)
    queries = pl.ds(first, Q_BLOCK)
    keys = pl.ds(start, width)
    bias_ref[...] = masked_distance(
        seg_row_ref[:, queries], seg_col_ref[keys, :], first, start, width
    )
    for pair in range(width_all // PAIR):
        cols = pair * PAIR
        query_pair = proj_ref[queries, cols : cols + PAIR] * 0.125
        key_pair = proj_ref[keys, width_all + cols : width_all + cols + PAIR]
        value_pair = proj_ref[keys, 2 * width_all + cols : 2 * width_all + cols + PAIR]
        grad_pair = grad_ref[queries, cols : cols + PAIR]
        query_grads = []
        key_part = value_part = None
        for half in range(2):
            head = 2 * pair + half
            query_half = half_lanes(query_pair, half)
            grad_half = half_lanes(grad_pair, half)
            scores = lax.dot_general(key_pair, query_half, NT, preferred_element_type=jnp.float32)
            probs = jnp.exp(scores + slope_ref[head] * bias_ref[...] - lse_ref[head : head + 1, queries])
            prob_grad = lax.dot_general(value_pair, grad_half, NT, preferred_element_type=jnp.float32)
            inner = jnp.sum(probs * prob_grad, axis=0, keepdims=True)
            score_grad = (probs * (prob_grad - inner)).astype(jnp.bfloat16)
            value_half = jnp.dot(probs.astype(jnp.bfloat16), grad_half, preferred_element_type=jnp.float32)
            key_half = jnp.dot(score_grad, query_half, preferred_element_type=jnp.float32)
            query_grads.append(
                jnp.dot(
                    key_t[cols + half * HEAD_DIM : cols + (half + 1) * HEAD_DIM, keys],
                    score_grad,
                    preferred_element_type=jnp.float32,
                )
                * 0.125
            )
            value_part = value_half if half == 0 else value_part + value_half
            key_part = key_half if half == 0 else key_part + key_half
        key_sum[keys, cols : cols + PAIR] += key_part
        value_sum[keys, cols : cols + PAIR] += value_part
        out_ref[queries, cols : cols + PAIR] = (
            jnp.concatenate(query_grads, axis=0).T.astype(jnp.bfloat16)
        )

    @pl.when(block == pl.num_programs(0) - 1)
    def _():
        out_ref[:, width_all : 2 * width_all] = key_sum[...].astype(jnp.bfloat16)
        out_ref[:, 2 * width_all :] = value_sum[...].astype(jnp.bfloat16)


def attention_backward(projected, head_grad, segments, slopes, log_sums):
    seq_len, all_cols = projected.shape
    cols = all_cols // 3
    heads = cols // HEAD_DIM
    width = min(seq_len, Q_BLOCK + seq_len // 4)
    return pl.pallas_call(
        backward_kernel,
        grid=(seq_len // Q_BLOCK,),
        in_specs=[
            pl.BlockSpec(memory_space=pltpu.SMEM),
            pl.BlockSpec((seq_len, all_cols), lambda i: (0, 0)),
            pl.BlockSpec((seq_len, cols), lambda i: (0, 0)),
            pl.BlockSpec((heads, seq_len), lambda i: (0, 0)),
            pl.BlockSpec((1, seq_len), lambda i: (0, 0)),
            pl.BlockSpec((seq_len, 1), lambda i: (0, 0)),
        ],
        out_specs=pl.BlockSpec((seq_len, all_cols), lambda i: (0, 0)),
        out_shape=jax.ShapeDtypeStruct((seq_len, all_cols), jnp.bfloat16),
        scratch_shapes=[
            pltpu.VMEM((cols, seq_len), jnp.bfloat16),
            pltpu.VMEM((width, Q_BLOCK), jnp.float32),
            pltpu.VMEM((seq_len, cols), jnp.float32),
            pltpu.VMEM((seq_len, cols), jnp.float32),
        ],
        compiler_params=pltpu.CompilerParams(vmem_limit_bytes=48 * 2**20),
        cost_estimate=pl.CostEstimate(flops=10 * seq_len * width * cols, bytes_accessed=14 * seq_len * cols, transcendentals=0),
        name="attention_backward",
    )(slopes, projected, head_grad, log_sums, segments[None, :], segments[:, None])


ROW_TILE = 16
SUBS = 4
LAG = 0


def remote(src, dst, send_sem, recv_sem, peer):
    return pltpu.make_async_remote_copy(
        src_ref=src,
        dst_ref=dst,
        send_sem=send_sem,
        recv_sem=recv_sem,
        device_id={"tensor": peer},
        device_id_type=MESH,
    )


class Line:
    def __init__(self, chips, rows):
        self.chips = chips
        self.sub_rows = rows // SUBS
        self.me = lax.axis_index("tensor")
        self.place = self.me // 2
        self.core = self.me % 2
        self.above = self.me + 2
        self.below = self.me - 2
        self.partner = self.me + 1 - 2 * self.core
        self.has_above = self.place < chips - 1
        self.has_below = self.place > 0

    def rows(self, sub):
        return pl.ds(pl.multiple_of(sub * self.sub_rows, self.sub_rows), self.sub_rows)

    def tile(self, sub, tile):
        return pl.ds(pl.multiple_of(sub * self.sub_rows + tile * ROW_TILE, ROW_TILE), ROW_TILE)

    def enter(self):
        barrier = pltpu.get_barrier_semaphore()

        def greet(peer):
            pl.semaphore_signal(barrier, inc=1, device_id={"tensor": peer}, device_id_type=MESH)

        pl.when(self.has_above)(lambda: greet(self.above))
        pl.when(self.has_below)(lambda: greet(self.below))
        greet(self.partner)
        pl.semaphore_wait(
            barrier, 1 + self.has_above.astype(jnp.int32) + self.has_below.astype(jnp.int32)
        )


class Gather:
    def __init__(self, line, source, target, sems):
        self.line, self.source, self.target = line, source, target
        self.own_sem, self.line_send, self.line_recv, self.pair_send, self.pair_recv = sems

    @staticmethod
    def scratch(chips):
        dma = pltpu.SemaphoreType.DMA
        return [
            dma((SUBS,)),
            dma((2, chips, SUBS)),
            dma((2, chips, SUBS)),
            dma((chips, SUBS)),
            dma((chips, SUBS)),
        ]

    def hop(self, way, step, sub, src, block):
        peer = self.line.above if way == 0 else self.line.below
        return remote(
            src,
            self.target.at[block, self.line.rows(sub)],
            self.line_send.at[way, step, sub],
            self.line_recv.at[way, step, sub],
            peer,
        )

    def across(self, chip, sub, src, block):
        return remote(
            src,
            self.target.at[block, self.line.rows(sub)],
            self.pair_send.at[chip, sub],
            self.pair_recv.at[chip, sub],
            self.line.partner,
        )

    def own(self, sub):
        return pltpu.make_async_copy(
            self.source.at[self.line.rows(sub)],
            self.target.at[self.line.me, self.line.rows(sub)],
            self.own_sem.at[sub],
        )

    def start(self, sub):
        line = self.line
        src = self.source.at[line.rows(sub)]
        pl.when(line.has_above)(lambda: self.hop(0, 0, sub, src, line.me).start())
        pl.when(line.has_below)(lambda: self.hop(1, 0, sub, src, line.me).start())
        self.across(line.place, sub, src, line.me).start()
        self.own(sub).start()

    def step(self, sub, step, live):
        line = self.line
        for way, sign in ((0, -1), (1, 1)):
            block = line.me + 2 * sign * (step + 1)
            onward = line.has_above if way == 0 else line.has_below
            inside = block >= 0 if way == 0 else block < 2 * line.chips

            @pl.when(live & inside)
            def _():
                src = self.target.at[block, line.rows(sub)]
                self.hop(way, step, sub, src, block).wait_recv()

                @pl.when(onward)
                def _():
                    self.hop(way, step + 1, sub, src, block).start()

                self.across(block // 2, sub, src, block).start()

    def finish(self):
        line = self.line

        @pl.loop(0, SUBS)
        def _(sub):
            src = self.source.at[line.rows(sub)]
            for chip in range(line.chips):
                copy = self.across(chip, sub, src, 2 * chip + 1 - line.core)
                copy.wait_recv()
                copy.wait_send()
            for step in range(line.chips - 1):
                sent_up = line.has_above & (line.place >= step)
                sent_down = line.has_below & (line.place + step < line.chips)
                pl.when(sent_up)(lambda: self.hop(0, step, sub, src, line.me).wait_send())
                pl.when(sent_down)(lambda: self.hop(1, step, sub, src, line.me).wait_send())
            self.own(sub).wait()


class Reduce:
    def __init__(self, line, partial, bufs, sems):
        self.line, self.partial = line, partial
        self.held, self.paired, self.from_below, self.from_above = bufs
        self.held_sem, self.pair_send, self.pair_recv, self.line_send, self.line_recv = sems

    @staticmethod
    def scratch(chips, rows, width):
        dma = pltpu.SemaphoreType.DMA
        return [pltpu.VMEM((chips, rows, width), jnp.bfloat16)] * 4 + [
            dma((chips, SUBS)),
            dma((chips, SUBS)),
            dma((chips, SUBS)),
            dma((2, chips, SUBS)),
            dma((2, chips, SUBS)),
        ]

    def load(self, chip, sub):
        rows = self.line.rows(sub)
        return pltpu.make_async_copy(
            self.partial.at[2 * chip + self.line.core, rows],
            self.held.at[chip, rows],
            self.held_sem.at[chip, sub],
        )

    def across(self, chip, sub):
        rows = self.line.rows(sub)
        return remote(
            self.partial.at[2 * chip + 1 - self.line.core, rows],
            self.paired.at[chip, rows],
            self.pair_send.at[chip, sub],
            self.pair_recv.at[chip, sub],
            self.line.partner,
        )

    def hop(self, way, chip, sub):
        rows = self.line.rows(sub)
        return remote(
            self.held.at[chip, rows],
            (self.from_below if way == 0 else self.from_above).at[chip, rows],
            self.line_send.at[way, chip, sub],
            self.line_recv.at[way, chip, sub],
            self.line.above if way == 0 else self.line.below,
        )

    def start(self):
        line = self.line
        order = []
        for step in range(line.chips):
            chip = line.chips - 1 - step // 2 if step % 2 == 0 else step // 2
            order.append(chip)

        @pl.loop(0, SUBS)
        def _(sub):
            for chip in order:
                self.across(chip, sub).start()
                self.load(chip, sub).start()

        zeros = jnp.zeros((ROW_TILE, self.held.shape[2]), jnp.bfloat16)

        def clear(buf, chip):
            @pl.loop(0, self.held.shape[1] // ROW_TILE)
            def _(tile):
                buf[chip, pl.ds(pl.multiple_of(tile * ROW_TILE, ROW_TILE), ROW_TILE), :] = zeros

        pl.when(jnp.logical_not(line.has_below))(lambda: clear(self.from_below, 0))
        pl.when(jnp.logical_not(line.has_above))(lambda: clear(self.from_above, line.chips - 1))

    def step(self, way, sub, step, live):
        line = self.line
        chip = line.chips - 1 - step if way == 0 else step
        arrived = self.from_below if way == 0 else self.from_above
        inner = line.has_below if way == 0 else line.has_above

        @pl.when(live & (chip > line.place if way == 0 else chip < line.place))
        def _():
            self.load(chip, sub).wait()
            self.across(chip, sub).wait_recv()

            def add(with_arrived):
                @pl.loop(0, line.sub_rows // ROW_TILE)
                def _(tile):
                    at = line.tile(sub, tile)
                    total = self.held[chip, at, :].astype(jnp.float32)
                    total = total + self.paired[chip, at, :].astype(jnp.float32)
                    if with_arrived:
                        total = total + arrived[chip, at, :].astype(jnp.float32)
                    self.held[chip, at, :] = total.astype(jnp.bfloat16)

            @pl.when(inner)
            def _():
                self.hop(way, chip, sub).wait_recv()
                add(True)

            pl.when(jnp.logical_not(inner))(lambda: add(False))
            self.hop(way, chip, sub).start()

    def arrive(self, sub):
        line = self.line
        place = line.place
        self.load(place, sub).wait()
        self.across(place, sub).wait_recv()
        pl.when(line.has_below)(lambda: self.hop(0, place, sub).wait_recv())
        pl.when(line.has_above)(lambda: self.hop(1, place, sub).wait_recv())

    def total(self, at):
        place = self.line.place
        total = self.held[place, at, :].astype(jnp.float32)
        total = total + self.paired[place, at, :].astype(jnp.float32)
        total = total + self.from_below[place, at, :].astype(jnp.float32)
        return total + self.from_above[place, at, :].astype(jnp.float32)

    def finish(self):
        line = self.line

        @pl.loop(0, SUBS)
        def _(sub):
            for chip in range(line.chips):
                self.across(chip, sub).wait_send()
                pl.when(chip > line.place)(lambda: self.hop(0, chip, sub).wait_send())
                pl.when(chip < line.place)(lambda: self.hop(1, chip, sub).wait_send())


def for_tiles(line, sub, body):
    @pl.loop(0, line.sub_rows // ROW_TILE)
    def _(tile):
        body(line.tile(sub, tile))


def run_gather(line, gather, rows_done):
    line.enter()
    steps = line.chips - 1

    @pl.loop(0, SUBS)
    def _(sub):
        for_tiles(line, sub, rows_done)
        gather.start(sub)

    @pl.loop(0, steps * SUBS)
    def _(at):
        gather.step(at % SUBS, at // SUBS, True)

    gather.finish()


def run_line(line, reduce, gather, rows_done):
    steps = line.chips - 1
    line.enter()
    reduce.start()
    slots = steps * SUBS + LAG + (steps if gather is not None else 0) + 1

    @pl.loop(0, slots)
    def _(slot):
        for way in range(2):
            at = slot - (line.place if way == 0 else steps - line.place)
            sub = jnp.maximum(at, 0) // steps
            reduce.step(way, jnp.minimum(sub, SUBS - 1), jnp.maximum(at, 0) % steps, (at >= 0) & (sub < SUBS))
        at = slot - steps - LAG
        sub = jnp.maximum(at, 0) // steps

        @pl.when((at >= 0) & (at % steps == 0) & (sub < SUBS))
        def _():
            reduce.arrive(sub)
            for_tiles(line, sub, rows_done)
            if gather is not None:
                gather.start(sub)

        if gather is not None:
            at = slot - steps - LAG - 1
            sub = jnp.maximum(at, 0) // steps
            gather.step(
                jnp.minimum(sub, SUBS - 1), jnp.maximum(at, 0) % steps, (at >= 0) & (sub < SUBS)
            )

    reduce.finish()
    if gather is not None:
        gather.finish()


def unit_of(rows):
    centre = jnp.mean(rows, axis=1, keepdims=True)
    centred = rows - centre
    inv_std = lax.rsqrt(jnp.mean(centred * centred, axis=1, keepdims=True) + EPSILON)
    return centred * inv_std, inv_std


def norm_back(grad, unit, inv_std, gain):
    scaled = grad * gain
    return inv_std * (
        scaled
        - jnp.mean(scaled, axis=1, keepdims=True)
        - unit * jnp.mean(scaled * unit, axis=1, keepdims=True)
    )


def fold(rows):
    return jnp.sum(rows.reshape(-1, 8, rows.shape[1]), axis=0)


def norm_gather_kernel(chips, input_ref, gain_ref, shift_ref, whole_ref, normed_ref, *sems):
    line = Line(chips, input_ref.shape[0])
    gather = Gather(line, normed_ref, whole_ref, sems)

    def rows_done(at):
        unit, _ = unit_of(input_ref[at, :].astype(jnp.float32))
        normed_ref[at, :] = (unit * gain_ref[...] + shift_ref[...]).astype(jnp.bfloat16)

    run_gather(line, gather, rows_done)


def branch_norm_gather_kernel(
    chips, partial_ref, input_ref, bias_ref, gain_ref, shift_ref, whole_ref, residual_ref, normed_ref, *rest
):
    line = Line(chips, input_ref.shape[0])
    reduce = Reduce(line, partial_ref, rest[:4], rest[4:9])
    gather = Gather(line, normed_ref, whole_ref, rest[9:])

    def rows_done(at):
        residual = input_ref[at, :].astype(jnp.float32) + (reduce.total(at) + bias_ref[...])
        residual_ref[at, :] = residual
        unit, _ = unit_of(residual)
        normed_ref[at, :] = (unit * gain_ref[...] + shift_ref[...]).astype(jnp.bfloat16)

    run_line(line, reduce, gather, rows_done)


def grad_gather_kernel(
    chips, partial_ref, residual_ref, grad_ref, gain_ref, whole_ref, residual_grad_ref, sums_ref, branch_ref, *rest
):
    line = Line(chips, grad_ref.shape[0])
    reduce = Reduce(line, partial_ref, rest[:4], rest[4:9])
    gather = Gather(line, branch_ref, whole_ref, rest[9:])
    sums_ref[...] = jnp.zeros_like(sums_ref)

    def rows_done(at):
        unit, inv_std = unit_of(residual_ref[at, :])
        grad = reduce.total(at)
        out_grad = grad_ref[at, :].astype(jnp.float32)
        residual_grad = out_grad + norm_back(grad, unit, inv_std, gain_ref[...])
        residual_grad_ref[at, :] = residual_grad
        branch = residual_grad.astype(jnp.bfloat16)
        branch_ref[at, :] = branch
        sums_ref[0] += fold(grad * unit)
        sums_ref[1] += fold(grad)
        sums_ref[2] += fold(branch.astype(jnp.float32))
        sums_ref[3] += fold(out_grad)

    run_line(line, reduce, gather, rows_done)


def grad_kernel(chips, partial_ref, input_ref, residual_grad_ref, gain_ref, out_ref, sums_ref, *rest):
    line = Line(chips, input_ref.shape[0])
    reduce = Reduce(line, partial_ref, rest[:4], rest[4:9])
    sums_ref[...] = jnp.zeros_like(sums_ref)

    def rows_done(at):
        unit, inv_std = unit_of(input_ref[at, :].astype(jnp.float32))
        grad = reduce.total(at)
        out_ref[at, :] = residual_grad_ref[at, :] + norm_back(grad, unit, inv_std, gain_ref[...])
        sums_ref[0] += fold(grad * unit)
        sums_ref[1] += fold(grad)

    run_line(line, reduce, None, rows_done)


def line_call(kernel, collective_id, operands, outs, gathers, reduces, rows, width):
    chips = lax.axis_size("tensor") // 2
    whole = jax.ShapeDtypeStruct((2 * chips, rows, width), jnp.bfloat16)
    in_vmem = pl.BlockSpec(memory_space=pltpu.VMEM)
    in_place = pl.BlockSpec(memory_space=pl.ANY)
    scratch = []
    if gathers:
        scratch.append(pltpu.VMEM((rows, width), jnp.bfloat16))
    if reduces:
        scratch += Reduce.scratch(chips, rows, width)
    if gathers:
        scratch += Gather.scratch(chips)
    return pl.pallas_call(
        functools.partial(kernel, chips),
        in_specs=([in_place] if reduces else []) + [in_vmem] * (len(operands) - int(reduces)),
        out_specs=([in_place] if gathers else []) + [in_vmem] * len(outs),
        out_shape=([whole] if gathers else []) + list(outs),
        scratch_shapes=scratch,
        compiler_params=pltpu.CompilerParams(
            collective_id=collective_id, has_side_effects=True, vmem_limit_bytes=48 * 2**20
        ),
        cost_estimate=pl.CostEstimate(
            flops=8 * rows * width * 100, bytes_accessed=100 * rows * width, transcendentals=0
        ),
    )(*operands)


def total_kernel(ranks, groups, late_ref, early_ref, own_ref, all_ref, dp_ref, mine, first, stage, second, sems):
    send1, recv1, send2, recv2, send3, recv3 = sems
    me = lax.axis_index("tensor")
    group = lax.axis_index("dp")
    part = mine.shape[1] // ranks
    barrier = pltpu.get_barrier_semaphore()
    for step in range(1, ranks):
        pl.semaphore_signal(
            barrier, inc=1, device_id={"tensor": lax.rem(me + step, ranks)}, device_id_type=MESH
        )
    for step in range(1, groups):
        pl.semaphore_signal(
            barrier, inc=1, device_id={"dp": lax.rem(group + step, groups)}, device_id_type=MESH
        )
    mine[...] = jnp.zeros_like(mine)
    for row in range(late_ref.shape[0]):
        mine[row : row + 1, :] = jnp.sum(late_ref[row], axis=0, keepdims=True)
    for row in range(early_ref.shape[0]):
        at = late_ref.shape[0] + row
        mine[at : at + 1, :] = jnp.sum(early_ref[row], axis=0, keepdims=True)
    pl.semaphore_wait(barrier, ranks + groups - 2)

    def columns(rank):
        return pl.ds(pl.multiple_of(rank * part, part), part)

    def scatter(peer, slot, sem):
        return pltpu.make_async_remote_copy(
            src_ref=mine.at[:, columns(peer)],
            dst_ref=first.at[slot],
            send_sem=send1.at[sem],
            recv_sem=recv1.at[slot],
            device_id={"tensor": peer},
            device_id_type=MESH,
        )

    def exchange(peer, slot, sem):
        return pltpu.make_async_remote_copy(
            src_ref=stage,
            dst_ref=second.at[slot],
            send_sem=send2.at[sem],
            recv_sem=recv2.at[slot],
            device_id={"dp": peer},
            device_id_type=MESH,
        )

    def spread(peer, rank, sem):
        return pltpu.make_async_remote_copy(
            src_ref=all_ref.at[:, columns(me)],
            dst_ref=all_ref.at[:, columns(rank)],
            send_sem=send3.at[sem],
            recv_sem=recv3.at[rank],
            device_id={"tensor": peer},
            device_id_type=MESH,
        )

    for step in range(1, ranks):
        scatter(lax.rem(me + step, ranks), me, step).start()
    first[me] = mine[:, columns(me)]
    for step in range(1, ranks):
        other = lax.rem(me + step, ranks)
        scatter(other, other, step).wait_recv()
    rows = mine.shape[0]
    total = first[0]
    for rank in range(1, ranks):
        total = total + first[rank]
    stage[:rows, :] = total
    stage[rows:, :] = own_ref[...]
    for step in range(1, groups):
        exchange(lax.rem(group + step, groups), group, step).start()
    second[group] = stage[...]
    for step in range(1, groups):
        other = lax.rem(group + step, groups)
        exchange(other, other, step).wait_recv()
    total = second[0]
    for index in range(1, groups):
        total = total + second[index]
    all_ref[:, columns(me)] = total[:rows]
    dp_ref[...] = total[rows:]
    for step in range(1, ranks):
        spread(lax.rem(me + step, ranks), me, step).start()
    for step in range(1, ranks):
        other = lax.rem(me + step, ranks)
        spread(other, other, step).wait_recv()
    for step in range(1, ranks):
        other = lax.rem(me + step, ranks)
        scatter(other, me, step).wait_send()
        spread(other, me, step).wait_send()
    for step in range(1, groups):
        exchange(lax.rem(group + step, groups), group, step).wait_send()


def total_call(late, early, own):
    ranks = lax.axis_size("tensor")
    groups = lax.axis_size("dp")
    width = late.shape[2]
    part = width // ranks
    dma = pltpu.SemaphoreType.DMA

    def kernel(late_ref, early_ref, own_ref, all_ref, dp_ref, mine, first, stage, second, *sems):
        total_kernel(
            ranks, groups, late_ref, early_ref, own_ref, all_ref, dp_ref, mine, first, stage, second, sems
        )

    in_vmem = pl.BlockSpec(memory_space=pltpu.VMEM)
    return pl.pallas_call(
        kernel,
        in_specs=[in_vmem] * 3,
        out_specs=[in_vmem] * 2,
        out_shape=[
            jax.ShapeDtypeStruct((8, width), jnp.float32),
            jax.ShapeDtypeStruct((8, part), jnp.float32),
        ],
        scratch_shapes=[
            pltpu.VMEM((8, width), jnp.float32),
            pltpu.VMEM((ranks, 8, part), jnp.float32),
            pltpu.VMEM((16, part), jnp.float32),
            pltpu.VMEM((groups, 16, part), jnp.float32),
            dma((ranks,)),
            dma((ranks,)),
            dma((groups,)),
            dma((groups,)),
            dma((ranks,)),
            dma((ranks,)),
        ],
        compiler_params=pltpu.CompilerParams(collective_id=5, has_side_effects=True),
        name="total_sums",
    )(late, early, own)


MLP_TILE = 256


def mlp_forward_kernel(rows_ref, up_ref, bias_ref, down_ref, active_ref, slope_ref, out_ref):
    width = up_ref.shape[1]
    for first in range(0, width, MLP_TILE):
        cols = slice(first, first + MLP_TILE)
        value = jnp.dot(rows_ref[...], up_ref[:, cols], preferred_element_type=jnp.float32)
        value = value + bias_ref[:, cols]
        below = 0.5 + 0.5 * lax.erf(value * math.sqrt(0.5))
        density = jnp.exp(-0.5 * value * value) * (1.0 / math.sqrt(2.0 * math.pi))
        slope_ref[:, cols] = below + value * density
        active_ref[:, cols] = (value * below).astype(jnp.bfloat16)
    out_ref[...] = jnp.dot(
        active_ref[...], down_ref[...], preferred_element_type=jnp.float32
    ).astype(jnp.bfloat16)


def resident(shape):
    return pl.BlockSpec(shape, lambda i: (0,) * len(shape), pipeline_mode=pl.Buffered(1))


def mlp_forward(rows, up_full, up_bias, down_full):
    tokens, width = rows.shape
    hidden = up_full.shape[1]
    block = min(256, tokens)
    return pl.pallas_call(
        mlp_forward_kernel,
        grid=(tokens // block,),
        in_specs=[
            pl.BlockSpec((block, width), lambda i: (i, 0)),
            resident((width, hidden)),
            resident((1, hidden)),
            resident((hidden, width)),
        ],
        out_specs=[
            pl.BlockSpec((block, hidden), lambda i: (i, 0)),
            pl.BlockSpec((block, hidden), lambda i: (i, 0)),
            pl.BlockSpec((block, width), lambda i: (i, 0)),
        ],
        out_shape=[
            jax.ShapeDtypeStruct((tokens, hidden), jnp.bfloat16),
            jax.ShapeDtypeStruct((tokens, hidden), jnp.float32),
            jax.ShapeDtypeStruct((tokens, width), jnp.bfloat16),
        ],
        compiler_params=pltpu.CompilerParams(vmem_limit_bytes=48 * 2**20),
        cost_estimate=pl.CostEstimate(
            flops=4 * tokens * width * hidden, bytes_accessed=8 * tokens * width, transcendentals=0
        ),
        name="mlp_forward",
    )(rows, up_full, up_bias[None], down_full)


def mlp_backward_kernel(
    one_ref, two_ref, slope_ref, down_ref, up_ref, whole_ref, pre_ref, part_ref, sums_ref
):
    half = one_ref.shape[1]
    whole_ref[:half, :] = one_ref[0]
    whole_ref[half:, :] = two_ref[0]
    hidden = slope_ref.shape[1]

    @pl.when(pl.program_id(0) == 0)
    def _():
        sums_ref[...] = jnp.zeros_like(sums_ref)

    for first in range(0, hidden, MLP_TILE):
        cols = slice(first, first + MLP_TILE)
        grad = lax.dot_general(
            whole_ref[...], down_ref[cols, :], NT, preferred_element_type=jnp.float32
        )
        pre = (grad * slope_ref[:, cols]).astype(jnp.bfloat16)
        pre_ref[:, cols] = pre
        sums_ref[:, cols] += jnp.sum(pre.astype(jnp.float32).reshape(-1, 8, MLP_TILE), axis=0)
    part_ref[...] = lax.dot_general(
        pre_ref[...], up_ref[...], NT, preferred_element_type=jnp.float32
    ).astype(jnp.bfloat16)


def mlp_backward(one, two, slope, down_full, up_full):
    ranks, half, width = one.shape
    rows = 2 * half
    hidden = slope.shape[1]
    tokens = ranks * rows
    return pl.pallas_call(
        mlp_backward_kernel,
        grid=(ranks,),
        in_specs=[
            pl.BlockSpec((1, half, width), lambda i: (i, 0, 0)),
            pl.BlockSpec((1, half, width), lambda i: (i, 0, 0)),
            pl.BlockSpec((rows, hidden), lambda i: (i, 0)),
            resident((hidden, width)),
            resident((width, hidden)),
        ],
        out_specs=[
            pl.BlockSpec((rows, width), lambda i: (i, 0)),
            pl.BlockSpec((rows, hidden), lambda i: (i, 0)),
            pl.BlockSpec((rows, width), lambda i: (i, 0)),
            pl.BlockSpec((8, hidden), lambda i: (0, 0)),
        ],
        out_shape=[
            jax.ShapeDtypeStruct((tokens, width), jnp.bfloat16),
            jax.ShapeDtypeStruct((tokens, hidden), jnp.bfloat16),
            jax.ShapeDtypeStruct((tokens, width), jnp.bfloat16),
            jax.ShapeDtypeStruct((8, hidden), jnp.float32),
        ],
        compiler_params=pltpu.CompilerParams(vmem_limit_bytes=48 * 2**20),
        cost_estimate=pl.CostEstimate(
            flops=4 * tokens * width * hidden, bytes_accessed=10 * tokens * width, transcendentals=0
        ),
        name="mlp_backward",
    )(one, two, slope, down_full, up_full)


def over_dp(grad, dimension):
    return lax.psum_scatter(grad, "dp", scatter_dimension=dimension, tiled=True).astype(jnp.float32)


def layer(
    layer_input,
    segment_ids,
    first_gain,
    first_shift,
    qkv_weight,
    query_value_bias,
    dense_weight,
    dense_bias,
    second_gain,
    second_shift,
    up_weight,
    up_bias,
    down_weight,
    down_bias,
    out_grad,
):
    rows, width = layer_input.shape
    ranks = lax.axis_size("tensor")
    tokens = ranks * rows
    f32_rows = jax.ShapeDtypeStruct((rows, width), jnp.float32)

    qkv_full = lax.all_gather(qkv_weight, "dp", axis=1, tiled=True)
    dense_full = lax.all_gather(dense_weight, "dp", axis=1, tiled=True)
    up_full = lax.all_gather(up_weight, "dp", axis=0, tiled=True)
    down_full = lax.all_gather(down_weight, "dp", axis=1, tiled=True)
    half = rows // 2
    out_one = lax.all_gather(out_grad[:half], "tensor", axis=0, tiled=False)
    out_two = lax.all_gather(out_grad[half:], "tensor", axis=0, tiled=False)

    head_width = qkv_full.shape[2]
    up_width = up_bias.shape[0]
    qkv_cat = jnp.transpose(qkv_full, (1, 0, 2)).reshape(width, 3 * head_width)

    (whole1,) = line_call(
        norm_gather_kernel, 1,
        (layer_input, first_gain[None], first_shift[None]), (), True, False, rows, width,
    )
    whole1 = whole1.reshape(tokens, width)
    zero_bias = jnp.zeros_like(query_value_bias[0])
    bias_cat = jnp.concatenate([query_value_bias[0], zero_bias, query_value_bias[1]])
    projected = (jnp.dot(whole1, qkv_cat, preferred_element_type=jnp.float32) + bias_cat).astype(
        jnp.bfloat16
    )
    head_count = head_width // HEAD_DIM
    tensor_pos = lax.axis_index("tensor")
    global_heads = tensor_pos * head_count + jnp.arange(head_count, dtype=jnp.int32)
    slopes = jnp.power(2.0, -8.0 * (global_heads + 1).astype(jnp.float32) / HEADS)
    attended, log_sums = attention_forward(projected, segment_ids, slopes)
    attn_part = jnp.dot(attended, dense_full, preferred_element_type=jnp.float32).astype(jnp.bfloat16)
    whole2, residual = line_call(
        branch_norm_gather_kernel, 2,
        (attn_part.reshape(ranks, rows, width), layer_input, dense_bias[None], second_gain[None], second_shift[None]),
        (f32_rows,), True, True, rows, width,
    )
    whole2 = whole2.reshape(tokens, width)
    activated, slope, mlp_part = mlp_forward(whole2, up_full, up_bias, down_full)
    out_whole, pre_grad, normed2_part, up_bias_sums = mlp_backward(
        out_one, out_two, slope, down_full, up_full
    )
    up_bias_part = jnp.sum(up_bias_sums, axis=0)
    down_grad = lax.dot_general(
        activated, out_whole, (((0,), (0,)), ((), ())), preferred_element_type=jnp.float32
    ).astype(jnp.bfloat16)
    up_grad = lax.dot_general(
        whole2, pre_grad, (((0,), (0,)), ((), ())), preferred_element_type=jnp.float32
    ).astype(jnp.bfloat16)
    normed2_part, down_grad, up_grad = lax.optimization_barrier((normed2_part, down_grad, up_grad))
    down_wgrad = over_dp(down_grad, 1)
    up_wgrad = over_dp(up_grad, 0)
    mlp_rows = lax.psum_scatter(mlp_part, "tensor", scatter_dimension=0, tiled=True)
    mlp_branch = mlp_rows.astype(jnp.float32) + down_bias
    layer_out = (residual + mlp_branch).astype(jnp.bfloat16)

    branch_whole, residual_grad, second_sums = line_call(
        grad_gather_kernel, 3,
        (normed2_part.reshape(ranks, rows, width), residual, out_grad, second_gain[None]),
        (f32_rows, jax.ShapeDtypeStruct((4, 8, width), jnp.float32)), True, True, rows, width,
    )
    branch_whole = branch_whole.reshape(tokens, width)
    attended_grad = lax.dot_general(
        branch_whole, dense_full, (((1,), (1,)), ((), ())), preferred_element_type=jnp.float32
    ).astype(jnp.bfloat16)
    dense_grad = lax.dot_general(
        attended, branch_whole, (((0,), (0,)), ((), ())), preferred_element_type=jnp.float32
    ).astype(jnp.bfloat16)
    attended_grad, dense_grad = lax.optimization_barrier((attended_grad, dense_grad))
    qkv_grad_cat = attention_backward(projected, attended_grad, segment_ids, slopes, log_sums)
    dense_wgrad = over_dp(dense_grad, 1)
    qkv_sums = jnp.sum(qkv_grad_cat.astype(jnp.float32), axis=0)
    bias_part = jnp.stack([qkv_sums[:head_width], qkv_sums[2 * head_width :]])
    qkv_grad_flat = lax.dot_general(
        whole1, qkv_grad_cat, (((0,), (0,)), ((), ())), preferred_element_type=jnp.float32
    )
    qkv_grad = jnp.transpose(
        qkv_grad_flat.astype(jnp.bfloat16).reshape(width, 3, head_width), (1, 0, 2)
    )
    qkv_grad, qkv_grad_cat = lax.optimization_barrier((qkv_grad, qkv_grad_cat))
    qkv_wgrad = over_dp(qkv_grad, 1)
    normed1_part = lax.dot_general(
        qkv_grad_cat, qkv_cat, (((1,), (1,)), ((), ())), preferred_element_type=jnp.float32
    ).astype(jnp.bfloat16)
    input_grad, first_sums = line_call(
        grad_kernel, 4,
        (normed1_part.reshape(ranks, rows, width), layer_input, residual_grad, first_gain[None]),
        (f32_rows, jax.ShapeDtypeStruct((2, 8, width), jnp.float32)), False, True, rows, width,
    )
    part = width // ranks
    own = jnp.concatenate([bias_part.reshape(-1), up_bias_part]).reshape(-1, part)
    bias_rows = 2 * head_width // part
    own = jnp.pad(own, ((0, 8 - own.shape[0]), (0, 0)))
    sums, own = total_call(first_sums, second_sums, own)
    up_rows = up_width // part
    return (
        layer_out,
        input_grad,
        sums[0],
        sums[1],
        qkv_wgrad,
        own[:bias_rows].reshape(2, head_width),
        dense_wgrad,
        sums[4],
        sums[2],
        sums[3],
        up_wgrad,
        own[bias_rows : bias_rows + up_rows].reshape(up_width),
        down_wgrad,
        sums[5],
    )


def solution(mesh):
    token_rows = P(("dp", "tensor"), None)
    placed = (
        token_rows,
        P("dp"),
        P(),
        P(),
        P(None, "dp", "tensor"),
        P(None, "tensor"),
        P("tensor", "dp"),
        P(),
        P(),
        P(),
        P("dp", "tensor"),
        P("tensor"),
        P("tensor", "dp"),
        P(),
        token_rows,
    )
    return jax.shard_map(
        layer,
        mesh=mesh,
        in_specs=placed,
        out_specs=(
            token_rows,
            token_rows,
            P(),
            P(),
            P(None, "dp", "tensor"),
            P(None, "tensor"),
            P("tensor", "dp"),
            P(),
            P(),
            P(),
            P("dp", "tensor"),
            P("tensor"),
            P("tensor", "dp"),
            P(),
        ),
        check_vma=False,
    )
```

```python
import functools
import math

import jax
import jax.numpy as jnp
from jax import lax
from jax.experimental import pallas as pl
from jax.experimental.pallas import tpu as pltpu
from jax.sharding import PartitionSpec as P


HEADS = 32
EPSILON = 1e-05
MESH = pl.DeviceIdType.MESH
HEAD_DIM = 64
PAIR = 2 * HEAD_DIM
Q_BLOCK = 256
MASKED = -1e32
NT = (((1,), (1,)), ((), ()))
NN = (((1,), (0,)), ((), ()))


def key_window(seq_len, block):
    width = min(seq_len, Q_BLOCK + seq_len // 4)
    start = jnp.maximum(block * Q_BLOCK + Q_BLOCK - width, 0)
    return width, pl.multiple_of(start, 128)


def masked_distance(seg_row, seg_col, first_query, first_key, width):
    shape = (width, Q_BLOCK)
    key_pos = lax.broadcasted_iota(jnp.int32, shape, 0) + first_key
    query_pos = lax.broadcasted_iota(jnp.int32, shape, 1) + first_query
    delta = key_pos - query_pos
    allowed = (seg_col == seg_row) & (delta <= 0)
    return jnp.where(allowed, delta.astype(jnp.float32), MASKED)


def half_lanes(rows, half):
    lane = lax.broadcasted_iota(jnp.int32, rows.shape, 1)
    return jnp.where((lane < HEAD_DIM) == (half == 0), rows, jnp.zeros_like(rows))


def forward_kernel(slope_ref, proj_ref, seg_row_ref, seg_col_ref, out_ref, lse_ref, value_t, bias_ref):
    seq_len = proj_ref.shape[0]
    width_all = out_ref.shape[1]
    block = pl.program_id(0)

    @pl.when(block == 0)
    def _():
        value_t[...] = proj_ref[:, 2 * width_all :].T

    first = pl.multiple_of(block * Q_BLOCK, Q_BLOCK)
    width, start = key_window(seq_len, block)
    queries = pl.ds(first, Q_BLOCK)
    keys = pl.ds(start, width)
    bias_ref[...] = masked_distance(
        seg_row_ref[:, queries], seg_col_ref[keys, :], first, start, width
    )
    for pair in range(width_all // PAIR):
        cols = pair * PAIR
        query_pair = proj_ref[queries, cols : cols + PAIR] * 0.125
        key_pair = proj_ref[keys, width_all + cols : width_all + cols + PAIR]
        value_pair = value_t[cols : cols + PAIR, keys]
        mixed = []
        for half in range(2):
            head = 2 * pair + half
            scores = lax.dot_general(
                key_pair, half_lanes(query_pair, half), NT, preferred_element_type=jnp.float32
            )
            scores = scores + slope_ref[head] * bias_ref[...]
            highest = jnp.max(scores, axis=0, keepdims=True)
            exponent = jnp.exp(scores - highest)
            total = jnp.sum(exponent, axis=0, keepdims=True)
            part = lax.dot_general(
                value_pair[half * HEAD_DIM : (half + 1) * HEAD_DIM],
                exponent.astype(jnp.bfloat16),
                NN,
                preferred_element_type=jnp.float32,
            )
            mixed.append(part / total)
            lse_ref[head : head + 1, :] = highest + jnp.log(total)
        out_ref[:, cols : cols + PAIR] = jnp.concatenate(mixed, axis=0).T.astype(jnp.bfloat16)


def attention_forward(projected, segments, slopes):
    seq_len, all_cols = projected.shape
    cols = all_cols // 3
    heads = cols // HEAD_DIM
    width = min(seq_len, Q_BLOCK + seq_len // 4)
    return pl.pallas_call(
        forward_kernel,
        grid=(seq_len // Q_BLOCK,),
        in_specs=[
            pl.BlockSpec(memory_space=pltpu.SMEM),
            pl.BlockSpec((seq_len, all_cols), lambda i: (0, 0)),
            pl.BlockSpec((1, seq_len), lambda i: (0, 0)),
            pl.BlockSpec((seq_len, 1), lambda i: (0, 0)),
        ],
        out_specs=[
            pl.BlockSpec((Q_BLOCK, cols), lambda i: (i, 0)),
            pl.BlockSpec((heads, Q_BLOCK), lambda i: (0, i)),
        ],
        out_shape=[
            jax.ShapeDtypeStruct((seq_len, cols), jnp.bfloat16),
            jax.ShapeDtypeStruct((heads, seq_len), jnp.float32),
        ],
        scratch_shapes=[
            pltpu.VMEM((cols, seq_len), jnp.bfloat16),
            pltpu.VMEM((width, Q_BLOCK), jnp.float32),
        ],
        compiler_params=pltpu.CompilerParams(vmem_limit_bytes=40 * 2**20),
        cost_estimate=pl.CostEstimate(flops=4 * seq_len * width * cols, bytes_accessed=6 * seq_len * cols, transcendentals=0),
        name="attention_forward",
    )(slopes, projected, segments[None, :], segments[:, None])


def backward_kernel(slope_ref, proj_ref, grad_ref, lse_ref, seg_row_ref, seg_col_ref, out_ref,
                    key_t, bias_ref, key_sum, value_sum):
    seq_len = proj_ref.shape[0]
    width_all = grad_ref.shape[1]
    block = pl.program_id(0)

    @pl.when(block == 0)
    def _():
        key_t[...] = proj_ref[:, width_all : 2 * width_all].T
        key_sum[...] = jnp.zeros_like(key_sum)
        value_sum[...] = jnp.zeros_like(value_sum)

    first = pl.multiple_of(block * Q_BLOCK, Q_BLOCK)
    width, start = key_window(seq_len, block)
    queries = pl.ds(first, Q_BLOCK)
    keys = pl.ds(start, width)
    bias_ref[...] = masked_distance(
        seg_row_ref[:, queries], seg_col_ref[keys, :], first, start, width
    )
    for pair in range(width_all // PAIR):
        cols = pair * PAIR
        query_pair = proj_ref[queries, cols : cols + PAIR] * 0.125
        key_pair = proj_ref[keys, width_all + cols : width_all + cols + PAIR]
        value_pair = proj_ref[keys, 2 * width_all + cols : 2 * width_all + cols + PAIR]
        grad_pair = grad_ref[queries, cols : cols + PAIR]
        query_grads = []
        key_part = value_part = None
        for half in range(2):
            head = 2 * pair + half
            query_half = half_lanes(query_pair, half)
            grad_half = half_lanes(grad_pair, half)
            scores = lax.dot_general(key_pair, query_half, NT, preferred_element_type=jnp.float32)
            probs = jnp.exp(scores + slope_ref[head] * bias_ref[...] - lse_ref[head : head + 1, queries])
            prob_grad = lax.dot_general(value_pair, grad_half, NT, preferred_element_type=jnp.float32)
            inner = jnp.sum(probs * prob_grad, axis=0, keepdims=True)
            score_grad = (probs * (prob_grad - inner)).astype(jnp.bfloat16)
            value_half = jnp.dot(probs.astype(jnp.bfloat16), grad_half, preferred_element_type=jnp.float32)
            key_half = jnp.dot(score_grad, query_half, preferred_element_type=jnp.float32)
            query_grads.append(
                jnp.dot(
                    key_t[cols + half * HEAD_DIM : cols + (half + 1) * HEAD_DIM, keys],
                    score_grad,
                    preferred_element_type=jnp.float32,
                )
                * 0.125
            )
            value_part = value_half if half == 0 else value_part + value_half
            key_part = key_half if half == 0 else key_part + key_half
        key_sum[keys, cols : cols + PAIR] += key_part
        value_sum[keys, cols : cols + PAIR] += value_part
        out_ref[queries, cols : cols + PAIR] = (
            jnp.concatenate(query_grads, axis=0).T.astype(jnp.bfloat16)
        )

    @pl.when(block == pl.num_programs(0) - 1)
    def _():
        out_ref[:, width_all : 2 * width_all] = key_sum[...].astype(jnp.bfloat16)
        out_ref[:, 2 * width_all :] = value_sum[...].astype(jnp.bfloat16)


def attention_backward(projected, head_grad, segments, slopes, log_sums):
    seq_len, all_cols = projected.shape
    cols = all_cols // 3
    heads = cols // HEAD_DIM
    width = min(seq_len, Q_BLOCK + seq_len // 4)
    return pl.pallas_call(
        backward_kernel,
        grid=(seq_len // Q_BLOCK,),
        in_specs=[
            pl.BlockSpec(memory_space=pltpu.SMEM),
            pl.BlockSpec((seq_len, all_cols), lambda i: (0, 0)),
            pl.BlockSpec((seq_len, cols), lambda i: (0, 0)),
            pl.BlockSpec((heads, seq_len), lambda i: (0, 0)),
            pl.BlockSpec((1, seq_len), lambda i: (0, 0)),
            pl.BlockSpec((seq_len, 1), lambda i: (0, 0)),
        ],
        out_specs=pl.BlockSpec((seq_len, all_cols), lambda i: (0, 0)),
        out_shape=jax.ShapeDtypeStruct((seq_len, all_cols), jnp.bfloat16),
        scratch_shapes=[
            pltpu.VMEM((cols, seq_len), jnp.bfloat16),
            pltpu.VMEM((width, Q_BLOCK), jnp.float32),
            pltpu.VMEM((seq_len, cols), jnp.float32),
            pltpu.VMEM((seq_len, cols), jnp.float32),
        ],
        compiler_params=pltpu.CompilerParams(vmem_limit_bytes=48 * 2**20),
        cost_estimate=pl.CostEstimate(flops=10 * seq_len * width * cols, bytes_accessed=14 * seq_len * cols, transcendentals=0),
        name="attention_backward",
    )(slopes, projected, head_grad, log_sums, segments[None, :], segments[:, None])


ROW_TILE = 16
SUBS = 4
LAG = 0


def remote(src, dst, send_sem, recv_sem, peer):
    return pltpu.make_async_remote_copy(
        src_ref=src,
        dst_ref=dst,
        send_sem=send_sem,
        recv_sem=recv_sem,
        device_id={"tensor": peer},
        device_id_type=MESH,
    )


class Line:
    def __init__(self, chips, rows):
        self.chips = chips
        self.sub_rows = rows // SUBS
        self.me = lax.axis_index("tensor")
        self.place = self.me // 2
        self.core = self.me % 2
        self.above = self.me + 2
        self.below = self.me - 2
        self.partner = self.me + 1 - 2 * self.core
        self.has_above = self.place < chips - 1
        self.has_below = self.place > 0

    def rows(self, sub):
        return pl.ds(pl.multiple_of(sub * self.sub_rows, self.sub_rows), self.sub_rows)

    def tile(self, sub, tile):
        return pl.ds(pl.multiple_of(sub * self.sub_rows + tile * ROW_TILE, ROW_TILE), ROW_TILE)

    def enter(self):
        barrier = pltpu.get_barrier_semaphore()

        def greet(peer):
            pl.semaphore_signal(barrier, inc=1, device_id={"tensor": peer}, device_id_type=MESH)

        pl.when(self.has_above)(lambda: greet(self.above))
        pl.when(self.has_below)(lambda: greet(self.below))
        greet(self.partner)
        pl.semaphore_wait(
            barrier, 1 + self.has_above.astype(jnp.int32) + self.has_below.astype(jnp.int32)
        )


class Gather:
    def __init__(self, line, source, target, sems):
        self.line, self.source, self.target = line, source, target
        self.own_sem, self.line_send, self.line_recv, self.pair_send, self.pair_recv = sems

    @staticmethod
    def scratch(chips):
        dma = pltpu.SemaphoreType.DMA
        return [
            dma((SUBS,)),
            dma((2, chips, SUBS)),
            dma((2, chips, SUBS)),
            dma((chips, SUBS)),
            dma((chips, SUBS)),
        ]

    def hop(self, way, step, sub, src, block):
        peer = self.line.above if way == 0 else self.line.below
        return remote(
            src,
            self.target.at[block, self.line.rows(sub)],
            self.line_send.at[way, step, sub],
            self.line_recv.at[way, step, sub],
            peer,
        )

    def across(self, chip, sub, src, block):
        return remote(
            src,
            self.target.at[block, self.line.rows(sub)],
            self.pair_send.at[chip, sub],
            self.pair_recv.at[chip, sub],
            self.line.partner,
        )

    def own(self, sub):
        return pltpu.make_async_copy(
            self.source.at[self.line.rows(sub)],
            self.target.at[self.line.me, self.line.rows(sub)],
            self.own_sem.at[sub],
        )

    def start(self, sub):
        line = self.line
        src = self.source.at[line.rows(sub)]
        pl.when(line.has_above)(lambda: self.hop(0, 0, sub, src, line.me).start())
        pl.when(line.has_below)(lambda: self.hop(1, 0, sub, src, line.me).start())
        self.across(line.place, sub, src, line.me).start()
        self.own(sub).start()

    def step(self, sub, step, live):
        line = self.line
        for way, sign in ((0, -1), (1, 1)):
            block = line.me + 2 * sign * (step + 1)
            onward = line.has_above if way == 0 else line.has_below
            inside = block >= 0 if way == 0 else block < 2 * line.chips

            @pl.when(live & inside)
            def _():
                src = self.target.at[block, line.rows(sub)]
                self.hop(way, step, sub, src, block).wait_recv()

                @pl.when(onward)
                def _():
                    self.hop(way, step + 1, sub, src, block).start()

                self.across(block // 2, sub, src, block).start()

    def finish(self):
        line = self.line

        @pl.loop(0, SUBS)
        def _(sub):
            src = self.source.at[line.rows(sub)]
            for chip in range(line.chips):
                copy = self.across(chip, sub, src, 2 * chip + 1 - line.core)
                copy.wait_recv()
                copy.wait_send()
            for step in range(line.chips - 1):
                sent_up = line.has_above & (line.place >= step)
                sent_down = line.has_below & (line.place + step < line.chips)
                pl.when(sent_up)(lambda: self.hop(0, step, sub, src, line.me).wait_send())
                pl.when(sent_down)(lambda: self.hop(1, step, sub, src, line.me).wait_send())
            self.own(sub).wait()


class Reduce:
    def __init__(self, line, partial, bufs, sems, product=None):
        self.line, self.partial, self.product = line, partial, product
        self.held, self.paired, self.from_below, self.from_above = bufs
        self.held_sem, self.pair_send, self.pair_recv, self.line_send, self.line_recv = sems

    @staticmethod
    def scratch(chips, rows, width):
        dma = pltpu.SemaphoreType.DMA
        return [pltpu.VMEM((chips, rows, width), jnp.bfloat16)] * 4 + [
            dma((chips, SUBS)),
            dma((chips, SUBS)),
            dma((chips, SUBS)),
            dma((2, chips, SUBS)),
            dma((2, chips, SUBS)),
        ]

    def load(self, chip, sub):
        rows = self.line.rows(sub)
        return pltpu.make_async_copy(
            self.partial.at[2 * chip + self.line.core, rows],
            self.held.at[chip, rows],
            self.held_sem.at[chip, sub],
        )

    def across(self, chip, sub):
        rows = self.line.rows(sub)
        block = chip if self.product is not None else 2 * chip + 1 - self.line.core
        return remote(
            self.partial.at[block, rows],
            self.paired.at[chip, rows],
            self.pair_send.at[chip, sub],
            self.pair_recv.at[chip, sub],
            self.line.partner,
        )

    def hop(self, way, chip, sub):
        rows = self.line.rows(sub)
        return remote(
            self.held.at[chip, rows],
            (self.from_below if way == 0 else self.from_above).at[chip, rows],
            self.line_send.at[way, chip, sub],
            self.line_recv.at[way, chip, sub],
            self.line.above if way == 0 else self.line.below,
        )

    def start(self):
        line = self.line
        order = []
        for step in range(line.chips):
            chip = line.chips - 1 - step // 2 if step % 2 == 0 else step // 2
            order.append(chip)

        if self.product is None:

            @pl.loop(0, SUBS)
            def _(sub):
                for chip in order:
                    self.across(chip, sub).start()
                    self.load(chip, sub).start()

        zeros = jnp.zeros((ROW_TILE, self.held.shape[2]), jnp.bfloat16)

        def clear(buf, chip):
            @pl.loop(0, self.held.shape[1] // ROW_TILE)
            def _(tile):
                buf[chip, pl.ds(pl.multiple_of(tile * ROW_TILE, ROW_TILE), ROW_TILE), :] = zeros

        pl.when(jnp.logical_not(line.has_below))(lambda: clear(self.from_below, 0))
        pl.when(jnp.logical_not(line.has_above))(lambda: clear(self.from_above, line.chips - 1))

    def multiply(self, slot):
        line = self.line

        @pl.when(slot < line.chips // 2)
        def _():
            chips = (line.chips - 1 - slot, slot)
            for chip in chips:
                self.product(2 * chip + 1 - line.core, self.partial, chip)

                @pl.loop(0, SUBS)
                def _(sub):
                    self.across(chip, sub).start()

            for chip in chips:
                self.product(2 * chip + line.core, self.held, chip)

    def step(self, way, sub, step, live):
        line = self.line
        chip = line.chips - 1 - step if way == 0 else step
        arrived = self.from_below if way == 0 else self.from_above
        inner = line.has_below if way == 0 else line.has_above

        @pl.when(live & (chip > line.place if way == 0 else chip < line.place))
        def _():
            if self.product is None:
                self.load(chip, sub).wait()
            self.across(chip, sub).wait_recv()

            def add(with_arrived):
                @pl.loop(0, line.sub_rows // ROW_TILE)
                def _(tile):
                    at = line.tile(sub, tile)
                    total = self.held[chip, at, :].astype(jnp.float32)
                    total = total + self.paired[chip, at, :].astype(jnp.float32)
                    if with_arrived:
                        total = total + arrived[chip, at, :].astype(jnp.float32)
                    self.held[chip, at, :] = total.astype(jnp.bfloat16)

            @pl.when(inner)
            def _():
                self.hop(way, chip, sub).wait_recv()
                add(True)

            pl.when(jnp.logical_not(inner))(lambda: add(False))
            self.hop(way, chip, sub).start()

    def arrive(self, sub):
        line = self.line
        place = line.place
        if self.product is None:
            self.load(place, sub).wait()
        self.across(place, sub).wait_recv()
        pl.when(line.has_below)(lambda: self.hop(0, place, sub).wait_recv())
        pl.when(line.has_above)(lambda: self.hop(1, place, sub).wait_recv())

    def total(self, at):
        place = self.line.place
        total = self.held[place, at, :].astype(jnp.float32)
        total = total + self.paired[place, at, :].astype(jnp.float32)
        total = total + self.from_below[place, at, :].astype(jnp.float32)
        return total + self.from_above[place, at, :].astype(jnp.float32)

    def finish(self):
        line = self.line

        @pl.loop(0, SUBS)
        def _(sub):
            for chip in range(line.chips):
                self.across(chip, sub).wait_send()
                pl.when(chip > line.place)(lambda: self.hop(0, chip, sub).wait_send())
                pl.when(chip < line.place)(lambda: self.hop(1, chip, sub).wait_send())


def for_tiles(line, sub, body):
    @pl.loop(0, line.sub_rows // ROW_TILE)
    def _(tile):
        body(line.tile(sub, tile))


def run_gather(line, gather, rows_done):
    line.enter()
    steps = line.chips - 1

    @pl.loop(0, SUBS)
    def _(sub):
        for_tiles(line, sub, rows_done)
        gather.start(sub)

    @pl.loop(0, steps * SUBS)
    def _(at):
        gather.step(at % SUBS, at // SUBS, True)

    gather.finish()


def run_line(line, reduce, gather, rows_done, beside=None):
    steps = line.chips - 1
    if beside is None:
        line.enter()
    reduce.start()
    slots = steps * SUBS + LAG + (steps if gather is not None else 0) + 1

    @pl.loop(0, slots)
    def _(slot):
        if reduce.product is not None:
            reduce.multiply(slot)
        if beside is not None:
            beside(slot)
        for way in range(2):
            at = slot - (line.place if way == 0 else steps - line.place)
            sub = jnp.maximum(at, 0) // steps
            reduce.step(way, jnp.minimum(sub, SUBS - 1), jnp.maximum(at, 0) % steps, (at >= 0) & (sub < SUBS))
        at = slot - steps - LAG
        sub = jnp.maximum(at, 0) // steps

        @pl.when((at >= 0) & (at % steps == 0) & (sub < SUBS))
        def _():
            reduce.arrive(sub)
            for_tiles(line, sub, rows_done)
            if gather is not None:
                gather.start(sub)

        if gather is not None:
            at = slot - steps - LAG - 1
            sub = jnp.maximum(at, 0) // steps
            gather.step(
                jnp.minimum(sub, SUBS - 1), jnp.maximum(at, 0) % steps, (at >= 0) & (sub < SUBS)
            )

    reduce.finish()
    if gather is not None:
        gather.finish()


def unit_of(rows):
    centre = jnp.mean(rows, axis=1, keepdims=True)
    centred = rows - centre
    inv_std = lax.rsqrt(jnp.mean(centred * centred, axis=1, keepdims=True) + EPSILON)
    return centred * inv_std, inv_std


def norm_back(grad, unit, inv_std, gain):
    scaled = grad * gain
    return inv_std * (
        scaled
        - jnp.mean(scaled, axis=1, keepdims=True)
        - unit * jnp.mean(scaled * unit, axis=1, keepdims=True)
    )


def fold(rows):
    return jnp.sum(rows.reshape(-1, 8, rows.shape[1]), axis=0)


def norm_gather_kernel(chips, input_ref, gain_ref, shift_ref, whole_ref, normed_ref, *sems):
    line = Line(chips, input_ref.shape[0])
    gather = Gather(line, normed_ref, whole_ref, sems)

    def rows_done(at):
        unit, _ = unit_of(input_ref[at, :].astype(jnp.float32))
        normed_ref[at, :] = (unit * gain_ref[...] + shift_ref[...]).astype(jnp.bfloat16)

    run_gather(line, gather, rows_done)


def branch_norm_gather_kernel(
    chips, attended_ref, dense_ref, input_ref, bias_ref, gain_ref, shift_ref, whole_ref, residual_ref, normed_ref, mirror, *rest
):
    line = Line(chips, input_ref.shape[0])
    rows = input_ref.shape[0]
    parts, _, part = dense_ref.shape

    def product(block, target, slot):
        source = attended_ref[pl.ds(pl.multiple_of(block * rows, rows), rows), :]
        for index in range(parts):
            target[slot, :, index * part : (index + 1) * part] = jnp.dot(
                source, dense_ref[index], preferred_element_type=jnp.float32
            ).astype(jnp.bfloat16)

    reduce = Reduce(line, mirror, rest[:4], rest[4:9], product)
    gather = Gather(line, normed_ref, whole_ref, rest[9:])

    def rows_done(at):
        residual = input_ref[at, :].astype(jnp.float32) + (reduce.total(at) + bias_ref[...])
        residual_ref[at, :] = residual
        unit, _ = unit_of(residual)
        normed_ref[at, :] = (unit * gain_ref[...] + shift_ref[...]).astype(jnp.bfloat16)

    run_line(line, reduce, gather, rows_done)


def grad_gather_kernel(
    chips, partial_ref, residual_ref, grad_ref, gain_ref, whole_ref, residual_grad_ref, sums_ref, branch_ref, *rest
):
    line = Line(chips, grad_ref.shape[0])
    reduce = Reduce(line, partial_ref, rest[:4], rest[4:9])
    gather = Gather(line, branch_ref, whole_ref, rest[9:])
    sums_ref[...] = jnp.zeros_like(sums_ref)

    def rows_done(at):
        unit, inv_std = unit_of(residual_ref[at, :])
        grad = reduce.total(at)
        out_grad = grad_ref[at, :].astype(jnp.float32)
        residual_grad = out_grad + norm_back(grad, unit, inv_std, gain_ref[...])
        residual_grad_ref[at, :] = residual_grad
        branch = residual_grad.astype(jnp.bfloat16)
        branch_ref[at, :] = branch
        sums_ref[0] += fold(grad * unit)
        sums_ref[1] += fold(grad)
        sums_ref[2] += fold(branch.astype(jnp.float32))
        sums_ref[3] += fold(out_grad)

    run_line(line, reduce, gather, rows_done)


def grad_kernel(
    chips, grad_cat_ref, weight_ref, input_ref, residual_grad_ref, gain_ref, early_ref, own_ref,
    out_ref, early_out_ref, own_out_ref, late_ref, mirror, *rest
):
    line = Line(chips, input_ref.shape[0])
    rows = input_ref.shape[0]
    parts, three, part, head_width = weight_ref.shape

    def product(block, target, slot):
        at = pl.ds(pl.multiple_of(block * rows, rows), rows)
        for index in range(parts):
            total = None
            for kind in range(three):
                term = lax.dot_general(
                    grad_cat_ref[at, kind * head_width : (kind + 1) * head_width],
                    weight_ref[index, kind],
                    NT,
                    preferred_element_type=jnp.float32,
                )
                total = term if kind == 0 else total + term
            target[slot, :, index * part : (index + 1) * part] = total.astype(jnp.bfloat16)

    reduce = Reduce(line, mirror, rest[:4], rest[4:9], product)
    sums = Sums(2 * chips, early_ref, own_ref, early_out_ref, own_out_ref, late_ref, rest[9:])
    sums.late_sum[...] = jnp.zeros_like(sums.late_sum)

    def rows_done(at):
        unit, inv_std = unit_of(input_ref[at, :].astype(jnp.float32))
        grad = reduce.total(at)
        out_ref[at, :] = residual_grad_ref[at, :] + norm_back(grad, unit, inv_std, gain_ref[...])
        sums.late_sum[0] += fold(grad * unit)
        sums.late_sum[1] += fold(grad)

    sums.greet()
    run_line(line, reduce, None, rows_done, sums.beside)
    sums.close()


class Sums:
    def __init__(self, ranks, early_ref, own_ref, early_out, own_out, late_out, scratch):
        self.ranks = ranks
        self.groups = lax.axis_size("dp")
        self.me = lax.axis_index("tensor")
        self.group = lax.axis_index("dp")
        self.early, self.own = early_ref, own_ref
        self.early_out, self.own_out, self.late_out = early_out, own_out, late_out
        (
            self.late_sum, self.mine, self.first, self.stage, self.second,
            self.late_mine, self.late_group, self.late_stage, self.late_all,
        ) = scratch[:9]
        self.sems = scratch[9:]
        self.part = self.mine.shape[1] // ranks

    @staticmethod
    def scratch(ranks, groups, width):
        part = width // ranks
        f32 = jnp.float32
        dma = pltpu.SemaphoreType.DMA
        return [
            pltpu.VMEM((2, 8, width), f32),
            pltpu.VMEM((8, width), f32),
            pltpu.VMEM((ranks, 8, part), f32),
            pltpu.VMEM((16, part), f32),
            pltpu.VMEM((groups, 16, part), f32),
            pltpu.VMEM((8, width), f32),
            pltpu.VMEM((groups, 8, width), f32),
            pltpu.VMEM((8, width), f32),
            pltpu.VMEM((ranks, 8, width), f32),
        ] + [dma((ranks,)), dma((ranks,)), dma((groups,)), dma((groups,)), dma((ranks,)), dma((ranks,)),
             dma((groups,)), dma((groups,)), dma((ranks,)), dma((ranks,))]

    def rank(self, step):
        return lax.rem(self.me + step, self.ranks)

    def peer(self, step):
        return lax.rem(self.group + step, self.groups)

    def columns(self, rank):
        return pl.ds(pl.multiple_of(rank * self.part, self.part), self.part)

    def greet(self):
        barrier = pltpu.get_barrier_semaphore()
        for step in range(1, self.ranks):
            pl.semaphore_signal(
                barrier, inc=1, device_id={"tensor": self.rank(step)}, device_id_type=MESH
            )
        for step in range(1, self.groups):
            pl.semaphore_signal(
                barrier, inc=1, device_id={"dp": self.peer(step)}, device_id_type=MESH
            )
        pl.semaphore_wait(barrier, self.ranks + self.groups - 2)

    def copy(self, stage, src, dst, sem, slot, axis, peer):
        return pltpu.make_async_remote_copy(
            src_ref=src,
            dst_ref=dst,
            send_sem=self.sems[2 * stage].at[sem],
            recv_sem=self.sems[2 * stage + 1].at[slot],
            device_id={axis: peer},
            device_id_type=MESH,
        )

    def scatter(self, peer, slot, sem):
        return self.copy(0, self.mine.at[:, self.columns(peer)], self.first.at[slot], sem, slot, "tensor", peer)

    def exchange(self, peer, slot, sem):
        return self.copy(1, self.stage, self.second.at[slot], sem, slot, "dp", peer)

    def spread(self, peer, rank, sem):
        return self.copy(
            2, self.early_out.at[:, self.columns(self.me)], self.early_out.at[:, self.columns(rank)],
            sem, rank, "tensor", peer,
        )

    def late_exchange(self, peer, slot, sem):
        return self.copy(3, self.late_mine, self.late_group.at[slot], sem, slot, "dp", peer)

    def late_spread(self, peer, slot, sem):
        return self.copy(4, self.late_stage, self.late_all.at[slot], sem, slot, "tensor", peer)

    def beside(self, slot):
        @pl.when(slot == 1)
        def _():
            self.mine[...] = jnp.zeros_like(self.mine)
            for row in range(self.early.shape[0]):
                self.mine[row : row + 1, :] = jnp.sum(self.early[row], axis=0, keepdims=True)
            for step in range(1, self.ranks):
                self.scatter(self.rank(step), self.me, step).start()
            self.first[self.me] = self.mine[:, self.columns(self.me)]

        @pl.when(slot == 4)
        def _():
            for step in range(1, self.ranks):
                self.scatter(self.rank(step), self.rank(step), step).wait_recv()
            total = self.first[0]
            for rank in range(1, self.ranks):
                total = total + self.first[rank]
            self.stage[:8, :] = total
            self.stage[8:, :] = self.own[...]
            for step in range(1, self.groups):
                self.exchange(self.peer(step), self.group, step).start()
            self.second[self.group] = self.stage[...]

        @pl.when(slot == 7)
        def _():
            for step in range(1, self.groups):
                self.exchange(self.peer(step), self.peer(step), step).wait_recv()
            total = self.second[0]
            for index in range(1, self.groups):
                total = total + self.second[index]
            self.early_out[:, self.columns(self.me)] = total[:8]
            self.own_out[...] = total[8:]
            for step in range(1, self.ranks):
                self.spread(self.rank(step), self.me, step).start()

    def close(self):
        self.late_mine[...] = jnp.zeros_like(self.late_mine)
        for row in range(2):
            self.late_mine[row : row + 1, :] = jnp.sum(self.late_sum[row], axis=0, keepdims=True)
        for step in range(1, self.groups):
            self.late_exchange(self.peer(step), self.group, step).start()
        self.late_group[self.group] = self.late_mine[...]
        for step in range(1, self.groups):
            self.late_exchange(self.peer(step), self.peer(step), step).wait_recv()
        total = self.late_group[0]
        for index in range(1, self.groups):
            total = total + self.late_group[index]
        self.late_stage[...] = total
        for step in range(1, self.ranks):
            self.late_spread(self.rank(step), self.me, step).start()
        self.late_all[self.me] = total
        for step in range(1, self.ranks):
            self.spread(self.rank(step), self.rank(step), step).wait_recv()
        for step in range(1, self.ranks):
            self.late_spread(self.rank(step), self.rank(step), step).wait_recv()
        total = self.late_all[0]
        for rank in range(1, self.ranks):
            total = total + self.late_all[rank]
        self.late_out[...] = total
        for step in range(1, self.ranks):
            self.scatter(self.rank(step), self.me, step).wait_send()
            self.spread(self.rank(step), self.me, step).wait_send()
            self.late_spread(self.rank(step), self.me, step).wait_send()
        for step in range(1, self.groups):
            self.exchange(self.peer(step), self.group, step).wait_send()
            self.late_exchange(self.peer(step), self.group, step).wait_send()


def line_call(kernel, collective_id, operands, outs, rows, width, gathers=True, reduces=True, product=False, sums=False):
    ranks = lax.axis_size("tensor")
    chips = ranks // 2
    whole = jax.ShapeDtypeStruct((ranks, rows, width), jnp.bfloat16)
    in_vmem = pl.BlockSpec(memory_space=pltpu.VMEM)
    in_place = pl.BlockSpec(memory_space=pl.ANY)
    streamed = int(reduces and not product)
    scratch = []
    if gathers:
        scratch.append(pltpu.VMEM((rows, width), jnp.bfloat16))
    if product:
        scratch.append(pltpu.VMEM((chips, rows, width), jnp.bfloat16))
    if reduces:
        scratch += Reduce.scratch(chips, rows, width)
    if gathers:
        scratch += Gather.scratch(chips)
    if sums:
        scratch += Sums.scratch(ranks, lax.axis_size("dp"), width)
    return pl.pallas_call(
        functools.partial(kernel, chips),
        in_specs=[in_place] * streamed + [in_vmem] * (len(operands) - streamed),
        out_specs=([in_place] if gathers else []) + [in_vmem] * len(outs),
        out_shape=([whole] if gathers else []) + list(outs),
        scratch_shapes=scratch,
        compiler_params=pltpu.CompilerParams(
            collective_id=collective_id, has_side_effects=True, vmem_limit_bytes=52 * 2**20
        ),
        cost_estimate=pl.CostEstimate(
            flops=8 * rows * width * 100, bytes_accessed=100 * rows * width, transcendentals=0
        ),
    )(*operands)


def qkv_grad_kernel(rows_ref, grad_ref, out_ref, sums_ref):
    head_width = out_ref.shape[2]

    @pl.when(pl.program_id(0) == 0)
    def _():
        for kind in range(3):
            cols = slice(kind * head_width, (kind + 1) * head_width)
            sums_ref[kind] = jnp.sum(
                grad_ref[:, cols].astype(jnp.float32).reshape(-1, 8, head_width), axis=0
            )

    product = lax.dot_general(
        rows_ref[...], grad_ref[...], (((0,), (0,)), ((), ())), preferred_element_type=jnp.float32
    )
    for kind in range(3):
        out_ref[kind] = product[:, kind * head_width : (kind + 1) * head_width].astype(jnp.bfloat16)


def qkv_weight_grad(whole, grad_cat):
    tokens, width = whole.shape
    head_width = grad_cat.shape[1] // 3
    block = 256
    return pl.pallas_call(
        qkv_grad_kernel,
        grid=(width // block,),
        in_specs=[
            pl.BlockSpec((tokens, block), lambda i: (0, i)),
            pl.BlockSpec(grad_cat.shape, lambda i: (0, 0)),
        ],
        out_specs=[
            pl.BlockSpec((3, block, head_width), lambda i: (0, i, 0)),
            pl.BlockSpec((3, 8, head_width), lambda i: (0, 0, 0)),
        ],
        out_shape=[
            jax.ShapeDtypeStruct((3, width, head_width), jnp.bfloat16),
            jax.ShapeDtypeStruct((3, 8, head_width), jnp.float32),
        ],
        compiler_params=pltpu.CompilerParams(vmem_limit_bytes=40 * 2**20),
        cost_estimate=pl.CostEstimate(
            flops=6 * tokens * width * head_width, bytes_accessed=4 * tokens * width, transcendentals=0
        ),
        name="qkv_weight_grad",
    )(whole, grad_cat)


def finish_kernel(down_ref, up_ref, dense_ref, qkv_ref, one_ref, two_ref, residual_ref, bias_ref, grad_ref,
                  down_out, up_out, dense_out, qkv_out, rows_out, grad_out):
    down_out[...] = down_ref[...].astype(jnp.float32)
    up_out[...] = up_ref[...].astype(jnp.float32)
    dense_out[...] = dense_ref[...].astype(jnp.float32)
    qkv_out[...] = qkv_ref[...].astype(jnp.float32)
    half = pl.program_id(0) < pl.num_programs(0) // 2
    branch = jnp.where(half, one_ref[...], two_ref[...]).astype(jnp.float32) + bias_ref[...]
    rows_out[...] = (residual_ref[...] + branch).astype(jnp.bfloat16)
    grad_out[...] = grad_ref[...]


def finish(down, up, dense, qkv, one, two, residual, bias, input_grad):
    steps = 4

    def split(shape):
        if len(shape) == 3:
            return pl.BlockSpec((shape[0], shape[1] // steps, shape[2]), lambda i: (0, i, 0))
        return pl.BlockSpec((shape[0] // steps, shape[1]), lambda i: (i, 0))

    operands = (down, up, dense, qkv, one, two, residual, bias[None], input_grad)
    specs = [split(item.shape) for item in operands]
    row_part = (residual.shape[0] // steps, residual.shape[1])
    specs[4] = pl.BlockSpec(row_part, lambda i: (jnp.minimum(i, steps // 2 - 1), 0))
    specs[5] = pl.BlockSpec(row_part, lambda i: (jnp.maximum(i - steps // 2, 0), 0))
    specs[7] = pl.BlockSpec((1, bias.shape[0]), lambda i: (0, 0))
    outs = [jax.ShapeDtypeStruct(item.shape, jnp.float32) for item in (down, up, dense, qkv)]
    outs.append(jax.ShapeDtypeStruct(residual.shape, jnp.bfloat16))
    outs.append(jax.ShapeDtypeStruct(input_grad.shape, jnp.float32))
    return pl.pallas_call(
        finish_kernel,
        grid=(steps,),
        in_specs=specs,
        out_specs=[split(item.shape) for item in outs],
        out_shape=outs,
        compiler_params=pltpu.CompilerParams(vmem_limit_bytes=32 * 2**20),
        name="finish",
    )(*operands)


def dense_backward_kernel(branch_ref, attended_ref, dense_ref, grad_ref, weight_ref, total):
    parts, _, part = dense_ref.shape
    block = pl.program_id(0)

    @pl.when(block == 0)
    def _():
        total[...] = jnp.zeros_like(total)

    back = None
    for index in range(parts):
        cols = slice(index * part, (index + 1) * part)
        term = lax.dot_general(
            branch_ref[:, cols], dense_ref[index], NT, preferred_element_type=jnp.float32
        )
        back = term if index == 0 else back + term
    grad_ref[...] = back.astype(jnp.bfloat16)
    total[...] += lax.dot_general(
        attended_ref[...], branch_ref[...], (((0,), (0,)), ((), ())), preferred_element_type=jnp.float32
    )

    @pl.when(block == pl.num_programs(0) - 1)
    def _():
        weight_ref[...] = total[...].astype(jnp.bfloat16)


def dense_backward(branch, attended, dense_all):
    tokens, width = branch.shape
    head_width = attended.shape[1]
    block = min(512, tokens)
    return pl.pallas_call(
        dense_backward_kernel,
        grid=(tokens // block,),
        in_specs=[
            pl.BlockSpec((block, width), lambda i: (i, 0)),
            pl.BlockSpec((block, head_width), lambda i: (i, 0)),
            pl.BlockSpec(dense_all.shape, lambda i: (0, 0, 0)),
        ],
        out_specs=[
            pl.BlockSpec((block, head_width), lambda i: (i, 0)),
            pl.BlockSpec((head_width, width), lambda i: (0, 0)),
        ],
        out_shape=[
            jax.ShapeDtypeStruct((tokens, head_width), jnp.bfloat16),
            jax.ShapeDtypeStruct((head_width, width), jnp.bfloat16),
        ],
        scratch_shapes=[pltpu.VMEM((head_width, width), jnp.float32)],
        compiler_params=pltpu.CompilerParams(vmem_limit_bytes=40 * 2**20),
        cost_estimate=pl.CostEstimate(
            flops=4 * tokens * width * head_width, bytes_accessed=2 * tokens * width, transcendentals=0
        ),
        name="dense_backward",
    )(branch, attended, dense_all)


def project_kernel(rows_ref, weight_ref, bias_ref, out_ref):
    parts, three, part, head_width = weight_ref.shape
    for kind in range(three):
        total = None
        for index in range(parts):
            term = jnp.dot(
                rows_ref[:, index * part : (index + 1) * part],
                weight_ref[index, kind],
                preferred_element_type=jnp.float32,
            )
            total = term if index == 0 else total + term
        cols = slice(kind * head_width, (kind + 1) * head_width)
        out_ref[:, cols] = (total + bias_ref[:, cols]).astype(jnp.bfloat16)


def project(whole, qkv_all, query_value_bias):
    tokens, width = whole.shape
    head_width = qkv_all.shape[3]
    bias = jnp.concatenate(
        [query_value_bias[0], jnp.zeros_like(query_value_bias[0]), query_value_bias[1]]
    )[None]
    block = min(512, tokens)
    return pl.pallas_call(
        project_kernel,
        grid=(tokens // block,),
        in_specs=[
            pl.BlockSpec((block, width), lambda i: (i, 0)),
            pl.BlockSpec(qkv_all.shape, lambda i: (0, 0, 0, 0)),
            pl.BlockSpec((1, 3 * head_width), lambda i: (0, 0)),
        ],
        out_specs=pl.BlockSpec((block, 3 * head_width), lambda i: (i, 0)),
        out_shape=jax.ShapeDtypeStruct((tokens, 3 * head_width), jnp.bfloat16),
        compiler_params=pltpu.CompilerParams(vmem_limit_bytes=40 * 2**20),
        cost_estimate=pl.CostEstimate(
            flops=6 * tokens * width * head_width, bytes_accessed=2 * tokens * width, transcendentals=0
        ),
        name="project",
    )(whole, qkv_all, bias)


MLP_TILE = 256


def mlp_forward_kernel(rows_ref, up_ref, bias_ref, down_ref, active_ref, slope_ref, one_ref, two_ref):
    width = up_ref.shape[1]
    for first in range(0, width, MLP_TILE):
        cols = slice(first, first + MLP_TILE)
        value = jnp.dot(rows_ref[...], up_ref[:, cols], preferred_element_type=jnp.float32)
        value = value + bias_ref[:, cols]
        below = 0.5 + 0.5 * lax.erf(value * math.sqrt(0.5))
        density = jnp.exp(-0.5 * value * value) * (1.0 / math.sqrt(2.0 * math.pi))
        slope_ref[:, cols] = below + value * density
        active_ref[:, cols] = (value * below).astype(jnp.bfloat16)
    branch = jnp.dot(
        active_ref[...], down_ref[...], preferred_element_type=jnp.float32
    ).astype(jnp.bfloat16)
    half = one_ref.shape[0]
    one_ref[...] = branch[:half]
    two_ref[...] = branch[half:]


def resident(shape):
    return pl.BlockSpec(shape, lambda i: (0,) * len(shape), pipeline_mode=pl.Buffered(1))


def mlp_forward(rows, block, up_full, up_bias, down_full):
    tokens, width = rows.shape
    hidden = up_full.shape[1]
    return pl.pallas_call(
        mlp_forward_kernel,
        grid=(tokens // block,),
        in_specs=[
            pl.BlockSpec((block, width), lambda i: (i, 0)),
            resident((width, hidden)),
            resident((1, hidden)),
            resident((hidden, width)),
        ],
        out_specs=[
            pl.BlockSpec((block, hidden), lambda i: (i, 0)),
            pl.BlockSpec((block, hidden), lambda i: (i, 0)),
            pl.BlockSpec((block // 2, width), lambda i: (i, 0)),
            pl.BlockSpec((block // 2, width), lambda i: (i, 0)),
        ],
        out_shape=[
            jax.ShapeDtypeStruct((tokens, hidden), jnp.bfloat16),
            jax.ShapeDtypeStruct((tokens, hidden), jnp.float32),
            jax.ShapeDtypeStruct((tokens // 2, width), jnp.bfloat16),
            jax.ShapeDtypeStruct((tokens // 2, width), jnp.bfloat16),
        ],
        compiler_params=pltpu.CompilerParams(vmem_limit_bytes=48 * 2**20),
        cost_estimate=pl.CostEstimate(
            flops=4 * tokens * width * hidden, bytes_accessed=8 * tokens * width, transcendentals=0
        ),
        name="mlp_forward",
    )(rows, up_full, up_bias[None], down_full)


def mlp_backward_kernel(
    one_ref, two_ref, slope_ref, down_ref, up_ref, whole_ref, pre_ref, part_ref, sums_ref
):
    half = one_ref.shape[1]
    whole_ref[:half, :] = one_ref[0]
    whole_ref[half:, :] = two_ref[0]
    hidden = slope_ref.shape[1]

    @pl.when(pl.program_id(0) == 0)
    def _():
        sums_ref[...] = jnp.zeros_like(sums_ref)

    for first in range(0, hidden, MLP_TILE):
        cols = slice(first, first + MLP_TILE)
        grad = lax.dot_general(
            whole_ref[...], down_ref[cols, :], NT, preferred_element_type=jnp.float32
        )
        pre = (grad * slope_ref[:, cols]).astype(jnp.bfloat16)
        pre_ref[:, cols] = pre
        sums_ref[:, cols] += jnp.sum(pre.astype(jnp.float32).reshape(-1, 8, MLP_TILE), axis=0)
    part_ref[...] = lax.dot_general(
        pre_ref[...], up_ref[...], NT, preferred_element_type=jnp.float32
    ).astype(jnp.bfloat16)


def mlp_backward(one, two, slope, down_full, up_full):
    ranks, half, width = one.shape
    rows = 2 * half
    hidden = slope.shape[1]
    tokens = ranks * rows
    return pl.pallas_call(
        mlp_backward_kernel,
        grid=(ranks,),
        in_specs=[
            pl.BlockSpec((1, half, width), lambda i: (i, 0, 0)),
            pl.BlockSpec((1, half, width), lambda i: (i, 0, 0)),
            pl.BlockSpec((rows, hidden), lambda i: (i, 0)),
            resident((hidden, width)),
            resident((width, hidden)),
        ],
        out_specs=[
            pl.BlockSpec((rows, width), lambda i: (i, 0)),
            pl.BlockSpec((rows, hidden), lambda i: (i, 0)),
            pl.BlockSpec((rows, width), lambda i: (i, 0)),
            pl.BlockSpec((8, hidden), lambda i: (0, 0)),
        ],
        out_shape=[
            jax.ShapeDtypeStruct((tokens, width), jnp.bfloat16),
            jax.ShapeDtypeStruct((tokens, hidden), jnp.bfloat16),
            jax.ShapeDtypeStruct((tokens, width), jnp.bfloat16),
            jax.ShapeDtypeStruct((8, hidden), jnp.float32),
        ],
        compiler_params=pltpu.CompilerParams(vmem_limit_bytes=48 * 2**20),
        cost_estimate=pl.CostEstimate(
            flops=4 * tokens * width * hidden, bytes_accessed=10 * tokens * width, transcendentals=0
        ),
        name="mlp_backward",
    )(one, two, slope, down_full, up_full)


def over_dp(grad, dimension):
    return lax.psum_scatter(grad, "dp", scatter_dimension=dimension, tiled=True)


def layer(
    layer_input,
    segment_ids,
    first_gain,
    first_shift,
    qkv_weight,
    query_value_bias,
    dense_weight,
    dense_bias,
    second_gain,
    second_shift,
    up_weight,
    up_bias,
    down_weight,
    down_bias,
    out_grad,
):
    rows, width = layer_input.shape
    ranks = lax.axis_size("tensor")
    tokens = ranks * rows
    f32_rows = jax.ShapeDtypeStruct((rows, width), jnp.float32)

    qkv_all = lax.all_gather(qkv_weight, "dp", axis=0, tiled=False)
    dense_all = lax.all_gather(dense_weight, "dp", axis=0, tiled=False)
    up_full = lax.all_gather(up_weight, "dp", axis=0, tiled=True)
    down_full = lax.all_gather(down_weight, "dp", axis=1, tiled=True)
    half = rows // 2
    out_one = lax.all_gather(out_grad[:half], "tensor", axis=0, tiled=False)
    out_two = lax.all_gather(out_grad[half:], "tensor", axis=0, tiled=False)

    head_width = qkv_all.shape[3]
    up_width = up_bias.shape[0]
    (whole1,) = line_call(
        norm_gather_kernel, 1,
        (layer_input, first_gain[None], first_shift[None]), (), rows, width, reduces=False,
    )
    whole1 = whole1.reshape(tokens, width)
    projected = project(whole1, qkv_all, query_value_bias)
    head_count = head_width // HEAD_DIM
    tensor_pos = lax.axis_index("tensor")
    global_heads = tensor_pos * head_count + jnp.arange(head_count, dtype=jnp.int32)
    slopes = jnp.power(2.0, -8.0 * (global_heads + 1).astype(jnp.float32) / HEADS)
    attended, log_sums = attention_forward(projected, segment_ids, slopes)
    whole2, residual = line_call(
        branch_norm_gather_kernel, 2,
        (attended, dense_all, layer_input, dense_bias[None], second_gain[None], second_shift[None]),
        (f32_rows,), rows, width, product=True,
    )
    whole2 = whole2.reshape(tokens, width)
    activated, slope, mlp_one, mlp_two = mlp_forward(whole2, rows, up_full, up_bias, down_full)
    out_whole, pre_grad, normed2_part, up_bias_sums = mlp_backward(
        out_one, out_two, slope, down_full, up_full
    )
    up_bias_part = jnp.sum(up_bias_sums, axis=0)
    down_grad = lax.dot_general(
        activated, out_whole, (((0,), (0,)), ((), ())), preferred_element_type=jnp.float32
    ).astype(jnp.bfloat16)
    up_grad = lax.dot_general(
        whole2, pre_grad, (((0,), (0,)), ((), ())), preferred_element_type=jnp.float32
    ).astype(jnp.bfloat16)
    normed2_part, down_grad, up_grad = lax.optimization_barrier((normed2_part, down_grad, up_grad))
    down_wgrad = over_dp(down_grad, 1)
    up_wgrad = over_dp(up_grad, 0)
    mlp_rows_one = lax.psum_scatter(mlp_one, "tensor", scatter_dimension=0, tiled=True)
    mlp_rows_two = lax.psum_scatter(mlp_two, "tensor", scatter_dimension=0, tiled=True)

    branch_whole, residual_grad, second_sums = line_call(
        grad_gather_kernel, 3,
        (normed2_part.reshape(ranks, rows, width), residual, out_grad, second_gain[None]),
        (f32_rows, jax.ShapeDtypeStruct((4, 8, width), jnp.float32)), rows, width,
    )
    branch_whole = branch_whole.reshape(tokens, width)
    attended_grad, dense_grad = dense_backward(branch_whole, attended, dense_all)
    qkv_grad_cat = attention_backward(projected, attended_grad, segment_ids, slopes, log_sums)
    dense_wgrad = over_dp(dense_grad, 1)
    qkv_grad, qkv_sums = qkv_weight_grad(whole1, qkv_grad_cat)
    qkv_grad, qkv_grad_cat = lax.optimization_barrier((qkv_grad, qkv_grad_cat))
    qkv_wgrad = over_dp(qkv_grad, 1)
    qkv_sums = jnp.sum(qkv_sums, axis=1)
    part = width // ranks
    bias_rows = 2 * head_width // part
    up_rows = up_width // part
    own = jnp.concatenate([qkv_sums[0], qkv_sums[2], up_bias_part]).reshape(-1, part)
    own = jnp.pad(own, ((0, 8 - own.shape[0]), (0, 0)))
    f32_sums = jax.ShapeDtypeStruct((8, width), jnp.float32)
    input_grad, early, own, late = line_call(
        grad_kernel, 4,
        (qkv_grad_cat, qkv_all, layer_input, residual_grad, first_gain[None], second_sums, own),
        (f32_rows, f32_sums, jax.ShapeDtypeStruct((8, part), jnp.float32), f32_sums),
        rows, width, gathers=False, product=True, sums=True,
    )
    down_wgrad, up_wgrad, dense_wgrad, qkv_wgrad, layer_out, input_grad = finish(
        down_wgrad, up_wgrad, dense_wgrad, qkv_wgrad,
        mlp_rows_one, mlp_rows_two, residual, down_bias, input_grad,
    )
    return (
        layer_out,
        input_grad,
        late[0],
        late[1],
        qkv_wgrad,
        own[:bias_rows].reshape(2, head_width),
        dense_wgrad,
        early[2],
        early[0],
        early[1],
        up_wgrad,
        own[bias_rows : bias_rows + up_rows].reshape(up_width),
        down_wgrad,
        early[3],
    )


def solution(mesh):
    token_rows = P(("dp", "tensor"), None)
    placed = (
        token_rows,
        P("dp"),
        P(),
        P(),
        P(None, "dp", "tensor"),
        P(None, "tensor"),
        P("tensor", "dp"),
        P(),
        P(),
        P(),
        P("dp", "tensor"),
        P("tensor"),
        P("tensor", "dp"),
        P(),
        token_rows,
    )
    return jax.shard_map(
        layer,
        mesh=mesh,
        in_specs=placed,
        out_specs=(
            token_rows,
            token_rows,
            P(),
            P(),
            P(None, "dp", "tensor"),
            P(None, "tensor"),
            P("tensor", "dp"),
            P(),
            P(),
            P(),
            P("dp", "tensor"),
            P("tensor"),
            P("tensor", "dp"),
            P(),
        ),
        check_vma=False,
    )
```

```python
import functools
import math

import jax
import jax.numpy as jnp
from jax import lax
from jax.experimental import pallas as pl
from jax.experimental.pallas import tpu as pltpu
from jax.sharding import PartitionSpec as P


HEADS = 32
EPSILON = 1e-05
MESH = pl.DeviceIdType.MESH
HEAD_DIM = 64
PAIR = 2 * HEAD_DIM
Q_BLOCK = 256
MASKED = -1e32
VMEM_BYTES = 67043328
NT = (((1,), (1,)), ((), ()))
NN = (((1,), (0,)), ((), ()))


def key_window(seq_len, block):
    width = min(seq_len, Q_BLOCK + seq_len // 4)
    start = jnp.maximum(block * Q_BLOCK + Q_BLOCK - width, 0)
    return width, pl.multiple_of(start, 128)


def masked_distance(seg_row, seg_col, first_query, first_key, width):
    shape = (width, Q_BLOCK)
    key_pos = lax.broadcasted_iota(jnp.int32, shape, 0) + first_key
    query_pos = lax.broadcasted_iota(jnp.int32, shape, 1) + first_query
    delta = key_pos - query_pos
    allowed = (seg_col == seg_row) & (delta <= 0)
    return jnp.where(allowed, delta.astype(jnp.float32), MASKED)


def half_lanes(rows, half):
    lane = lax.broadcasted_iota(jnp.int32, rows.shape, 1)
    return jnp.where((lane < HEAD_DIM) == (half == 0), rows, jnp.zeros_like(rows))


def forward_kernel(slope_ref, proj_ref, seg_row_ref, seg_col_ref, out_ref, lse_ref, value_t, bias_ref):
    seq_len = proj_ref.shape[0]
    width_all = out_ref.shape[1]
    block = pl.program_id(0)

    @pl.when(block == 0)
    def _():
        value_t[...] = proj_ref[:, 2 * width_all :].T

    first = pl.multiple_of(block * Q_BLOCK, Q_BLOCK)
    width, start = key_window(seq_len, block)
    queries = pl.ds(first, Q_BLOCK)
    keys = pl.ds(start, width)
    bias_ref[...] = masked_distance(
        seg_row_ref[:, queries], seg_col_ref[keys, :], first, start, width
    )
    for pair in range(width_all // PAIR):
        cols = pair * PAIR
        query_pair = proj_ref[queries, cols : cols + PAIR] * 0.125
        key_pair = proj_ref[keys, width_all + cols : width_all + cols + PAIR]
        value_pair = value_t[cols : cols + PAIR, keys]
        mixed = []
        for half in range(2):
            head = 2 * pair + half
            scores = lax.dot_general(
                key_pair, half_lanes(query_pair, half), NT, preferred_element_type=jnp.float32
            )
            scores = scores + slope_ref[head] * bias_ref[...]
            highest = jnp.max(scores, axis=0, keepdims=True)
            exponent = jnp.exp(scores - highest)
            total = jnp.sum(exponent, axis=0, keepdims=True)
            part = lax.dot_general(
                value_pair[half * HEAD_DIM : (half + 1) * HEAD_DIM],
                exponent.astype(jnp.bfloat16),
                NN,
                preferred_element_type=jnp.float32,
            )
            mixed.append(part / total)
            lse_ref[head : head + 1, :] = highest + jnp.log(total)
        out_ref[:, cols : cols + PAIR] = jnp.concatenate(mixed, axis=0).T.astype(jnp.bfloat16)


def attention_forward(projected, segments, slopes):
    seq_len, all_cols = projected.shape
    cols = all_cols // 3
    heads = cols // HEAD_DIM
    width = min(seq_len, Q_BLOCK + seq_len // 4)
    return pl.pallas_call(
        forward_kernel,
        grid=(seq_len // Q_BLOCK,),
        in_specs=[
            pl.BlockSpec(memory_space=pltpu.SMEM),
            pl.BlockSpec((seq_len, all_cols), lambda i: (0, 0)),
            pl.BlockSpec((1, seq_len), lambda i: (0, 0)),
            pl.BlockSpec((seq_len, 1), lambda i: (0, 0)),
        ],
        out_specs=[
            pl.BlockSpec((Q_BLOCK, cols), lambda i: (i, 0)),
            pl.BlockSpec((heads, Q_BLOCK), lambda i: (0, i)),
        ],
        out_shape=[
            jax.ShapeDtypeStruct((seq_len, cols), jnp.bfloat16),
            jax.ShapeDtypeStruct((heads, seq_len), jnp.float32),
        ],
        scratch_shapes=[
            pltpu.VMEM((cols, seq_len), jnp.bfloat16),
            pltpu.VMEM((width, Q_BLOCK), jnp.float32),
        ],
        compiler_params=pltpu.CompilerParams(vmem_limit_bytes=VMEM_BYTES),
        cost_estimate=pl.CostEstimate(flops=4 * seq_len * width * cols, bytes_accessed=6 * seq_len * cols, transcendentals=0),
        name="attention_forward",
    )(slopes, projected, segments[None, :], segments[:, None])


def backward_kernel(slope_ref, proj_ref, grad_ref, lse_ref, seg_row_ref, seg_col_ref, out_ref,
                    key_t, bias_ref, key_sum, value_sum):
    seq_len = proj_ref.shape[0]
    width_all = grad_ref.shape[1]
    block = pl.program_id(0)

    @pl.when(block == 0)
    def _():
        key_t[...] = proj_ref[:, width_all : 2 * width_all].T
        key_sum[...] = jnp.zeros_like(key_sum)
        value_sum[...] = jnp.zeros_like(value_sum)

    first = pl.multiple_of(block * Q_BLOCK, Q_BLOCK)
    width, start = key_window(seq_len, block)
    queries = pl.ds(first, Q_BLOCK)
    keys = pl.ds(start, width)
    bias_ref[...] = masked_distance(
        seg_row_ref[:, queries], seg_col_ref[keys, :], first, start, width
    )
    for pair in range(width_all // PAIR):
        cols = pair * PAIR
        query_pair = proj_ref[queries, cols : cols + PAIR] * 0.125
        key_pair = proj_ref[keys, width_all + cols : width_all + cols + PAIR]
        value_pair = proj_ref[keys, 2 * width_all + cols : 2 * width_all + cols + PAIR]
        grad_pair = grad_ref[queries, cols : cols + PAIR]
        query_grads = []
        key_part = value_part = None
        for half in range(2):
            head = 2 * pair + half
            query_half = half_lanes(query_pair, half)
            grad_half = half_lanes(grad_pair, half)
            scores = lax.dot_general(key_pair, query_half, NT, preferred_element_type=jnp.float32)
            probs = jnp.exp(scores + slope_ref[head] * bias_ref[...] - lse_ref[head : head + 1, queries])
            prob_grad = lax.dot_general(value_pair, grad_half, NT, preferred_element_type=jnp.float32)
            inner = jnp.sum(probs * prob_grad, axis=0, keepdims=True)
            score_grad = (probs * (prob_grad - inner)).astype(jnp.bfloat16)
            value_half = jnp.dot(probs.astype(jnp.bfloat16), grad_half, preferred_element_type=jnp.float32)
            key_half = jnp.dot(score_grad, query_half, preferred_element_type=jnp.float32)
            query_grads.append(
                jnp.dot(
                    key_t[cols + half * HEAD_DIM : cols + (half + 1) * HEAD_DIM, keys],
                    score_grad,
                    preferred_element_type=jnp.float32,
                )
                * 0.125
            )
            value_part = value_half if half == 0 else value_part + value_half
            key_part = key_half if half == 0 else key_part + key_half
        key_sum[keys, cols : cols + PAIR] += key_part
        value_sum[keys, cols : cols + PAIR] += value_part
        out_ref[queries, cols : cols + PAIR] = (
            jnp.concatenate(query_grads, axis=0).T.astype(jnp.bfloat16)
        )

    @pl.when(block == pl.num_programs(0) - 1)
    def _():
        out_ref[:, width_all : 2 * width_all] = key_sum[...].astype(jnp.bfloat16)
        out_ref[:, 2 * width_all :] = value_sum[...].astype(jnp.bfloat16)


def attention_backward(projected, head_grad, segments, slopes, log_sums):
    seq_len, all_cols = projected.shape
    cols = all_cols // 3
    heads = cols // HEAD_DIM
    width = min(seq_len, Q_BLOCK + seq_len // 4)
    return pl.pallas_call(
        backward_kernel,
        grid=(seq_len // Q_BLOCK,),
        in_specs=[
            pl.BlockSpec(memory_space=pltpu.SMEM),
            pl.BlockSpec((seq_len, all_cols), lambda i: (0, 0)),
            pl.BlockSpec((seq_len, cols), lambda i: (0, 0)),
            pl.BlockSpec((heads, seq_len), lambda i: (0, 0)),
            pl.BlockSpec((1, seq_len), lambda i: (0, 0)),
            pl.BlockSpec((seq_len, 1), lambda i: (0, 0)),
        ],
        out_specs=pl.BlockSpec((seq_len, all_cols), lambda i: (0, 0)),
        out_shape=jax.ShapeDtypeStruct((seq_len, all_cols), jnp.bfloat16),
        scratch_shapes=[
            pltpu.VMEM((cols, seq_len), jnp.bfloat16),
            pltpu.VMEM((width, Q_BLOCK), jnp.float32),
            pltpu.VMEM((seq_len, cols), jnp.float32),
            pltpu.VMEM((seq_len, cols), jnp.float32),
        ],
        compiler_params=pltpu.CompilerParams(vmem_limit_bytes=VMEM_BYTES),
        cost_estimate=pl.CostEstimate(flops=10 * seq_len * width * cols, bytes_accessed=14 * seq_len * cols, transcendentals=0),
        name="attention_backward",
    )(slopes, projected, head_grad, log_sums, segments[None, :], segments[:, None])


ROW_TILE = 16
SUBS = 4
LAG = 0


def remote(src, dst, send_sem, recv_sem, peer):
    return pltpu.make_async_remote_copy(
        src_ref=src,
        dst_ref=dst,
        send_sem=send_sem,
        recv_sem=recv_sem,
        device_id={"tensor": peer},
        device_id_type=MESH,
    )


class Line:
    def __init__(self, chips, rows):
        self.chips = chips
        self.sub_rows = rows // SUBS
        self.me = lax.axis_index("tensor")
        self.place = self.me // 2
        self.core = self.me % 2
        self.above = self.me + 2
        self.below = self.me - 2
        self.partner = self.me + 1 - 2 * self.core
        self.has_above = self.place < chips - 1
        self.has_below = self.place > 0

    def rows(self, sub):
        return pl.ds(pl.multiple_of(sub * self.sub_rows, self.sub_rows), self.sub_rows)

    def tile(self, sub, tile):
        return pl.ds(pl.multiple_of(sub * self.sub_rows + tile * ROW_TILE, ROW_TILE), ROW_TILE)

    def enter(self):
        barrier = pltpu.get_barrier_semaphore()

        def greet(peer):
            pl.semaphore_signal(barrier, inc=1, device_id={"tensor": peer}, device_id_type=MESH)

        pl.when(self.has_above)(lambda: greet(self.above))
        pl.when(self.has_below)(lambda: greet(self.below))
        greet(self.partner)
        pl.semaphore_wait(
            barrier, 1 + self.has_above.astype(jnp.int32) + self.has_below.astype(jnp.int32)
        )


class Gather:
    def __init__(self, line, source, target, sems):
        self.line, self.source, self.target = line, source, target
        self.own_sem, self.line_send, self.line_recv, self.pair_send, self.pair_recv = sems

    @staticmethod
    def scratch(chips):
        dma = pltpu.SemaphoreType.DMA
        return [
            dma((SUBS,)),
            dma((2, chips, SUBS)),
            dma((2, chips, SUBS)),
            dma((chips, SUBS)),
            dma((chips, SUBS)),
        ]

    def hop(self, way, step, sub, src, block):
        peer = self.line.above if way == 0 else self.line.below
        return remote(
            src,
            self.target.at[block, self.line.rows(sub)],
            self.line_send.at[way, step, sub],
            self.line_recv.at[way, step, sub],
            peer,
        )

    def across(self, chip, sub, src, block):
        return remote(
            src,
            self.target.at[block, self.line.rows(sub)],
            self.pair_send.at[chip, sub],
            self.pair_recv.at[chip, sub],
            self.line.partner,
        )

    def own(self, sub):
        return pltpu.make_async_copy(
            self.source.at[self.line.rows(sub)],
            self.target.at[self.line.me, self.line.rows(sub)],
            self.own_sem.at[sub],
        )

    def start(self, sub):
        line = self.line
        src = self.source.at[line.rows(sub)]
        pl.when(line.has_above)(lambda: self.hop(0, 0, sub, src, line.me).start())
        pl.when(line.has_below)(lambda: self.hop(1, 0, sub, src, line.me).start())
        self.across(line.place, sub, src, line.me).start()
        self.own(sub).start()

    def step(self, sub, step, live):
        line = self.line
        for way, sign in ((0, -1), (1, 1)):
            block = line.me + 2 * sign * (step + 1)
            onward = line.has_above if way == 0 else line.has_below
            inside = block >= 0 if way == 0 else block < 2 * line.chips

            @pl.when(live & inside)
            def _():
                src = self.target.at[block, line.rows(sub)]
                self.hop(way, step, sub, src, block).wait_recv()

                @pl.when(onward)
                def _():
                    self.hop(way, step + 1, sub, src, block).start()

                self.across(block // 2, sub, src, block).start()

    def finish(self):
        line = self.line

        @pl.loop(0, SUBS)
        def _(sub):
            src = self.source.at[line.rows(sub)]
            for chip in range(line.chips):
                copy = self.across(chip, sub, src, 2 * chip + 1 - line.core)
                copy.wait_recv()
                copy.wait_send()
            for step in range(line.chips - 1):
                sent_up = line.has_above & (line.place >= step)
                sent_down = line.has_below & (line.place + step < line.chips)
                pl.when(sent_up)(lambda: self.hop(0, step, sub, src, line.me).wait_send())
                pl.when(sent_down)(lambda: self.hop(1, step, sub, src, line.me).wait_send())
            self.own(sub).wait()


class Reduce:
    def __init__(self, line, partial, bufs, sems, product=None):
        self.line, self.partial, self.product = line, partial, product
        self.held, self.paired, self.from_below, self.from_above = bufs
        self.held_sem, self.pair_send, self.pair_recv, self.line_send, self.line_recv = sems

    @staticmethod
    def scratch(chips, rows, width):
        dma = pltpu.SemaphoreType.DMA
        return [pltpu.VMEM((chips, rows, width), jnp.bfloat16)] * 4 + [
            dma((chips, SUBS)),
            dma((chips, SUBS)),
            dma((chips, SUBS)),
            dma((2, chips, SUBS)),
            dma((2, chips, SUBS)),
        ]

    def load(self, chip, sub):
        rows = self.line.rows(sub)
        return pltpu.make_async_copy(
            self.partial.at[2 * chip + self.line.core, rows],
            self.held.at[chip, rows],
            self.held_sem.at[chip, sub],
        )

    def across(self, chip, sub):
        rows = self.line.rows(sub)
        block = chip if self.product is not None else 2 * chip + 1 - self.line.core
        return remote(
            self.partial.at[block, rows],
            self.paired.at[chip, rows],
            self.pair_send.at[chip, sub],
            self.pair_recv.at[chip, sub],
            self.line.partner,
        )

    def hop(self, way, chip, sub):
        rows = self.line.rows(sub)
        return remote(
            self.held.at[chip, rows],
            (self.from_below if way == 0 else self.from_above).at[chip, rows],
            self.line_send.at[way, chip, sub],
            self.line_recv.at[way, chip, sub],
            self.line.above if way == 0 else self.line.below,
        )

    def start(self):
        line = self.line
        order = []
        for step in range(line.chips):
            chip = line.chips - 1 - step // 2 if step % 2 == 0 else step // 2
            order.append(chip)

        if self.product is None:

            @pl.loop(0, SUBS)
            def _(sub):
                for chip in order:
                    self.across(chip, sub).start()
                    self.load(chip, sub).start()

        zeros = jnp.zeros((ROW_TILE, self.held.shape[2]), jnp.bfloat16)

        def clear(buf, chip):
            @pl.loop(0, self.held.shape[1] // ROW_TILE)
            def _(tile):
                buf[chip, pl.ds(pl.multiple_of(tile * ROW_TILE, ROW_TILE), ROW_TILE), :] = zeros

        pl.when(jnp.logical_not(line.has_below))(lambda: clear(self.from_below, 0))
        pl.when(jnp.logical_not(line.has_above))(lambda: clear(self.from_above, line.chips - 1))

    def multiply(self, slot):
        line = self.line

        @pl.when(slot < line.chips // 2)
        def _():
            chips = (line.chips - 1 - slot, slot)
            for chip in chips:
                self.product(2 * chip + 1 - line.core, self.partial, chip)

                @pl.loop(0, SUBS)
                def _(sub):
                    self.across(chip, sub).start()

            for chip in chips:
                self.product(2 * chip + line.core, self.held, chip)

    def step(self, way, sub, step, live):
        line = self.line
        chip = line.chips - 1 - step if way == 0 else step
        arrived = self.from_below if way == 0 else self.from_above
        inner = line.has_below if way == 0 else line.has_above

        @pl.when(live & (chip > line.place if way == 0 else chip < line.place))
        def _():
            if self.product is None:
                self.load(chip, sub).wait()
            self.across(chip, sub).wait_recv()

            def add(with_arrived):
                @pl.loop(0, line.sub_rows // ROW_TILE)
                def _(tile):
                    at = line.tile(sub, tile)
                    total = self.held[chip, at, :].astype(jnp.float32)
                    total = total + self.paired[chip, at, :].astype(jnp.float32)
                    if with_arrived:
                        total = total + arrived[chip, at, :].astype(jnp.float32)
                    self.held[chip, at, :] = total.astype(jnp.bfloat16)

            @pl.when(inner)
            def _():
                self.hop(way, chip, sub).wait_recv()
                add(True)

            pl.when(jnp.logical_not(inner))(lambda: add(False))
            self.hop(way, chip, sub).start()

    def arrive(self, sub):
        line = self.line
        place = line.place
        if self.product is None:
            self.load(place, sub).wait()
        self.across(place, sub).wait_recv()
        pl.when(line.has_below)(lambda: self.hop(0, place, sub).wait_recv())
        pl.when(line.has_above)(lambda: self.hop(1, place, sub).wait_recv())

    def total(self, at):
        place = self.line.place
        total = self.held[place, at, :].astype(jnp.float32)
        total = total + self.paired[place, at, :].astype(jnp.float32)
        total = total + self.from_below[place, at, :].astype(jnp.float32)
        return total + self.from_above[place, at, :].astype(jnp.float32)

    def finish(self):
        line = self.line

        @pl.loop(0, SUBS)
        def _(sub):
            for chip in range(line.chips):
                self.across(chip, sub).wait_send()
                pl.when(chip > line.place)(lambda: self.hop(0, chip, sub).wait_send())
                pl.when(chip < line.place)(lambda: self.hop(1, chip, sub).wait_send())


def for_tiles(line, sub, body):
    size = min(2 * ROW_TILE, line.sub_rows)

    @pl.loop(0, line.sub_rows // size)
    def _(tile):
        body(pl.ds(pl.multiple_of(sub * line.sub_rows + tile * size, size), size))


def run_gather(line, gather, rows_done):
    line.enter()
    steps = line.chips - 1

    @pl.loop(0, SUBS)
    def _(sub):
        for_tiles(line, sub, rows_done)
        gather.start(sub)

    @pl.loop(0, steps * SUBS)
    def _(at):
        gather.step(at % SUBS, at // SUBS, True)

    gather.finish()


def run_line(line, reduce, gather, rows_done, beside=None, entered=False):
    steps = line.chips - 1
    if not entered:
        line.enter()
    reduce.start()
    slots = steps * SUBS + LAG + (steps if gather is not None else 0) + 1

    @pl.loop(0, slots)
    def _(slot):
        if reduce.product is not None:
            reduce.multiply(slot)
        if beside is not None:
            beside(slot)
        for way in range(2):
            at = slot - (line.place if way == 0 else steps - line.place)
            sub = jnp.maximum(at, 0) // steps
            reduce.step(way, jnp.minimum(sub, SUBS - 1), jnp.maximum(at, 0) % steps, (at >= 0) & (sub < SUBS))
        at = slot - steps - LAG
        sub = jnp.maximum(at, 0) // steps

        @pl.when((at >= 0) & (at % steps == 0) & (sub < SUBS))
        def _():
            reduce.arrive(sub)
            for_tiles(line, sub, rows_done)
            if gather is not None:
                gather.start(sub)

        if gather is not None:
            at = slot - steps - LAG - 1
            sub = jnp.maximum(at, 0) // steps
            gather.step(
                jnp.minimum(sub, SUBS - 1), jnp.maximum(at, 0) % steps, (at >= 0) & (sub < SUBS)
            )

    reduce.finish()
    if gather is not None:
        gather.finish()


def unit_of(rows):
    centre = jnp.mean(rows, axis=1, keepdims=True)
    centred = rows - centre
    inv_std = lax.rsqrt(jnp.mean(centred * centred, axis=1, keepdims=True) + EPSILON)
    return centred * inv_std, inv_std


def norm_back(grad, unit, inv_std, gain):
    scaled = grad * gain
    return inv_std * (
        scaled
        - jnp.mean(scaled, axis=1, keepdims=True)
        - unit * jnp.mean(scaled * unit, axis=1, keepdims=True)
    )


def fold(rows):
    return jnp.sum(rows.reshape(-1, 8, rows.shape[1]), axis=0)


def norm_gather_kernel(chips, input_ref, gain_ref, shift_ref, whole_ref, normed_ref, *sems):
    line = Line(chips, input_ref.shape[0])
    gather = Gather(line, normed_ref, whole_ref, sems)

    def rows_done(at):
        unit, _ = unit_of(input_ref[at, :].astype(jnp.float32))
        normed_ref[at, :] = (unit * gain_ref[...] + shift_ref[...]).astype(jnp.bfloat16)

    run_gather(line, gather, rows_done)


def branch_norm_gather_kernel(
    chips, attended_ref, dense_ref, input_ref, bias_ref, gain_ref, shift_ref, whole_ref, residual_ref, normed_ref, mirror, *rest
):
    line = Line(chips, input_ref.shape[0])
    rows = input_ref.shape[0]
    parts, _, part = dense_ref.shape

    def product(block, target, slot):
        source = attended_ref[pl.ds(pl.multiple_of(block * rows, rows), rows), :]
        for index in range(parts):
            target[slot, :, index * part : (index + 1) * part] = jnp.dot(
                source, dense_ref[index], preferred_element_type=jnp.float32
            ).astype(jnp.bfloat16)

    reduce = Reduce(line, mirror, rest[:4], rest[4:9], product)
    gather = Gather(line, normed_ref, whole_ref, rest[9:])

    def rows_done(at):
        residual = input_ref[at, :].astype(jnp.float32) + (reduce.total(at) + bias_ref[...])
        residual_ref[at, :] = residual
        unit, _ = unit_of(residual)
        normed_ref[at, :] = (unit * gain_ref[...] + shift_ref[...]).astype(jnp.bfloat16)

    run_line(line, reduce, gather, rows_done)


class Beside:
    def __init__(self, whole, pre, out, scratch):
        self.whole, self.pre, self.out = whole, pre, out
        self.loaded, self.stored, self.load_sem, self.store_sem = scratch
        self.block = self.loaded.shape[2]
        self.count = out.shape[0] // self.block

    @staticmethod
    def scratch(tokens, width, hidden):
        block = min(256, width)
        dma = pltpu.SemaphoreType.DMA
        return [
            pltpu.VMEM((2, tokens, block), jnp.bfloat16),
            pltpu.VMEM((2, block, hidden), jnp.bfloat16),
            dma((2,)),
            dma((2,)),
        ]

    def at(self, index):
        return pl.ds(pl.multiple_of(index * self.block, self.block), self.block)

    def load(self, index):
        return pltpu.make_async_copy(
            self.whole.at[:, self.at(index)], self.loaded.at[index % 2], self.load_sem.at[index % 2]
        )

    def store(self, index):
        return pltpu.make_async_copy(
            self.stored.at[index % 2], self.out.at[self.at(index)], self.store_sem.at[index % 2]
        )

    def start(self):
        self.load(0).start()

    def slot(self, slot):
        index = slot - 1

        @pl.when((index >= 0) & (index < self.count))
        def _():
            self.load(index).wait()
            pl.when(index + 1 < self.count)(lambda: self.load(index + 1).start())
            pl.when(index >= 2)(lambda: self.store(index - 2).wait())
            self.stored[index % 2] = lax.dot_general(
                self.loaded[index % 2],
                self.pre[...],
                (((0,), (0,)), ((), ())),
                preferred_element_type=jnp.float32,
            ).astype(jnp.bfloat16)
            self.store(index).start()

    def finish(self):
        for index in range(max(self.count - 2, 0), self.count):
            self.store(index).wait()


def grad_gather_kernel(
    chips, partial_ref, whole_in_ref, residual_ref, grad_ref, gain_ref, pre_ref,
    whole_ref, up_ref, residual_grad_ref, sums_ref, branch_ref, *rest
):
    line = Line(chips, grad_ref.shape[0])
    reduce = Reduce(line, partial_ref, rest[:4], rest[4:9])
    gather = Gather(line, branch_ref, whole_ref, rest[9:14])
    beside = Beside(whole_in_ref, pre_ref, up_ref, rest[14:])
    sums_ref[...] = jnp.zeros_like(sums_ref)

    def rows_done(at):
        unit, inv_std = unit_of(residual_ref[at, :])
        grad = reduce.total(at)
        out_grad = grad_ref[at, :].astype(jnp.float32)
        residual_grad = out_grad + norm_back(grad, unit, inv_std, gain_ref[...])
        residual_grad_ref[at, :] = residual_grad
        branch = residual_grad.astype(jnp.bfloat16)
        branch_ref[at, :] = branch
        sums_ref[0] += fold(grad * unit)
        sums_ref[1] += fold(grad)
        sums_ref[2] += fold(branch.astype(jnp.float32))
        sums_ref[3] += fold(out_grad)

    beside.start()
    run_line(line, reduce, gather, rows_done, beside.slot)
    beside.finish()


class Exchange:
    def __init__(self, partial, parts, scratch):
        self.partial, self.parts = partial, parts
        self.stage, self.in_sem, self.out_sem, self.send_sem, self.recv_sem = scratch
        self.groups = lax.axis_size("dp")
        self.group = lax.axis_index("dp")

    @staticmethod
    def scratch(groups, block):
        dma = pltpu.SemaphoreType.DMA
        return [pltpu.VMEM(block, jnp.bfloat16), dma, dma, dma((groups,)), dma((groups,))]

    def peer(self, step):
        return lax.rem(self.group + step, self.groups)

    def copy(self, peer, slot, step):
        return pltpu.make_async_remote_copy(
            src_ref=self.partial.at[peer],
            dst_ref=self.parts.at[slot],
            send_sem=self.send_sem.at[step],
            recv_sem=self.recv_sem.at[slot],
            device_id={"dp": peer},
            device_id_type=MESH,
        )

    def own_in(self):
        return pltpu.make_async_copy(self.partial.at[self.group], self.stage, self.in_sem)

    def own_out(self):
        return pltpu.make_async_copy(self.stage, self.parts.at[self.group], self.out_sem)

    def start(self):
        for step in range(1, self.groups):
            self.copy(self.peer(step), self.group, step).start()
        self.own_in().start()

    def slot(self, slot):
        @pl.when(slot == 2)
        def _():
            self.own_in().wait()
            self.own_out().start()

    def finish(self):
        for step in range(1, self.groups):
            self.copy(self.peer(step), self.peer(step), step).wait_recv()
            self.copy(self.peer(step), self.group, step).wait_send()
        self.own_out().wait()


def grad_kernel(
    chips, up_ref, grad_cat_ref, weight_ref, input_ref, residual_grad_ref, gain_ref, early_ref, own_ref,
    up_parts_ref, out_ref, early_out_ref, own_out_ref, late_ref, mirror, *rest
):
    line = Line(chips, input_ref.shape[0])
    rows = input_ref.shape[0]
    parts, three, part, head_width = weight_ref.shape

    def product(block, target, slot):
        at = pl.ds(pl.multiple_of(block * rows, rows), rows)
        for index in range(parts):
            total = None
            for kind in range(three):
                term = lax.dot_general(
                    grad_cat_ref[at, kind * head_width : (kind + 1) * head_width],
                    weight_ref[index, kind],
                    NT,
                    preferred_element_type=jnp.float32,
                )
                total = term if kind == 0 else total + term
            target[slot, :, index * part : (index + 1) * part] = total.astype(jnp.bfloat16)

    reduce = Reduce(line, mirror, rest[:4], rest[4:9], product)
    sums = Sums(2 * chips, early_ref, own_ref, early_out_ref, own_out_ref, late_ref, rest[9:28])
    exchange = Exchange(up_ref, up_parts_ref, rest[28:])
    sums.late_sum[...] = jnp.zeros_like(sums.late_sum)

    def rows_done(at):
        unit, inv_std = unit_of(input_ref[at, :].astype(jnp.float32))
        grad = reduce.total(at)
        out_ref[at, :] = residual_grad_ref[at, :] + norm_back(grad, unit, inv_std, gain_ref[...])
        sums.late_sum[0] += fold(grad * unit)
        sums.late_sum[1] += fold(grad)

    def beside(slot):
        sums.beside(slot)
        exchange.slot(slot)

    sums.greet()
    exchange.start()
    run_line(line, reduce, None, rows_done, beside, True)
    sums.close()
    exchange.finish()


class Sums:
    def __init__(self, ranks, early_ref, own_ref, early_out, own_out, late_out, scratch):
        self.ranks = ranks
        self.groups = lax.axis_size("dp")
        self.me = lax.axis_index("tensor")
        self.group = lax.axis_index("dp")
        self.early, self.own = early_ref, own_ref
        self.early_out, self.own_out, self.late_out = early_out, own_out, late_out
        (
            self.late_sum, self.mine, self.first, self.stage, self.second,
            self.late_mine, self.late_group, self.late_stage, self.late_all,
        ) = scratch[:9]
        self.sems = scratch[9:]
        self.part = self.mine.shape[1] // ranks

    @staticmethod
    def scratch(ranks, groups, width):
        part = width // ranks
        f32 = jnp.float32
        dma = pltpu.SemaphoreType.DMA
        return [
            pltpu.VMEM((2, 8, width), f32),
            pltpu.VMEM((8, width), f32),
            pltpu.VMEM((ranks, 8, part), f32),
            pltpu.VMEM((16, part), f32),
            pltpu.VMEM((groups, 16, part), f32),
            pltpu.VMEM((2, width), f32),
            pltpu.VMEM((groups, 2, width), f32),
            pltpu.VMEM((2, width), f32),
            pltpu.VMEM((ranks, 2, width), f32),
        ] + [dma((ranks,)), dma((ranks,)), dma((groups,)), dma((groups,)), dma((ranks,)), dma((ranks,)),
             dma((groups,)), dma((groups,)), dma((ranks,)), dma((ranks,))]

    def rank(self, step):
        return lax.rem(self.me + step, self.ranks)

    def peer(self, step):
        return lax.rem(self.group + step, self.groups)

    def columns(self, rank):
        return pl.ds(pl.multiple_of(rank * self.part, self.part), self.part)

    def greet(self):
        barrier = pltpu.get_barrier_semaphore()
        for step in range(1, self.ranks):
            pl.semaphore_signal(
                barrier, inc=1, device_id={"tensor": self.rank(step)}, device_id_type=MESH
            )
        for step in range(1, self.groups):
            pl.semaphore_signal(
                barrier, inc=1, device_id={"dp": self.peer(step)}, device_id_type=MESH
            )
        pl.semaphore_wait(barrier, self.ranks + self.groups - 2)

    def copy(self, stage, src, dst, sem, slot, axis, peer):
        return pltpu.make_async_remote_copy(
            src_ref=src,
            dst_ref=dst,
            send_sem=self.sems[2 * stage].at[sem],
            recv_sem=self.sems[2 * stage + 1].at[slot],
            device_id={axis: peer},
            device_id_type=MESH,
        )

    def scatter(self, peer, slot, sem):
        return self.copy(0, self.mine.at[:, self.columns(peer)], self.first.at[slot], sem, slot, "tensor", peer)

    def exchange(self, peer, slot, sem):
        return self.copy(1, self.stage, self.second.at[slot], sem, slot, "dp", peer)

    def spread(self, peer, rank, sem):
        return self.copy(
            2, self.early_out.at[:, self.columns(self.me)], self.early_out.at[:, self.columns(rank)],
            sem, rank, "tensor", peer,
        )

    def late_exchange(self, peer, slot, sem):
        return self.copy(3, self.late_mine, self.late_group.at[slot], sem, slot, "dp", peer)

    def late_spread(self, peer, slot, sem):
        return self.copy(4, self.late_stage, self.late_all.at[slot], sem, slot, "tensor", peer)

    def beside(self, slot):
        @pl.when(slot == 1)
        def _():
            self.mine[...] = jnp.zeros_like(self.mine)
            for row in range(self.early.shape[0]):
                self.mine[row : row + 1, :] = jnp.sum(self.early[row], axis=0, keepdims=True)
            for step in range(1, self.ranks):
                self.scatter(self.rank(step), self.me, step).start()
            self.first[self.me] = self.mine[:, self.columns(self.me)]

        @pl.when(slot == 4)
        def _():
            for step in range(1, self.ranks):
                self.scatter(self.rank(step), self.rank(step), step).wait_recv()
            total = self.first[0]
            for rank in range(1, self.ranks):
                total = total + self.first[rank]
            self.stage[:8, :] = total
            self.stage[8:, :] = self.own[...]
            for step in range(1, self.groups):
                self.exchange(self.peer(step), self.group, step).start()
            self.second[self.group] = self.stage[...]

        @pl.when(slot == 7)
        def _():
            for step in range(1, self.groups):
                self.exchange(self.peer(step), self.peer(step), step).wait_recv()
            total = self.second[0]
            for index in range(1, self.groups):
                total = total + self.second[index]
            self.early_out[:, self.columns(self.me)] = total[:8]
            self.own_out[...] = total[8:]
            for step in range(1, self.ranks):
                self.spread(self.rank(step), self.me, step).start()

    def close(self):
        for row in range(2):
            self.late_mine[row : row + 1, :] = jnp.sum(self.late_sum[row], axis=0, keepdims=True)
        for step in range(1, self.groups):
            self.late_exchange(self.peer(step), self.group, step).start()
        self.late_group[self.group] = self.late_mine[...]
        for step in range(1, self.groups):
            self.late_exchange(self.peer(step), self.peer(step), step).wait_recv()
        total = self.late_group[0]
        for index in range(1, self.groups):
            total = total + self.late_group[index]
        self.late_stage[...] = total
        for step in range(1, self.ranks):
            self.late_spread(self.rank(step), self.me, step).start()
        self.late_all[self.me] = total
        for step in range(1, self.ranks):
            self.spread(self.rank(step), self.rank(step), step).wait_recv()
        for step in range(1, self.ranks):
            self.late_spread(self.rank(step), self.rank(step), step).wait_recv()
        total = self.late_all[0]
        for rank in range(1, self.ranks):
            total = total + self.late_all[rank]
        self.late_out[...] = total
        for step in range(1, self.ranks):
            self.scatter(self.rank(step), self.me, step).wait_send()
            self.spread(self.rank(step), self.me, step).wait_send()
            self.late_spread(self.rank(step), self.me, step).wait_send()
        for step in range(1, self.groups):
            self.exchange(self.peer(step), self.group, step).wait_send()
            self.late_exchange(self.peer(step), self.group, step).wait_send()


def line_call(kernel, collective_id, operands, outs, rows, width, gathers=True, reduces=True, product=False, sums=False, placed=(), more=()):
    ranks = lax.axis_size("tensor")
    chips = ranks // 2
    whole = jax.ShapeDtypeStruct((ranks, rows, width), jnp.bfloat16)
    in_vmem = pl.BlockSpec(memory_space=pltpu.VMEM)
    in_place = pl.BlockSpec(memory_space=pl.ANY)
    ins_placed, outs_placed = placed or (0, 0)
    scratch = []
    if gathers:
        scratch.append(pltpu.VMEM((rows, width), jnp.bfloat16))
    if product:
        scratch.append(pltpu.VMEM((chips, rows, width), jnp.bfloat16))
    if reduces:
        scratch += Reduce.scratch(chips, rows, width)
    if gathers:
        scratch += Gather.scratch(chips)
    if sums:
        scratch += Sums.scratch(ranks, lax.axis_size("dp"), width)
    scratch += list(more)
    return pl.pallas_call(
        functools.partial(kernel, chips),
        in_specs=[in_place] * ins_placed + [in_vmem] * (len(operands) - ins_placed),
        out_specs=[in_place] * (outs_placed + int(gathers)) + [in_vmem] * (len(outs) - outs_placed),
        out_shape=([whole] if gathers else []) + list(outs),
        scratch_shapes=scratch,
        compiler_params=pltpu.CompilerParams(
            collective_id=collective_id, has_side_effects=True, vmem_limit_bytes=VMEM_BYTES
        ),
        cost_estimate=pl.CostEstimate(
            flops=8 * rows * width * 100, bytes_accessed=100 * rows * width, transcendentals=0
        ),
    )(*operands)


def qkv_grad_kernel(rows_ref, grad_ref, out_ref, sums_ref):
    head_width = out_ref.shape[2]

    @pl.when(pl.program_id(0) == 0)
    def _():
        for kind in range(3):
            cols = slice(kind * head_width, (kind + 1) * head_width)
            sums_ref[kind] = jnp.sum(
                grad_ref[:, cols].astype(jnp.float32).reshape(-1, 8, head_width), axis=0
            )

    product = lax.dot_general(
        rows_ref[...], grad_ref[...], (((0,), (0,)), ((), ())), preferred_element_type=jnp.float32
    )
    for kind in range(3):
        out_ref[kind] = product[:, kind * head_width : (kind + 1) * head_width].astype(jnp.bfloat16)


def qkv_weight_grad(whole, grad_cat):
    tokens, width = whole.shape
    head_width = grad_cat.shape[1] // 3
    block = 256
    return pl.pallas_call(
        qkv_grad_kernel,
        grid=(width // block,),
        in_specs=[
            pl.BlockSpec((tokens, block), lambda i: (0, i)),
            pl.BlockSpec(grad_cat.shape, lambda i: (0, 0)),
        ],
        out_specs=[
            pl.BlockSpec((3, block, head_width), lambda i: (0, i, 0)),
            pl.BlockSpec((3, 8, head_width), lambda i: (0, 0, 0)),
        ],
        out_shape=[
            jax.ShapeDtypeStruct((3, width, head_width), jnp.bfloat16),
            jax.ShapeDtypeStruct((3, 8, head_width), jnp.float32),
        ],
        compiler_params=pltpu.CompilerParams(vmem_limit_bytes=VMEM_BYTES),
        cost_estimate=pl.CostEstimate(
            flops=6 * tokens * width * head_width, bytes_accessed=4 * tokens * width, transcendentals=0
        ),
        name="qkv_weight_grad",
    )(whole, grad_cat)


def finish_kernel(down_ref, up_ref, dense_ref, qkv_ref, one_ref, two_ref, residual_ref, bias_ref, grad_ref,
                  down_out, up_out, dense_out, qkv_out, rows_out, grad_out):
    down_out[...] = down_ref[...].astype(jnp.float32)
    total = up_ref[0].astype(jnp.float32)
    for group in range(1, up_ref.shape[0]):
        total = total + up_ref[group].astype(jnp.float32)
    up_out[...] = total
    dense_out[...] = dense_ref[...].astype(jnp.float32)
    qkv_out[...] = qkv_ref[...].astype(jnp.float32)
    half = pl.program_id(0) < pl.num_programs(0) // 2
    branch = jnp.where(half, one_ref[...], two_ref[...]).astype(jnp.float32) + bias_ref[...]
    rows_out[...] = (residual_ref[...] + branch).astype(jnp.bfloat16)
    grad_out[...] = grad_ref[...]


def finish(down, up, dense, qkv, one, two, residual, bias, input_grad):
    steps = 4

    def split(shape):
        if len(shape) == 3:
            return pl.BlockSpec((shape[0], shape[1] // steps, shape[2]), lambda i: (0, i, 0))
        return pl.BlockSpec((shape[0] // steps, shape[1]), lambda i: (i, 0))

    operands = (down, up, dense, qkv, one, two, residual, bias[None], input_grad)
    specs = [split(item.shape) for item in operands]
    row_part = (residual.shape[0] // steps, residual.shape[1])
    specs[4] = pl.BlockSpec(row_part, lambda i: (jnp.minimum(i, steps // 2 - 1), 0))
    specs[5] = pl.BlockSpec(row_part, lambda i: (jnp.maximum(i - steps // 2, 0), 0))
    specs[7] = pl.BlockSpec((1, bias.shape[0]), lambda i: (0, 0))
    outs = [jax.ShapeDtypeStruct(item.shape, jnp.float32) for item in (down, up[0], dense, qkv)]
    outs.append(jax.ShapeDtypeStruct(residual.shape, jnp.bfloat16))
    outs.append(jax.ShapeDtypeStruct(input_grad.shape, jnp.float32))
    return pl.pallas_call(
        finish_kernel,
        grid=(steps,),
        in_specs=specs,
        out_specs=[split(item.shape) for item in outs],
        out_shape=outs,
        compiler_params=pltpu.CompilerParams(vmem_limit_bytes=VMEM_BYTES),
        name="finish",
    )(*operands)


def dense_backward_kernel(branch_ref, attended_ref, dense_ref, grad_ref, weight_ref, total):
    parts, _, part = dense_ref.shape
    block = pl.program_id(0)

    @pl.when(block == 0)
    def _():
        total[...] = jnp.zeros_like(total)

    back = None
    for index in range(parts):
        cols = slice(index * part, (index + 1) * part)
        term = lax.dot_general(
            branch_ref[:, cols], dense_ref[index], NT, preferred_element_type=jnp.float32
        )
        back = term if index == 0 else back + term
    grad_ref[...] = back.astype(jnp.bfloat16)
    total[...] += lax.dot_general(
        attended_ref[...], branch_ref[...], (((0,), (0,)), ((), ())), preferred_element_type=jnp.float32
    )

    @pl.when(block == pl.num_programs(0) - 1)
    def _():
        weight_ref[...] = total[...].astype(jnp.bfloat16)


def dense_backward(branch, attended, dense_all):
    tokens, width = branch.shape
    head_width = attended.shape[1]
    block = min(512, tokens)
    return pl.pallas_call(
        dense_backward_kernel,
        grid=(tokens // block,),
        in_specs=[
            pl.BlockSpec((block, width), lambda i: (i, 0)),
            pl.BlockSpec((block, head_width), lambda i: (i, 0)),
            pl.BlockSpec(dense_all.shape, lambda i: (0, 0, 0)),
        ],
        out_specs=[
            pl.BlockSpec((block, head_width), lambda i: (i, 0)),
            pl.BlockSpec((head_width, width), lambda i: (0, 0)),
        ],
        out_shape=[
            jax.ShapeDtypeStruct((tokens, head_width), jnp.bfloat16),
            jax.ShapeDtypeStruct((head_width, width), jnp.bfloat16),
        ],
        scratch_shapes=[pltpu.VMEM((head_width, width), jnp.float32)],
        compiler_params=pltpu.CompilerParams(vmem_limit_bytes=VMEM_BYTES),
        cost_estimate=pl.CostEstimate(
            flops=4 * tokens * width * head_width, bytes_accessed=2 * tokens * width, transcendentals=0
        ),
        name="dense_backward",
    )(branch, attended, dense_all)


def project_kernel(rows_ref, weight_ref, bias_ref, out_ref):
    parts, three, part, head_width = weight_ref.shape
    for kind in range(three):
        total = None
        for index in range(parts):
            term = jnp.dot(
                rows_ref[:, index * part : (index + 1) * part],
                weight_ref[index, kind],
                preferred_element_type=jnp.float32,
            )
            total = term if index == 0 else total + term
        cols = slice(kind * head_width, (kind + 1) * head_width)
        out_ref[:, cols] = (total + bias_ref[:, cols]).astype(jnp.bfloat16)


def project(whole, qkv_all, query_value_bias):
    tokens, width = whole.shape
    head_width = qkv_all.shape[3]
    bias = jnp.concatenate(
        [query_value_bias[0], jnp.zeros_like(query_value_bias[0]), query_value_bias[1]]
    )[None]
    block = min(512, tokens)
    return pl.pallas_call(
        project_kernel,
        grid=(tokens // block,),
        in_specs=[
            pl.BlockSpec((block, width), lambda i: (i, 0)),
            pl.BlockSpec(qkv_all.shape, lambda i: (0, 0, 0, 0)),
            pl.BlockSpec((1, 3 * head_width), lambda i: (0, 0)),
        ],
        out_specs=pl.BlockSpec((block, 3 * head_width), lambda i: (i, 0)),
        out_shape=jax.ShapeDtypeStruct((tokens, 3 * head_width), jnp.bfloat16),
        compiler_params=pltpu.CompilerParams(vmem_limit_bytes=VMEM_BYTES),
        cost_estimate=pl.CostEstimate(
            flops=6 * tokens * width * head_width, bytes_accessed=2 * tokens * width, transcendentals=0
        ),
        name="project",
    )(whole, qkv_all, bias)


MLP_TILE = 256


def mlp_forward_kernel(rows_ref, up_ref, bias_ref, down_ref, active_ref, slope_ref, one_ref, two_ref):
    width = up_ref.shape[1]
    for first in range(0, width, MLP_TILE):
        cols = slice(first, first + MLP_TILE)
        value = jnp.dot(rows_ref[...], up_ref[:, cols], preferred_element_type=jnp.float32)
        value = value + bias_ref[:, cols]
        below = 0.5 + 0.5 * lax.erf(value * math.sqrt(0.5))
        density = jnp.exp(-0.5 * value * value) * (1.0 / math.sqrt(2.0 * math.pi))
        slope_ref[:, cols] = below + value * density
        active_ref[:, cols] = (value * below).astype(jnp.bfloat16)
    branch = jnp.dot(
        active_ref[...], down_ref[...], preferred_element_type=jnp.float32
    ).astype(jnp.bfloat16)
    half = one_ref.shape[0]
    one_ref[...] = branch[:half]
    two_ref[...] = branch[half:]


def resident(shape):
    return pl.BlockSpec(shape, lambda i: (0,) * len(shape), pipeline_mode=pl.Buffered(1))


def mlp_forward(rows, block, up_full, up_bias, down_full):
    tokens, width = rows.shape
    hidden = up_full.shape[1]
    return pl.pallas_call(
        mlp_forward_kernel,
        grid=(tokens // block,),
        in_specs=[
            pl.BlockSpec((block, width), lambda i: (i, 0)),
            resident((width, hidden)),
            resident((1, hidden)),
            resident((hidden, width)),
        ],
        out_specs=[
            pl.BlockSpec((block, hidden), lambda i: (i, 0)),
            pl.BlockSpec((block, hidden), lambda i: (i, 0)),
            pl.BlockSpec((block // 2, width), lambda i: (i, 0)),
            pl.BlockSpec((block // 2, width), lambda i: (i, 0)),
        ],
        out_shape=[
            jax.ShapeDtypeStruct((tokens, hidden), jnp.bfloat16),
            jax.ShapeDtypeStruct((tokens, hidden), jnp.float32),
            jax.ShapeDtypeStruct((tokens // 2, width), jnp.bfloat16),
            jax.ShapeDtypeStruct((tokens // 2, width), jnp.bfloat16),
        ],
        compiler_params=pltpu.CompilerParams(vmem_limit_bytes=VMEM_BYTES),
        cost_estimate=pl.CostEstimate(
            flops=4 * tokens * width * hidden, bytes_accessed=8 * tokens * width, transcendentals=0
        ),
        name="mlp_forward",
    )(rows, up_full, up_bias[None], down_full)


def mlp_backward_kernel(
    one_ref, two_ref, slope_ref, down_ref, up_ref, whole_ref, pre_ref, part_ref, sums_ref
):
    half = one_ref.shape[1]
    whole_ref[:half, :] = one_ref[0]
    whole_ref[half:, :] = two_ref[0]
    hidden = slope_ref.shape[1]

    @pl.when(pl.program_id(0) == 0)
    def _():
        sums_ref[...] = jnp.zeros_like(sums_ref)

    for first in range(0, hidden, MLP_TILE):
        cols = slice(first, first + MLP_TILE)
        grad = lax.dot_general(
            whole_ref[...], down_ref[cols, :], NT, preferred_element_type=jnp.float32
        )
        pre = (grad * slope_ref[:, cols]).astype(jnp.bfloat16)
        pre_ref[:, cols] = pre
        sums_ref[:, cols] += jnp.sum(pre.astype(jnp.float32).reshape(-1, 8, MLP_TILE), axis=0)
    part_ref[...] = lax.dot_general(
        pre_ref[...], up_ref[...], NT, preferred_element_type=jnp.float32
    ).astype(jnp.bfloat16)


def mlp_backward(one, two, slope, down_full, up_full):
    ranks, half, width = one.shape
    rows = 2 * half
    hidden = slope.shape[1]
    tokens = ranks * rows
    return pl.pallas_call(
        mlp_backward_kernel,
        grid=(ranks,),
        in_specs=[
            pl.BlockSpec((1, half, width), lambda i: (i, 0, 0)),
            pl.BlockSpec((1, half, width), lambda i: (i, 0, 0)),
            pl.BlockSpec((rows, hidden), lambda i: (i, 0)),
            resident((hidden, width)),
            resident((width, hidden)),
        ],
        out_specs=[
            pl.BlockSpec((rows, width), lambda i: (i, 0)),
            pl.BlockSpec((rows, hidden), lambda i: (i, 0)),
            pl.BlockSpec((rows, width), lambda i: (i, 0)),
            pl.BlockSpec((8, hidden), lambda i: (0, 0)),
        ],
        out_shape=[
            jax.ShapeDtypeStruct((tokens, width), jnp.bfloat16),
            jax.ShapeDtypeStruct((tokens, hidden), jnp.bfloat16),
            jax.ShapeDtypeStruct((tokens, width), jnp.bfloat16),
            jax.ShapeDtypeStruct((8, hidden), jnp.float32),
        ],
        compiler_params=pltpu.CompilerParams(vmem_limit_bytes=VMEM_BYTES),
        cost_estimate=pl.CostEstimate(
            flops=4 * tokens * width * hidden, bytes_accessed=10 * tokens * width, transcendentals=0
        ),
        name="mlp_backward",
    )(one, two, slope, down_full, up_full)


def over_dp(grad, dimension):
    return lax.psum_scatter(grad, "dp", scatter_dimension=dimension, tiled=True)


def layer(
    layer_input,
    segment_ids,
    first_gain,
    first_shift,
    qkv_weight,
    query_value_bias,
    dense_weight,
    dense_bias,
    second_gain,
    second_shift,
    up_weight,
    up_bias,
    down_weight,
    down_bias,
    out_grad,
):
    rows, width = layer_input.shape
    ranks = lax.axis_size("tensor")
    tokens = ranks * rows
    f32_rows = jax.ShapeDtypeStruct((rows, width), jnp.float32)

    qkv_all = lax.all_gather(qkv_weight, "dp", axis=0, tiled=False)
    dense_all = lax.all_gather(dense_weight, "dp", axis=0, tiled=False)
    up_full = lax.all_gather(up_weight, "dp", axis=0, tiled=True)
    down_full = lax.all_gather(down_weight, "dp", axis=1, tiled=True)
    half = rows // 2
    out_one = lax.all_gather(out_grad[:half], "tensor", axis=0, tiled=False)
    out_two = lax.all_gather(out_grad[half:], "tensor", axis=0, tiled=False)

    head_width = qkv_all.shape[3]
    up_width = up_bias.shape[0]
    (whole1,) = line_call(
        norm_gather_kernel, 1,
        (layer_input, first_gain[None], first_shift[None]), (), rows, width, reduces=False,
    )
    whole1 = whole1.reshape(tokens, width)
    projected = project(whole1, qkv_all, query_value_bias)
    head_count = head_width // HEAD_DIM
    tensor_pos = lax.axis_index("tensor")
    global_heads = tensor_pos * head_count + jnp.arange(head_count, dtype=jnp.int32)
    slopes = jnp.power(2.0, -8.0 * (global_heads + 1).astype(jnp.float32) / HEADS)
    attended, log_sums = attention_forward(projected, segment_ids, slopes)
    whole2, residual = line_call(
        branch_norm_gather_kernel, 2,
        (attended, dense_all, layer_input, dense_bias[None], second_gain[None], second_shift[None]),
        (f32_rows,), rows, width, product=True,
    )
    whole2 = whole2.reshape(tokens, width)
    activated, slope, mlp_one, mlp_two = mlp_forward(whole2, rows, up_full, up_bias, down_full)
    out_whole, pre_grad, normed2_part, up_bias_sums = mlp_backward(
        out_one, out_two, slope, down_full, up_full
    )
    up_bias_part = jnp.sum(up_bias_sums, axis=0)
    down_grad = lax.dot_general(
        activated, out_whole, (((0,), (0,)), ((), ())), preferred_element_type=jnp.float32
    ).astype(jnp.bfloat16)
    normed2_part, down_grad = lax.optimization_barrier((normed2_part, down_grad))
    down_wgrad = over_dp(down_grad, 1)
    mlp_rows_one = lax.psum_scatter(mlp_one, "tensor", scatter_dimension=0, tiled=True)
    mlp_rows_two = lax.psum_scatter(mlp_two, "tensor", scatter_dimension=0, tiled=True)

    branch_whole, up_grad, residual_grad, second_sums = line_call(
        grad_gather_kernel, 3,
        (normed2_part.reshape(ranks, rows, width), whole2, residual, out_grad, second_gain[None], pre_grad),
        (
            jax.ShapeDtypeStruct((width, up_width), jnp.bfloat16),
            f32_rows,
            jax.ShapeDtypeStruct((4, 8, width), jnp.float32),
        ),
        rows, width, placed=(2, 1), more=Beside.scratch(tokens, width, up_width),
    )
    branch_whole = branch_whole.reshape(tokens, width)
    attended_grad, dense_grad = dense_backward(branch_whole, attended, dense_all)
    qkv_grad_cat = attention_backward(projected, attended_grad, segment_ids, slopes, log_sums)
    dense_wgrad = over_dp(dense_grad, 1)
    qkv_grad, qkv_sums = qkv_weight_grad(whole1, qkv_grad_cat)
    qkv_grad, qkv_grad_cat = lax.optimization_barrier((qkv_grad, qkv_grad_cat))
    qkv_wgrad = over_dp(qkv_grad, 1)
    qkv_sums = jnp.sum(qkv_sums, axis=1)
    part = width // ranks
    bias_rows = 2 * head_width // part
    up_rows = up_width // part
    own = jnp.concatenate([qkv_sums[0], qkv_sums[2], up_bias_part]).reshape(-1, part)
    own = jnp.pad(own, ((0, 8 - own.shape[0]), (0, 0)))
    f32_sums = jax.ShapeDtypeStruct((8, width), jnp.float32)
    groups = lax.axis_size("dp")
    up_block = (width // groups, up_width)
    up_parts, input_grad, early, own, late = line_call(
        grad_kernel, 4,
        (up_grad.reshape((groups,) + up_block), qkv_grad_cat, qkv_all, layer_input, residual_grad, first_gain[None], second_sums, own),
        (
            jax.ShapeDtypeStruct((groups,) + up_block, jnp.bfloat16),
            f32_rows,
            f32_sums,
            jax.ShapeDtypeStruct((8, part), jnp.float32),
            jax.ShapeDtypeStruct((2, width), jnp.float32),
        ),
        rows, width, gathers=False, product=True, sums=True, placed=(1, 1),
        more=Exchange.scratch(groups, up_block),
    )
    down_wgrad, up_wgrad, dense_wgrad, qkv_wgrad, layer_out, input_grad = finish(
        down_wgrad, up_parts, dense_wgrad, qkv_wgrad,
        mlp_rows_one, mlp_rows_two, residual, down_bias, input_grad,
    )
    return (
        layer_out,
        input_grad,
        late[0],
        late[1],
        qkv_wgrad,
        own[:bias_rows].reshape(2, head_width),
        dense_wgrad,
        early[2],
        early[0],
        early[1],
        up_wgrad,
        own[bias_rows : bias_rows + up_rows].reshape(up_width),
        down_wgrad,
        early[3],
    )


def solution(mesh):
    token_rows = P(("dp", "tensor"), None)
    placed = (
        token_rows,
        P("dp"),
        P(),
        P(),
        P(None, "dp", "tensor"),
        P(None, "tensor"),
        P("tensor", "dp"),
        P(),
        P(),
        P(),
        P("dp", "tensor"),
        P("tensor"),
        P("tensor", "dp"),
        P(),
        token_rows,
    )
    return jax.shard_map(
        layer,
        mesh=mesh,
        in_specs=placed,
        out_specs=(
            token_rows,
            token_rows,
            P(),
            P(),
            P(None, "dp", "tensor"),
            P(None, "tensor"),
            P("tensor", "dp"),
            P(),
            P(),
            P(),
            P("dp", "tensor"),
            P("tensor"),
            P("tensor", "dp"),
            P(),
        ),
        check_vma=False,
    )
```

```python
import functools
import math

import jax
import jax.numpy as jnp
from jax import lax
from jax.experimental import pallas as pl
from jax.experimental.pallas import tpu as pltpu
from jax.sharding import PartitionSpec as P


HEADS = 32
EPSILON = 1e-05
MESH = pl.DeviceIdType.MESH
HEAD_DIM = 64
PAIR = 2 * HEAD_DIM
Q_BLOCK = 256
MASKED = -1e32
VMEM_BYTES = 67043328
NT = (((1,), (1,)), ((), ()))
NN = (((1,), (0,)), ((), ()))


def key_window(seq_len, block):
    width = min(seq_len, Q_BLOCK + seq_len // 4)
    start = jnp.maximum(block * Q_BLOCK + Q_BLOCK - width, 0)
    return width, pl.multiple_of(start, 128)


def masked_distance(seg_row, seg_col, first_query, first_key, width):
    shape = (width, Q_BLOCK)
    key_pos = lax.broadcasted_iota(jnp.int32, shape, 0) + first_key
    query_pos = lax.broadcasted_iota(jnp.int32, shape, 1) + first_query
    delta = key_pos - query_pos
    allowed = (seg_col == seg_row) & (delta <= 0)
    return jnp.where(allowed, delta.astype(jnp.float32), MASKED)


def half_lanes(rows, half):
    lane = lax.broadcasted_iota(jnp.int32, rows.shape, 1)
    return jnp.where((lane < HEAD_DIM) == (half == 0), rows, jnp.zeros_like(rows))


def forward_kernel(slope_ref, proj_ref, seg_row_ref, seg_col_ref, out_ref, lse_ref, value_t, bias_ref):
    seq_len = proj_ref.shape[0]
    width_all = out_ref.shape[1]
    block = pl.program_id(0)

    @pl.when(block == 0)
    def _():
        value_t[...] = proj_ref[:, 2 * width_all :].T

    first = pl.multiple_of(block * Q_BLOCK, Q_BLOCK)
    width, start = key_window(seq_len, block)
    queries = pl.ds(first, Q_BLOCK)
    keys = pl.ds(start, width)
    bias_ref[...] = masked_distance(
        seg_row_ref[:, queries], seg_col_ref[keys, :], first, start, width
    )
    for pair in range(width_all // PAIR):
        cols = pair * PAIR
        query_pair = proj_ref[queries, cols : cols + PAIR] * 0.125
        key_pair = proj_ref[keys, width_all + cols : width_all + cols + PAIR]
        value_pair = value_t[cols : cols + PAIR, keys]
        mixed = []
        for half in range(2):
            head = 2 * pair + half
            scores = lax.dot_general(
                key_pair, half_lanes(query_pair, half), NT, preferred_element_type=jnp.float32
            )
            scores = scores + slope_ref[head] * bias_ref[...]
            highest = jnp.max(scores, axis=0, keepdims=True)
            exponent = jnp.exp(scores - highest)
            total = jnp.sum(exponent, axis=0, keepdims=True)
            part = lax.dot_general(
                value_pair[half * HEAD_DIM : (half + 1) * HEAD_DIM],
                exponent.astype(jnp.bfloat16),
                NN,
                preferred_element_type=jnp.float32,
            )
            mixed.append(part / total)
            lse_ref[head : head + 1, :] = highest + jnp.log(total)
        out_ref[:, cols : cols + PAIR] = jnp.concatenate(mixed, axis=0).T.astype(jnp.bfloat16)


def attention_forward(projected, segments, slopes):
    seq_len, all_cols = projected.shape
    cols = all_cols // 3
    heads = cols // HEAD_DIM
    width = min(seq_len, Q_BLOCK + seq_len // 4)
    return pl.pallas_call(
        forward_kernel,
        grid=(seq_len // Q_BLOCK,),
        in_specs=[
            pl.BlockSpec(memory_space=pltpu.SMEM),
            pl.BlockSpec((seq_len, all_cols), lambda i: (0, 0)),
            pl.BlockSpec((1, seq_len), lambda i: (0, 0)),
            pl.BlockSpec((seq_len, 1), lambda i: (0, 0)),
        ],
        out_specs=[
            pl.BlockSpec((Q_BLOCK, cols), lambda i: (i, 0)),
            pl.BlockSpec((heads, Q_BLOCK), lambda i: (0, i)),
        ],
        out_shape=[
            jax.ShapeDtypeStruct((seq_len, cols), jnp.bfloat16),
            jax.ShapeDtypeStruct((heads, seq_len), jnp.float32),
        ],
        scratch_shapes=[
            pltpu.VMEM((cols, seq_len), jnp.bfloat16),
            pltpu.VMEM((width, Q_BLOCK), jnp.float32),
        ],
        compiler_params=pltpu.CompilerParams(vmem_limit_bytes=VMEM_BYTES),
        cost_estimate=pl.CostEstimate(flops=4 * seq_len * width * cols, bytes_accessed=6 * seq_len * cols, transcendentals=0),
        name="attention_forward",
    )(slopes, projected, segments[None, :], segments[:, None])


def backward_kernel(slope_ref, proj_ref, grad_ref, lse_ref, seg_row_ref, seg_col_ref, out_ref,
                    key_t, bias_ref, key_sum, value_sum):
    seq_len = proj_ref.shape[0]
    width_all = grad_ref.shape[1]
    block = pl.program_id(0)

    @pl.when(block == 0)
    def _():
        key_t[...] = proj_ref[:, width_all : 2 * width_all].T
        key_sum[...] = jnp.zeros_like(key_sum)
        value_sum[...] = jnp.zeros_like(value_sum)

    first = pl.multiple_of(block * Q_BLOCK, Q_BLOCK)
    width, start = key_window(seq_len, block)
    queries = pl.ds(first, Q_BLOCK)
    keys = pl.ds(start, width)
    bias_ref[...] = masked_distance(
        seg_row_ref[:, queries], seg_col_ref[keys, :], first, start, width
    )
    for pair in range(width_all // PAIR):
        cols = pair * PAIR
        query_pair = proj_ref[queries, cols : cols + PAIR] * 0.125
        key_pair = proj_ref[keys, width_all + cols : width_all + cols + PAIR]
        value_pair = proj_ref[keys, 2 * width_all + cols : 2 * width_all + cols + PAIR]
        grad_pair = grad_ref[queries, cols : cols + PAIR]
        query_grads = []
        key_part = value_part = None
        for half in range(2):
            head = 2 * pair + half
            query_half = half_lanes(query_pair, half)
            grad_half = half_lanes(grad_pair, half)
            scores = lax.dot_general(key_pair, query_half, NT, preferred_element_type=jnp.float32)
            probs = jnp.exp(scores + slope_ref[head] * bias_ref[...] - lse_ref[head : head + 1, queries])
            prob_grad = lax.dot_general(value_pair, grad_half, NT, preferred_element_type=jnp.float32)
            inner = jnp.sum(probs * prob_grad, axis=0, keepdims=True)
            score_grad = (probs * (prob_grad - inner)).astype(jnp.bfloat16)
            value_half = jnp.dot(probs.astype(jnp.bfloat16), grad_half, preferred_element_type=jnp.float32)
            key_half = jnp.dot(score_grad, query_half, preferred_element_type=jnp.float32)
            query_grads.append(
                jnp.dot(
                    key_t[cols + half * HEAD_DIM : cols + (half + 1) * HEAD_DIM, keys],
                    score_grad,
                    preferred_element_type=jnp.float32,
                )
                * 0.125
            )
            value_part = value_half if half == 0 else value_part + value_half
            key_part = key_half if half == 0 else key_part + key_half
        key_sum[keys, cols : cols + PAIR] += key_part
        value_sum[keys, cols : cols + PAIR] += value_part
        out_ref[queries, cols : cols + PAIR] = (
            jnp.concatenate(query_grads, axis=0).T.astype(jnp.bfloat16)
        )

    @pl.when(block == pl.num_programs(0) - 1)
    def _():
        out_ref[:, width_all : 2 * width_all] = key_sum[...].astype(jnp.bfloat16)
        out_ref[:, 2 * width_all :] = value_sum[...].astype(jnp.bfloat16)


def attention_backward(projected, head_grad, segments, slopes, log_sums):
    seq_len, all_cols = projected.shape
    cols = all_cols // 3
    heads = cols // HEAD_DIM
    width = min(seq_len, Q_BLOCK + seq_len // 4)
    return pl.pallas_call(
        backward_kernel,
        grid=(seq_len // Q_BLOCK,),
        in_specs=[
            pl.BlockSpec(memory_space=pltpu.SMEM),
            pl.BlockSpec((seq_len, all_cols), lambda i: (0, 0)),
            pl.BlockSpec((seq_len, cols), lambda i: (0, 0)),
            pl.BlockSpec((heads, seq_len), lambda i: (0, 0)),
            pl.BlockSpec((1, seq_len), lambda i: (0, 0)),
            pl.BlockSpec((seq_len, 1), lambda i: (0, 0)),
        ],
        out_specs=pl.BlockSpec((seq_len, all_cols), lambda i: (0, 0)),
        out_shape=jax.ShapeDtypeStruct((seq_len, all_cols), jnp.bfloat16),
        scratch_shapes=[
            pltpu.VMEM((cols, seq_len), jnp.bfloat16),
            pltpu.VMEM((width, Q_BLOCK), jnp.float32),
            pltpu.VMEM((seq_len, cols), jnp.float32),
            pltpu.VMEM((seq_len, cols), jnp.float32),
        ],
        compiler_params=pltpu.CompilerParams(vmem_limit_bytes=VMEM_BYTES),
        cost_estimate=pl.CostEstimate(flops=10 * seq_len * width * cols, bytes_accessed=14 * seq_len * cols, transcendentals=0),
        name="attention_backward",
    )(slopes, projected, head_grad, log_sums, segments[None, :], segments[:, None])


ROW_TILE = 16
SUBS = 4
LAG = 0


def remote(src, dst, send_sem, recv_sem, peer):
    return pltpu.make_async_remote_copy(
        src_ref=src,
        dst_ref=dst,
        send_sem=send_sem,
        recv_sem=recv_sem,
        device_id={"tensor": peer},
        device_id_type=MESH,
    )


class Line:
    def __init__(self, chips, rows):
        self.chips = chips
        self.sub_rows = rows // SUBS
        self.me = lax.axis_index("tensor")
        self.place = self.me // 2
        self.core = self.me % 2
        self.above = self.me + 2
        self.below = self.me - 2
        self.partner = self.me + 1 - 2 * self.core
        self.has_above = self.place < chips - 1
        self.has_below = self.place > 0

    def rows(self, sub):
        return pl.ds(pl.multiple_of(sub * self.sub_rows, self.sub_rows), self.sub_rows)

    def tile(self, sub, tile):
        return pl.ds(pl.multiple_of(sub * self.sub_rows + tile * ROW_TILE, ROW_TILE), ROW_TILE)

    def enter(self, with_groups=False):
        barrier = pltpu.get_barrier_semaphore()
        groups = lax.axis_size("dp") if with_groups else 1
        for step in range(1, groups):
            peer = lax.rem(lax.axis_index("dp") + step, groups)
            pl.semaphore_signal(barrier, inc=1, device_id={"dp": peer}, device_id_type=MESH)

        def greet(peer):
            pl.semaphore_signal(barrier, inc=1, device_id={"tensor": peer}, device_id_type=MESH)

        pl.when(self.has_above)(lambda: greet(self.above))
        pl.when(self.has_below)(lambda: greet(self.below))
        greet(self.partner)
        pl.semaphore_wait(
            barrier, groups + self.has_above.astype(jnp.int32) + self.has_below.astype(jnp.int32)
        )


class Gather:
    def __init__(self, line, source, target, sems):
        self.line, self.source, self.target = line, source, target
        self.own_sem, self.line_send, self.line_recv, self.pair_send, self.pair_recv = sems

    @staticmethod
    def scratch(chips):
        dma = pltpu.SemaphoreType.DMA
        return [
            dma((SUBS,)),
            dma((2, chips, SUBS)),
            dma((2, chips, SUBS)),
            dma((chips, SUBS)),
            dma((chips, SUBS)),
        ]

    def hop(self, way, step, sub, src, block):
        peer = self.line.above if way == 0 else self.line.below
        return remote(
            src,
            self.target.at[block, self.line.rows(sub)],
            self.line_send.at[way, step, sub],
            self.line_recv.at[way, step, sub],
            peer,
        )

    def across(self, chip, sub, src, block):
        return remote(
            src,
            self.target.at[block, self.line.rows(sub)],
            self.pair_send.at[chip, sub],
            self.pair_recv.at[chip, sub],
            self.line.partner,
        )

    def own(self, sub):
        return pltpu.make_async_copy(
            self.source.at[self.line.rows(sub)],
            self.target.at[self.line.me, self.line.rows(sub)],
            self.own_sem.at[sub],
        )

    def start(self, sub):
        line = self.line
        src = self.source.at[line.rows(sub)]
        pl.when(line.has_above)(lambda: self.hop(0, 0, sub, src, line.me).start())
        pl.when(line.has_below)(lambda: self.hop(1, 0, sub, src, line.me).start())
        self.across(line.place, sub, src, line.me).start()
        self.own(sub).start()

    def step(self, sub, step, live):
        line = self.line
        for way, sign in ((0, -1), (1, 1)):
            block = line.me + 2 * sign * (step + 1)
            onward = line.has_above if way == 0 else line.has_below
            inside = block >= 0 if way == 0 else block < 2 * line.chips

            @pl.when(live & inside)
            def _():
                src = self.target.at[block, line.rows(sub)]
                self.hop(way, step, sub, src, block).wait_recv()

                @pl.when(onward)
                def _():
                    self.hop(way, step + 1, sub, src, block).start()

                self.across(block // 2, sub, src, block).start()

    def finish(self):
        line = self.line

        @pl.loop(0, SUBS)
        def _(sub):
            src = self.source.at[line.rows(sub)]
            for chip in range(line.chips):
                copy = self.across(chip, sub, src, 2 * chip + 1 - line.core)
                copy.wait_recv()
                copy.wait_send()
            for step in range(line.chips - 1):
                sent_up = line.has_above & (line.place >= step)
                sent_down = line.has_below & (line.place + step < line.chips)
                pl.when(sent_up)(lambda: self.hop(0, step, sub, src, line.me).wait_send())
                pl.when(sent_down)(lambda: self.hop(1, step, sub, src, line.me).wait_send())
            self.own(sub).wait()


class Reduce:
    def __init__(self, line, partial, bufs, sems, product=None):
        self.line, self.partial, self.product = line, partial, product
        self.held, self.paired, self.from_below, self.from_above = bufs
        self.held_sem, self.pair_send, self.pair_recv, self.line_send, self.line_recv = sems

    @staticmethod
    def scratch(chips, rows, width):
        dma = pltpu.SemaphoreType.DMA
        return [pltpu.VMEM((chips, rows, width), jnp.bfloat16)] * 4 + [
            dma((chips, SUBS)),
            dma((chips, SUBS)),
            dma((chips, SUBS)),
            dma((2, chips, SUBS)),
            dma((2, chips, SUBS)),
        ]

    def load(self, chip, sub):
        rows = self.line.rows(sub)
        return pltpu.make_async_copy(
            self.partial.at[2 * chip + self.line.core, rows],
            self.held.at[chip, rows],
            self.held_sem.at[chip, sub],
        )

    def across(self, chip, sub):
        rows = self.line.rows(sub)
        block = chip if self.product is not None else 2 * chip + 1 - self.line.core
        return remote(
            self.partial.at[block, rows],
            self.paired.at[chip, rows],
            self.pair_send.at[chip, sub],
            self.pair_recv.at[chip, sub],
            self.line.partner,
        )

    def hop(self, way, chip, sub):
        rows = self.line.rows(sub)
        return remote(
            self.held.at[chip, rows],
            (self.from_below if way == 0 else self.from_above).at[chip, rows],
            self.line_send.at[way, chip, sub],
            self.line_recv.at[way, chip, sub],
            self.line.above if way == 0 else self.line.below,
        )

    def start(self):
        line = self.line
        order = []
        for step in range(line.chips):
            chip = line.chips - 1 - step // 2 if step % 2 == 0 else step // 2
            order.append(chip)

        if self.product is None:

            @pl.loop(0, SUBS)
            def _(sub):
                for chip in order:
                    self.across(chip, sub).start()
                    self.load(chip, sub).start()

        zeros = jnp.zeros((ROW_TILE, self.held.shape[2]), jnp.bfloat16)

        def clear(buf, chip):
            @pl.loop(0, self.held.shape[1] // ROW_TILE)
            def _(tile):
                buf[chip, pl.ds(pl.multiple_of(tile * ROW_TILE, ROW_TILE), ROW_TILE), :] = zeros

        pl.when(jnp.logical_not(line.has_below))(lambda: clear(self.from_below, 0))
        pl.when(jnp.logical_not(line.has_above))(lambda: clear(self.from_above, line.chips - 1))

    def multiply(self, slot):
        line = self.line

        @pl.when(slot < line.chips // 2)
        def _():
            chips = (line.chips - 1 - slot, slot)
            for chip in chips:
                self.product(2 * chip + 1 - line.core, self.partial, chip)

                @pl.loop(0, SUBS)
                def _(sub):
                    self.across(chip, sub).start()

            for chip in chips:
                self.product(2 * chip + line.core, self.held, chip)

    def step(self, way, sub, step, live):
        line = self.line
        chip = line.chips - 1 - step if way == 0 else step
        arrived = self.from_below if way == 0 else self.from_above
        inner = line.has_below if way == 0 else line.has_above

        @pl.when(live & (chip > line.place if way == 0 else chip < line.place))
        def _():
            if self.product is None:
                self.load(chip, sub).wait()
            self.across(chip, sub).wait_recv()

            def add(with_arrived):
                @pl.loop(0, line.sub_rows // ROW_TILE)
                def _(tile):
                    at = line.tile(sub, tile)
                    total = self.held[chip, at, :].astype(jnp.float32)
                    total = total + self.paired[chip, at, :].astype(jnp.float32)
                    if with_arrived:
                        total = total + arrived[chip, at, :].astype(jnp.float32)
                    self.held[chip, at, :] = total.astype(jnp.bfloat16)

            @pl.when(inner)
            def _():
                self.hop(way, chip, sub).wait_recv()
                add(True)

            pl.when(jnp.logical_not(inner))(lambda: add(False))
            self.hop(way, chip, sub).start()

    def arrive(self, sub):
        line = self.line
        place = line.place
        if self.product is None:
            self.load(place, sub).wait()
        self.across(place, sub).wait_recv()
        pl.when(line.has_below)(lambda: self.hop(0, place, sub).wait_recv())
        pl.when(line.has_above)(lambda: self.hop(1, place, sub).wait_recv())

    def total(self, at):
        place = self.line.place
        total = self.held[place, at, :].astype(jnp.float32)
        total = total + self.paired[place, at, :].astype(jnp.float32)
        total = total + self.from_below[place, at, :].astype(jnp.float32)
        return total + self.from_above[place, at, :].astype(jnp.float32)

    def finish(self):
        line = self.line

        @pl.loop(0, SUBS)
        def _(sub):
            for chip in range(line.chips):
                self.across(chip, sub).wait_send()
                pl.when(chip > line.place)(lambda: self.hop(0, chip, sub).wait_send())
                pl.when(chip < line.place)(lambda: self.hop(1, chip, sub).wait_send())


def for_tiles(line, sub, body):
    size = min(2 * ROW_TILE, line.sub_rows)

    @pl.loop(0, line.sub_rows // size)
    def _(tile):
        body(pl.ds(pl.multiple_of(sub * line.sub_rows + tile * size, size), size))


def run_gather(line, gather, rows_done):
    line.enter()
    steps = line.chips - 1

    @pl.loop(0, SUBS)
    def _(sub):
        for_tiles(line, sub, rows_done)
        gather.start(sub)

    @pl.loop(0, steps * SUBS)
    def _(at):
        gather.step(at % SUBS, at // SUBS, True)

    gather.finish()


def run_line(line, reduce, gather, rows_done, beside=None, entered=False):
    steps = line.chips - 1
    if not entered:
        line.enter()
    reduce.start()
    slots = steps * SUBS + LAG + (steps if gather is not None else 0) + 1

    @pl.loop(0, slots)
    def _(slot):
        if reduce.product is not None:
            reduce.multiply(slot)
        if beside is not None:
            beside(slot)
        for way in range(2):
            at = slot - (line.place if way == 0 else steps - line.place)
            sub = jnp.maximum(at, 0) // steps
            reduce.step(way, jnp.minimum(sub, SUBS - 1), jnp.maximum(at, 0) % steps, (at >= 0) & (sub < SUBS))
        at = slot - steps - LAG
        sub = jnp.maximum(at, 0) // steps

        @pl.when((at >= 0) & (at % steps == 0) & (sub < SUBS))
        def _():
            reduce.arrive(sub)
            for_tiles(line, sub, rows_done)
            if gather is not None:
                gather.start(sub)

        if gather is not None:
            at = slot - steps - LAG - 1
            sub = jnp.maximum(at, 0) // steps
            gather.step(
                jnp.minimum(sub, SUBS - 1), jnp.maximum(at, 0) % steps, (at >= 0) & (sub < SUBS)
            )

    reduce.finish()
    if gather is not None:
        gather.finish()


def unit_of(rows):
    centre = jnp.mean(rows, axis=1, keepdims=True)
    centred = rows - centre
    inv_std = lax.rsqrt(jnp.mean(centred * centred, axis=1, keepdims=True) + EPSILON)
    return centred * inv_std, inv_std


def norm_back(grad, unit, inv_std, gain):
    scaled = grad * gain
    return inv_std * (
        scaled
        - jnp.mean(scaled, axis=1, keepdims=True)
        - unit * jnp.mean(scaled * unit, axis=1, keepdims=True)
    )


def fold(rows):
    return jnp.sum(rows.reshape(-1, 8, rows.shape[1]), axis=0)


def norm_gather_kernel(chips, input_ref, gain_ref, shift_ref, whole_ref, normed_ref, *sems):
    line = Line(chips, input_ref.shape[0])
    gather = Gather(line, normed_ref, whole_ref, sems)

    def rows_done(at):
        unit, _ = unit_of(input_ref[at, :].astype(jnp.float32))
        normed_ref[at, :] = (unit * gain_ref[...] + shift_ref[...]).astype(jnp.bfloat16)

    run_gather(line, gather, rows_done)


def branch_norm_gather_kernel(
    chips, attended_ref, dense_ref, input_ref, bias_ref, gain_ref, shift_ref, whole_ref, residual_ref, normed_ref, mirror, *rest
):
    line = Line(chips, input_ref.shape[0])
    rows = input_ref.shape[0]
    parts, _, part = dense_ref.shape

    def product(block, target, slot):
        source = attended_ref[pl.ds(pl.multiple_of(block * rows, rows), rows), :]
        for index in range(parts):
            target[slot, :, index * part : (index + 1) * part] = jnp.dot(
                source, dense_ref[index], preferred_element_type=jnp.float32
            ).astype(jnp.bfloat16)

    reduce = Reduce(line, mirror, rest[:4], rest[4:9], product)
    gather = Gather(line, normed_ref, whole_ref, rest[9:])

    def rows_done(at):
        residual = input_ref[at, :].astype(jnp.float32) + (reduce.total(at) + bias_ref[...])
        residual_ref[at, :] = residual
        unit, _ = unit_of(residual)
        normed_ref[at, :] = (unit * gain_ref[...] + shift_ref[...]).astype(jnp.bfloat16)

    run_line(line, reduce, gather, rows_done)


class Beside:
    def __init__(self, whole, pre, parts, scratch):
        self.whole, self.pre, self.parts = whole, pre, parts
        self.loaded, self.stored, self.load_sem, self.send_sem, self.recv_sem = scratch
        self.count, self.block = self.stored.shape[:2]
        self.groups = parts.shape[0]
        self.group = lax.axis_index("dp")
        self.each = self.count // self.groups

    @staticmethod
    def scratch(tokens, width, hidden, groups):
        block = min(256, width // groups)
        count = width // block
        dma = pltpu.SemaphoreType.DMA
        return [
            pltpu.VMEM((2, tokens, block), jnp.bfloat16),
            pltpu.VMEM((count, block, hidden), jnp.bfloat16),
            dma((2,)),
            dma((count,)),
            dma((count,)),
        ]

    def place(self, index):
        return lax.rem(index + self.group * self.each, self.count)

    def load(self, index):
        columns = pl.ds(pl.multiple_of(self.place(index) * self.block, self.block), self.block)
        return pltpu.make_async_copy(
            self.whole.at[:, columns], self.loaded.at[index % 2], self.load_sem.at[index % 2]
        )

    def target(self, source, within):
        return self.parts.at[source, pl.ds(pl.multiple_of(within * self.block, self.block), self.block)]

    def keep(self, index):
        return pltpu.make_async_copy(
            self.stored.at[index], self.target(self.group, index), self.send_sem.at[index]
        )

    def send(self, index, source, peer):
        within = index % self.each
        return pltpu.make_async_remote_copy(
            src_ref=self.stored.at[index],
            dst_ref=self.target(source, within),
            send_sem=self.send_sem.at[index],
            recv_sem=self.recv_sem.at[source * self.each + within],
            device_id={"dp": peer},
            device_id_type=MESH,
        )

    def peer(self, index):
        return lax.rem(index // self.each + self.group, self.groups)

    def start(self):
        self.load(0).start()

    def slot(self, slot):
        index = slot - 1

        @pl.when((index >= 0) & (index < self.count))
        def _():
            self.load(index).wait()
            pl.when(index + 1 < self.count)(lambda: self.load(index + 1).start())
            self.stored[index] = lax.dot_general(
                self.loaded[index % 2],
                self.pre[...],
                (((0,), (0,)), ((), ())),
                preferred_element_type=jnp.float32,
            ).astype(jnp.bfloat16)

            pl.when(index < self.each)(lambda: self.keep(index).start())
            pl.when(index >= self.each)(
                lambda: self.send(index, self.group, self.peer(index)).start()
            )

    def finish(self):
        for index in range(self.each):
            self.keep(index).wait()
        for index in range(self.each, self.count):
            source = self.peer(index)
            self.send(index, source, source).wait_recv()
            self.send(index, self.group, source).wait_send()


def grad_gather_kernel(
    chips, partial_ref, whole_in_ref, residual_ref, grad_ref, gain_ref, pre_ref,
    whole_ref, up_parts_ref, residual_grad_ref, sums_ref, branch_ref, *rest
):
    line = Line(chips, grad_ref.shape[0])
    reduce = Reduce(line, partial_ref, rest[:4], rest[4:9])
    gather = Gather(line, branch_ref, whole_ref, rest[9:14])
    beside = Beside(whole_in_ref, pre_ref, up_parts_ref, rest[14:])
    sums_ref[...] = jnp.zeros_like(sums_ref)

    def rows_done(at):
        unit, inv_std = unit_of(residual_ref[at, :])
        grad = reduce.total(at)
        out_grad = grad_ref[at, :].astype(jnp.float32)
        residual_grad = out_grad + norm_back(grad, unit, inv_std, gain_ref[...])
        residual_grad_ref[at, :] = residual_grad
        branch = residual_grad.astype(jnp.bfloat16)
        branch_ref[at, :] = branch
        sums_ref[0] += fold(grad * unit)
        sums_ref[1] += fold(grad)
        sums_ref[2] += fold(branch.astype(jnp.float32))
        sums_ref[3] += fold(out_grad)

    beside.start()
    line.enter(True)
    run_line(line, reduce, gather, rows_done, beside.slot, True)
    beside.finish()


def grad_kernel(
    chips, grad_cat_ref, weight_ref, input_ref, residual_grad_ref, gain_ref, first_ref, second_ref, own_ref,
    out_ref, sums_ref, own_out_ref, mirror, *rest
):
    line = Line(chips, input_ref.shape[0])
    rows = input_ref.shape[0]
    parts, three, part, head_width = weight_ref.shape

    def product(block, target, slot):
        at = pl.ds(pl.multiple_of(block * rows, rows), rows)
        for index in range(parts):
            total = None
            for kind in range(three):
                term = lax.dot_general(
                    grad_cat_ref[at, kind * head_width : (kind + 1) * head_width],
                    weight_ref[index, kind],
                    NT,
                    preferred_element_type=jnp.float32,
                )
                total = term if kind == 0 else total + term
            target[slot, :, index * part : (index + 1) * part] = total.astype(jnp.bfloat16)

    reduce = Reduce(line, mirror, rest[:4], rest[4:9], product)
    sums = Sums(2 * chips, first_ref, second_ref, own_ref, sums_ref, own_out_ref, rest[9:])

    def rows_done(at):
        unit, inv_std = unit_of(input_ref[at, :].astype(jnp.float32))
        grad = reduce.total(at)
        out_ref[at, :] = residual_grad_ref[at, :] + norm_back(grad, unit, inv_std, gain_ref[...])

    sums.greet()
    run_line(line, reduce, None, rows_done, sums.beside, True)
    sums.close()


class Sums:
    def __init__(self, ranks, first_ref, second_ref, own_ref, out_ref, own_out_ref, scratch):
        self.ranks = ranks
        self.groups = lax.axis_size("dp")
        self.me = lax.axis_index("tensor")
        self.group = lax.axis_index("dp")
        self.early, self.late, self.own = first_ref, second_ref, own_ref
        self.early_out, self.own_out = out_ref, own_out_ref
        self.mine, self.first, self.stage, self.second = scratch[:4]
        self.sems = scratch[4:]
        self.part = self.mine.shape[1] // ranks

    @staticmethod
    def scratch(ranks, groups, width):
        part = width // ranks
        f32 = jnp.float32
        dma = pltpu.SemaphoreType.DMA
        return [
            pltpu.VMEM((8, width), f32),
            pltpu.VMEM((ranks, 8, part), f32),
            pltpu.VMEM((16, part), f32),
            pltpu.VMEM((groups, 16, part), f32),
        ] + [dma((ranks,)), dma((ranks,)), dma((groups,)), dma((groups,)), dma((ranks,)), dma((ranks,))]

    def rank(self, step):
        return lax.rem(self.me + step, self.ranks)

    def peer(self, step):
        return lax.rem(self.group + step, self.groups)

    def columns(self, rank):
        return pl.ds(pl.multiple_of(rank * self.part, self.part), self.part)

    def greet(self):
        barrier = pltpu.get_barrier_semaphore()
        for step in range(1, self.ranks):
            pl.semaphore_signal(
                barrier, inc=1, device_id={"tensor": self.rank(step)}, device_id_type=MESH
            )
        for step in range(1, self.groups):
            pl.semaphore_signal(
                barrier, inc=1, device_id={"dp": self.peer(step)}, device_id_type=MESH
            )
        pl.semaphore_wait(barrier, self.ranks + self.groups - 2)

    def copy(self, stage, src, dst, sem, slot, axis, peer):
        return pltpu.make_async_remote_copy(
            src_ref=src,
            dst_ref=dst,
            send_sem=self.sems[2 * stage].at[sem],
            recv_sem=self.sems[2 * stage + 1].at[slot],
            device_id={axis: peer},
            device_id_type=MESH,
        )

    def scatter(self, peer, slot, sem):
        return self.copy(0, self.mine.at[:, self.columns(peer)], self.first.at[slot], sem, slot, "tensor", peer)

    def exchange(self, peer, slot, sem):
        return self.copy(1, self.stage, self.second.at[slot], sem, slot, "dp", peer)

    def spread(self, peer, rank, sem):
        return self.copy(
            2, self.early_out.at[:, self.columns(self.me)], self.early_out.at[:, self.columns(rank)],
            sem, rank, "tensor", peer,
        )

    def beside(self, slot):
        @pl.when(slot == 1)
        def _():
            self.mine[...] = self.early[...]
            for row in range(self.late.shape[0]):
                self.mine[row + 2 : row + 3, :] = jnp.sum(self.late[row], axis=0, keepdims=True)
            for step in range(1, self.ranks):
                self.scatter(self.rank(step), self.me, step).start()
            self.first[self.me] = self.mine[:, self.columns(self.me)]

        @pl.when(slot == 4)
        def _():
            for step in range(1, self.ranks):
                self.scatter(self.rank(step), self.rank(step), step).wait_recv()
            total = self.first[0]
            for rank in range(1, self.ranks):
                total = total + self.first[rank]
            self.stage[:8, :] = total
            self.stage[8:, :] = self.own[...]
            for step in range(1, self.groups):
                self.exchange(self.peer(step), self.group, step).start()
            self.second[self.group] = self.stage[...]

        @pl.when(slot == 7)
        def _():
            for step in range(1, self.groups):
                self.exchange(self.peer(step), self.peer(step), step).wait_recv()
            total = self.second[0]
            for index in range(1, self.groups):
                total = total + self.second[index]
            self.early_out[:, self.columns(self.me)] = total[:8]
            self.own_out[...] = total[8:]
            for step in range(1, self.ranks):
                self.spread(self.rank(step), self.me, step).start()

    def close(self):
        for step in range(1, self.ranks):
            self.spread(self.rank(step), self.rank(step), step).wait_recv()
            self.scatter(self.rank(step), self.me, step).wait_send()
            self.spread(self.rank(step), self.me, step).wait_send()
        for step in range(1, self.groups):
            self.exchange(self.peer(step), self.group, step).wait_send()


def line_call(kernel, collective_id, operands, outs, rows, width, gathers=True, reduces=True, product=False, sums=False, placed=(), more=()):
    ranks = lax.axis_size("tensor")
    chips = ranks // 2
    whole = jax.ShapeDtypeStruct((ranks, rows, width), jnp.bfloat16)
    in_vmem = pl.BlockSpec(memory_space=pltpu.VMEM)
    in_place = pl.BlockSpec(memory_space=pl.ANY)
    ins_placed, outs_placed = placed or (0, 0)
    scratch = []
    if gathers:
        scratch.append(pltpu.VMEM((rows, width), jnp.bfloat16))
    if product:
        scratch.append(pltpu.VMEM((chips, rows, width), jnp.bfloat16))
    if reduces:
        scratch += Reduce.scratch(chips, rows, width)
    if gathers:
        scratch += Gather.scratch(chips)
    if sums:
        scratch += Sums.scratch(ranks, lax.axis_size("dp"), width)
    scratch += list(more)
    return pl.pallas_call(
        functools.partial(kernel, chips),
        in_specs=[in_place] * ins_placed + [in_vmem] * (len(operands) - ins_placed),
        out_specs=[in_place] * (outs_placed + int(gathers)) + [in_vmem] * (len(outs) - outs_placed),
        out_shape=([whole] if gathers else []) + list(outs),
        scratch_shapes=scratch,
        compiler_params=pltpu.CompilerParams(
            collective_id=collective_id, has_side_effects=True, vmem_limit_bytes=VMEM_BYTES
        ),
        cost_estimate=pl.CostEstimate(
            flops=8 * rows * width * 100, bytes_accessed=100 * rows * width, transcendentals=0
        ),
    )(*operands)


def columns_of(row, count):
    return jnp.broadcast_to(row, (128, row.shape[1])).T[:, :count]


def qkv_grad_kernel(rows_ref, grad_ref, weight_ref, norm_ref, out_ref, sums_ref, first_ref, total):
    head_width = out_ref.shape[2]

    @pl.when(pl.program_id(0) == 0)
    def _():
        for kind in range(3):
            cols = slice(kind * head_width, (kind + 1) * head_width)
            parts = jnp.sum(
                grad_ref[:, cols].astype(jnp.float32).reshape(-1, 8, head_width), axis=0
            )
            sums_ref[kind] = parts
            total[kind] = jnp.broadcast_to(jnp.sum(parts, axis=0, keepdims=True), parts.shape)

    product = lax.dot_general(
        rows_ref[...], grad_ref[...], (((0,), (0,)), ((), ())), preferred_element_type=jnp.float32
    )
    gain = columns_of(norm_ref[0:1, :], 1)
    shift = columns_of(norm_ref[1:2, :], 1)
    gain_sum = shift_sum = None
    for kind in range(3):
        part = product[:, kind * head_width : (kind + 1) * head_width]
        out_ref[kind] = part.astype(jnp.bfloat16)
        weight = weight_ref[0, kind].astype(jnp.float32)
        sums = total[kind, 0:1, :]
        shift_term = jnp.sum(weight * sums, axis=1, keepdims=True)
        gain_term = jnp.sum(weight * (part - shift * sums), axis=1, keepdims=True)
        gain_sum = gain_term if kind == 0 else gain_sum + gain_term
        shift_sum = shift_term if kind == 0 else shift_sum + shift_term
    lane = lax.broadcasted_iota(jnp.int32, (product.shape[0], 128), 1)
    both = jnp.where(lane == 0, gain_sum / gain, jnp.where(lane == 1, shift_sum, 0.0))
    first_ref[...] = both.T[:8]


def qkv_weight_grad(whole, grad_cat, qkv_all, gain, shift):
    tokens, width = whole.shape
    part, head_width = qkv_all.shape[2:]
    block = min(256, part)
    each = part // block
    norm = jnp.stack([gain, shift])
    return pl.pallas_call(
        qkv_grad_kernel,
        grid=(width // block,),
        in_specs=[
            pl.BlockSpec((tokens, block), lambda i: (0, i)),
            pl.BlockSpec(grad_cat.shape, lambda i: (0, 0)),
            pl.BlockSpec((1, 3, block, head_width), lambda i: (i // each, 0, i % each, 0)),
            pl.BlockSpec((2, block), lambda i: (0, i)),
        ],
        out_specs=[
            pl.BlockSpec((3, block, head_width), lambda i: (0, i, 0)),
            pl.BlockSpec((3, 8, head_width), lambda i: (0, 0, 0)),
            pl.BlockSpec((8, block), lambda i: (0, i)),
        ],
        out_shape=[
            jax.ShapeDtypeStruct((3, width, head_width), jnp.bfloat16),
            jax.ShapeDtypeStruct((3, 8, head_width), jnp.float32),
            jax.ShapeDtypeStruct((8, width), jnp.float32),
        ],
        scratch_shapes=[pltpu.VMEM((3, 8, head_width), jnp.float32)],
        compiler_params=pltpu.CompilerParams(vmem_limit_bytes=VMEM_BYTES),
        cost_estimate=pl.CostEstimate(
            flops=6 * tokens * width * head_width, bytes_accessed=4 * tokens * width, transcendentals=0
        ),
        name="qkv_weight_grad",
    )(whole, grad_cat, qkv_all, norm)


def finish_kernel(down_ref, up_ref, dense_ref, qkv_ref, one_ref, two_ref, residual_ref, bias_ref, grad_ref,
                  down_out, up_out, dense_out, qkv_out, rows_out, grad_out):
    down_out[...] = down_ref[...].astype(jnp.float32)
    total = up_ref[0].astype(jnp.float32)
    for group in range(1, up_ref.shape[0]):
        total = total + up_ref[group].astype(jnp.float32)
    up_out[...] = total
    dense_out[...] = dense_ref[...].astype(jnp.float32)
    qkv_out[...] = qkv_ref[...].astype(jnp.float32)
    half = pl.program_id(0) < pl.num_programs(0) // 2
    branch = jnp.where(half, one_ref[...], two_ref[...]).astype(jnp.float32) + bias_ref[...]
    rows_out[...] = (residual_ref[...] + branch).astype(jnp.bfloat16)
    grad_out[...] = grad_ref[...]


def finish(down, up, dense, qkv, one, two, residual, bias, input_grad):
    steps = 4

    def split(shape):
        if len(shape) == 3:
            return pl.BlockSpec((shape[0], shape[1] // steps, shape[2]), lambda i: (0, i, 0))
        return pl.BlockSpec((shape[0] // steps, shape[1]), lambda i: (i, 0))

    operands = (down, up, dense, qkv, one, two, residual, bias[None], input_grad)
    specs = [split(item.shape) for item in operands]
    row_part = (residual.shape[0] // steps, residual.shape[1])
    specs[4] = pl.BlockSpec(row_part, lambda i: (jnp.minimum(i, steps // 2 - 1), 0))
    specs[5] = pl.BlockSpec(row_part, lambda i: (jnp.maximum(i - steps // 2, 0), 0))
    specs[7] = pl.BlockSpec((1, bias.shape[0]), lambda i: (0, 0))
    outs = [jax.ShapeDtypeStruct(item.shape, jnp.float32) for item in (down, up[0], dense, qkv)]
    outs.append(jax.ShapeDtypeStruct(residual.shape, jnp.bfloat16))
    outs.append(jax.ShapeDtypeStruct(input_grad.shape, jnp.float32))
    return pl.pallas_call(
        finish_kernel,
        grid=(steps,),
        in_specs=specs,
        out_specs=[split(item.shape) for item in outs],
        out_shape=outs,
        compiler_params=pltpu.CompilerParams(vmem_limit_bytes=VMEM_BYTES),
        name="finish",
    )(*operands)


def dense_backward_kernel(branch_ref, attended_ref, dense_ref, grad_ref, weight_ref, total):
    parts, _, part = dense_ref.shape
    block = pl.program_id(0)

    @pl.when(block == 0)
    def _():
        total[...] = jnp.zeros_like(total)

    back = None
    for index in range(parts):
        cols = slice(index * part, (index + 1) * part)
        term = lax.dot_general(
            branch_ref[:, cols], dense_ref[index], NT, preferred_element_type=jnp.float32
        )
        back = term if index == 0 else back + term
    grad_ref[...] = back.astype(jnp.bfloat16)
    total[...] += lax.dot_general(
        attended_ref[...], branch_ref[...], (((0,), (0,)), ((), ())), preferred_element_type=jnp.float32
    )

    @pl.when(block == pl.num_programs(0) - 1)
    def _():
        weight_ref[...] = total[...].astype(jnp.bfloat16)


def dense_backward(branch, attended, dense_all):
    tokens, width = branch.shape
    head_width = attended.shape[1]
    block = min(512, tokens)
    return pl.pallas_call(
        dense_backward_kernel,
        grid=(tokens // block,),
        in_specs=[
            pl.BlockSpec((block, width), lambda i: (i, 0)),
            pl.BlockSpec((block, head_width), lambda i: (i, 0)),
            pl.BlockSpec(dense_all.shape, lambda i: (0, 0, 0)),
        ],
        out_specs=[
            pl.BlockSpec((block, head_width), lambda i: (i, 0)),
            pl.BlockSpec((head_width, width), lambda i: (0, 0)),
        ],
        out_shape=[
            jax.ShapeDtypeStruct((tokens, head_width), jnp.bfloat16),
            jax.ShapeDtypeStruct((head_width, width), jnp.bfloat16),
        ],
        scratch_shapes=[pltpu.VMEM((head_width, width), jnp.float32)],
        compiler_params=pltpu.CompilerParams(vmem_limit_bytes=VMEM_BYTES),
        cost_estimate=pl.CostEstimate(
            flops=4 * tokens * width * head_width, bytes_accessed=2 * tokens * width, transcendentals=0
        ),
        name="dense_backward",
    )(branch, attended, dense_all)


def project_kernel(rows_ref, weight_ref, bias_ref, out_ref):
    parts, three, part, head_width = weight_ref.shape
    for kind in range(three):
        total = None
        for index in range(parts):
            term = jnp.dot(
                rows_ref[:, index * part : (index + 1) * part],
                weight_ref[index, kind],
                preferred_element_type=jnp.float32,
            )
            total = term if index == 0 else total + term
        cols = slice(kind * head_width, (kind + 1) * head_width)
        out_ref[:, cols] = (total + bias_ref[:, cols]).astype(jnp.bfloat16)


def project(whole, qkv_all, query_value_bias):
    tokens, width = whole.shape
    head_width = qkv_all.shape[3]
    bias = jnp.concatenate(
        [query_value_bias[0], jnp.zeros_like(query_value_bias[0]), query_value_bias[1]]
    )[None]
    block = min(512, tokens)
    return pl.pallas_call(
        project_kernel,
        grid=(tokens // block,),
        in_specs=[
            pl.BlockSpec((block, width), lambda i: (i, 0)),
            pl.BlockSpec(qkv_all.shape, lambda i: (0, 0, 0, 0)),
            pl.BlockSpec((1, 3 * head_width), lambda i: (0, 0)),
        ],
        out_specs=pl.BlockSpec((block, 3 * head_width), lambda i: (i, 0)),
        out_shape=jax.ShapeDtypeStruct((tokens, 3 * head_width), jnp.bfloat16),
        compiler_params=pltpu.CompilerParams(vmem_limit_bytes=VMEM_BYTES),
        cost_estimate=pl.CostEstimate(
            flops=6 * tokens * width * head_width, bytes_accessed=2 * tokens * width, transcendentals=0
        ),
        name="project",
    )(whole, qkv_all, bias)


MLP_TILE = 256


def mlp_forward_kernel(rows_ref, up_ref, bias_ref, down_ref, active_ref, slope_ref, one_ref, two_ref):
    width = up_ref.shape[1]
    for first in range(0, width, MLP_TILE):
        cols = slice(first, first + MLP_TILE)
        value = jnp.dot(rows_ref[...], up_ref[:, cols], preferred_element_type=jnp.float32)
        value = value + bias_ref[:, cols]
        below = 0.5 + 0.5 * lax.erf(value * math.sqrt(0.5))
        density = jnp.exp(-0.5 * value * value) * (1.0 / math.sqrt(2.0 * math.pi))
        slope_ref[:, cols] = below + value * density
        active_ref[:, cols] = (value * below).astype(jnp.bfloat16)
    branch = jnp.dot(
        active_ref[...], down_ref[...], preferred_element_type=jnp.float32
    ).astype(jnp.bfloat16)
    half = one_ref.shape[0]
    one_ref[...] = branch[:half]
    two_ref[...] = branch[half:]


def resident(shape):
    return pl.BlockSpec(shape, lambda i: (0,) * len(shape), pipeline_mode=pl.Buffered(1))


def mlp_forward(rows, block, up_full, up_bias, down_full):
    tokens, width = rows.shape
    hidden = up_full.shape[1]
    return pl.pallas_call(
        mlp_forward_kernel,
        grid=(tokens // block,),
        in_specs=[
            pl.BlockSpec((block, width), lambda i: (i, 0)),
            resident((width, hidden)),
            resident((1, hidden)),
            resident((hidden, width)),
        ],
        out_specs=[
            pl.BlockSpec((block, hidden), lambda i: (i, 0)),
            pl.BlockSpec((block, hidden), lambda i: (i, 0)),
            pl.BlockSpec((block // 2, width), lambda i: (i, 0)),
            pl.BlockSpec((block // 2, width), lambda i: (i, 0)),
        ],
        out_shape=[
            jax.ShapeDtypeStruct((tokens, hidden), jnp.bfloat16),
            jax.ShapeDtypeStruct((tokens, hidden), jnp.float32),
            jax.ShapeDtypeStruct((tokens // 2, width), jnp.bfloat16),
            jax.ShapeDtypeStruct((tokens // 2, width), jnp.bfloat16),
        ],
        compiler_params=pltpu.CompilerParams(vmem_limit_bytes=VMEM_BYTES),
        cost_estimate=pl.CostEstimate(
            flops=4 * tokens * width * hidden, bytes_accessed=8 * tokens * width, transcendentals=0
        ),
        name="mlp_forward",
    )(rows, up_full, up_bias[None], down_full)


def mlp_backward_kernel(
    one_ref, two_ref, slope_ref, down_ref, up_ref, whole_ref, pre_ref, part_ref, sums_ref
):
    half = one_ref.shape[1]
    whole_ref[:half, :] = one_ref[0]
    whole_ref[half:, :] = two_ref[0]
    hidden = slope_ref.shape[1]

    @pl.when(pl.program_id(0) == 0)
    def _():
        sums_ref[...] = jnp.zeros_like(sums_ref)

    for first in range(0, hidden, MLP_TILE):
        cols = slice(first, first + MLP_TILE)
        grad = lax.dot_general(
            whole_ref[...], down_ref[cols, :], NT, preferred_element_type=jnp.float32
        )
        pre = (grad * slope_ref[:, cols]).astype(jnp.bfloat16)
        pre_ref[:, cols] = pre
        sums_ref[:, cols] += jnp.sum(pre.astype(jnp.float32).reshape(-1, 8, MLP_TILE), axis=0)
    part_ref[...] = lax.dot_general(
        pre_ref[...], up_ref[...], NT, preferred_element_type=jnp.float32
    ).astype(jnp.bfloat16)


def mlp_backward(one, two, slope, down_full, up_full):
    ranks, half, width = one.shape
    rows = 2 * half
    hidden = slope.shape[1]
    tokens = ranks * rows
    return pl.pallas_call(
        mlp_backward_kernel,
        grid=(ranks,),
        in_specs=[
            pl.BlockSpec((1, half, width), lambda i: (i, 0, 0)),
            pl.BlockSpec((1, half, width), lambda i: (i, 0, 0)),
            pl.BlockSpec((rows, hidden), lambda i: (i, 0)),
            resident((hidden, width)),
            resident((width, hidden)),
        ],
        out_specs=[
            pl.BlockSpec((rows, width), lambda i: (i, 0)),
            pl.BlockSpec((rows, hidden), lambda i: (i, 0)),
            pl.BlockSpec((rows, width), lambda i: (i, 0)),
            pl.BlockSpec((8, hidden), lambda i: (0, 0)),
        ],
        out_shape=[
            jax.ShapeDtypeStruct((tokens, width), jnp.bfloat16),
            jax.ShapeDtypeStruct((tokens, hidden), jnp.bfloat16),
            jax.ShapeDtypeStruct((tokens, width), jnp.bfloat16),
            jax.ShapeDtypeStruct((8, hidden), jnp.float32),
        ],
        compiler_params=pltpu.CompilerParams(vmem_limit_bytes=VMEM_BYTES),
        cost_estimate=pl.CostEstimate(
            flops=4 * tokens * width * hidden, bytes_accessed=10 * tokens * width, transcendentals=0
        ),
        name="mlp_backward",
    )(one, two, slope, down_full, up_full)


def over_dp(grad, dimension):
    return lax.psum_scatter(grad, "dp", scatter_dimension=dimension, tiled=True)


def layer(
    layer_input,
    segment_ids,
    first_gain,
    first_shift,
    qkv_weight,
    query_value_bias,
    dense_weight,
    dense_bias,
    second_gain,
    second_shift,
    up_weight,
    up_bias,
    down_weight,
    down_bias,
    out_grad,
):
    rows, width = layer_input.shape
    ranks = lax.axis_size("tensor")
    groups = lax.axis_size("dp")
    tokens = ranks * rows
    f32_rows = jax.ShapeDtypeStruct((rows, width), jnp.float32)

    qkv_all = lax.all_gather(qkv_weight, "dp", axis=0, tiled=False)
    dense_all = lax.all_gather(dense_weight, "dp", axis=0, tiled=False)
    up_full = lax.all_gather(up_weight, "dp", axis=0, tiled=True)
    down_full = lax.all_gather(down_weight, "dp", axis=1, tiled=True)
    half = rows // 2
    out_one = lax.all_gather(out_grad[:half], "tensor", axis=0, tiled=False)
    out_two = lax.all_gather(out_grad[half:], "tensor", axis=0, tiled=False)

    head_width = qkv_all.shape[3]
    up_width = up_bias.shape[0]
    (whole1,) = line_call(
        norm_gather_kernel, 1,
        (layer_input, first_gain[None], first_shift[None]), (), rows, width, reduces=False,
    )
    whole1 = whole1.reshape(tokens, width)
    projected = project(whole1, qkv_all, query_value_bias)
    head_count = head_width // HEAD_DIM
    tensor_pos = lax.axis_index("tensor")
    global_heads = tensor_pos * head_count + jnp.arange(head_count, dtype=jnp.int32)
    slopes = jnp.power(2.0, -8.0 * (global_heads + 1).astype(jnp.float32) / HEADS)
    attended, log_sums = attention_forward(projected, segment_ids, slopes)
    whole2, residual = line_call(
        branch_norm_gather_kernel, 2,
        (attended, dense_all, layer_input, dense_bias[None], second_gain[None], second_shift[None]),
        (f32_rows,), rows, width, product=True,
    )
    whole2 = whole2.reshape(tokens, width)
    activated, slope, mlp_one, mlp_two = mlp_forward(whole2, rows, up_full, up_bias, down_full)
    out_whole, pre_grad, normed2_part, up_bias_sums = mlp_backward(
        out_one, out_two, slope, down_full, up_full
    )
    up_bias_part = jnp.sum(up_bias_sums, axis=0)
    down_grad = lax.dot_general(
        activated, out_whole, (((0,), (0,)), ((), ())), preferred_element_type=jnp.float32
    ).astype(jnp.bfloat16)
    normed2_part, down_grad = lax.optimization_barrier((normed2_part, down_grad))
    down_wgrad = over_dp(down_grad, 1)
    mlp_rows_one = lax.psum_scatter(mlp_one, "tensor", scatter_dimension=0, tiled=True)
    mlp_rows_two = lax.psum_scatter(mlp_two, "tensor", scatter_dimension=0, tiled=True)

    branch_whole, up_parts, residual_grad, second_sums = line_call(
        grad_gather_kernel, 3,
        (normed2_part.reshape(ranks, rows, width), whole2, residual, out_grad, second_gain[None], pre_grad),
        (
            jax.ShapeDtypeStruct((groups, width // groups, up_width), jnp.bfloat16),
            f32_rows,
            jax.ShapeDtypeStruct((4, 8, width), jnp.float32),
        ),
        rows, width, placed=(2, 1), more=Beside.scratch(tokens, width, up_width, groups),
    )
    branch_whole = branch_whole.reshape(tokens, width)
    attended_grad, dense_grad = dense_backward(branch_whole, attended, dense_all)
    qkv_grad_cat = attention_backward(projected, attended_grad, segment_ids, slopes, log_sums)
    dense_wgrad = over_dp(dense_grad, 1)
    qkv_grad, qkv_sums, first_sums = qkv_weight_grad(
        whole1, qkv_grad_cat, qkv_all, first_gain, first_shift
    )
    qkv_grad, qkv_grad_cat = lax.optimization_barrier((qkv_grad, qkv_grad_cat))
    qkv_wgrad = over_dp(qkv_grad, 1)
    qkv_sums = jnp.sum(qkv_sums, axis=1)
    part = width // ranks
    bias_rows = 2 * head_width // part
    up_rows = up_width // part
    own = jnp.concatenate([qkv_sums[0], qkv_sums[2], up_bias_part]).reshape(-1, part)
    own = jnp.pad(own, ((0, 8 - own.shape[0]), (0, 0)))
    f32_sums = jax.ShapeDtypeStruct((8, width), jnp.float32)
    input_grad, sums, own = line_call(
        grad_kernel, 4,
        (qkv_grad_cat, qkv_all, layer_input, residual_grad, first_gain[None], first_sums, second_sums, own),
        (f32_rows, f32_sums, jax.ShapeDtypeStruct((8, part), jnp.float32)),
        rows, width, gathers=False, product=True, sums=True,
    )
    down_wgrad, up_wgrad, dense_wgrad, qkv_wgrad, layer_out, input_grad = finish(
        down_wgrad, up_parts, dense_wgrad, qkv_wgrad,
        mlp_rows_one, mlp_rows_two, residual, down_bias, input_grad,
    )
    return (
        layer_out,
        input_grad,
        sums[0],
        sums[1],
        qkv_wgrad,
        own[:bias_rows].reshape(2, head_width),
        dense_wgrad,
        sums[4],
        sums[2],
        sums[3],
        up_wgrad,
        own[bias_rows : bias_rows + up_rows].reshape(up_width),
        down_wgrad,
        sums[5],
    )


def solution(mesh):
    token_rows = P(("dp", "tensor"), None)
    placed = (
        token_rows,
        P("dp"),
        P(),
        P(),
        P(None, "dp", "tensor"),
        P(None, "tensor"),
        P("tensor", "dp"),
        P(),
        P(),
        P(),
        P("dp", "tensor"),
        P("tensor"),
        P("tensor", "dp"),
        P(),
        token_rows,
    )
    return jax.shard_map(
        layer,
        mesh=mesh,
        in_specs=placed,
        out_specs=(
            token_rows,
            token_rows,
            P(),
            P(),
            P(None, "dp", "tensor"),
            P(None, "tensor"),
            P("tensor", "dp"),
            P(),
            P(),
            P(),
            P("dp", "tensor"),
            P("tensor"),
            P("tensor", "dp"),
            P(),
        ),
        check_vma=False,
    )
```
